8 devices in a mesh: rep: 1 (over z), dp: 8 (over x, y, core).
Axes of the slice: x: 2, y: 2, z: 1, core: 2. Of those that a mesh axis runs over, the one named last changes fastest.
Arguments:
- x: bfloat16 [8, 2048, 768], P(('rep', 'dp'))
- dy: bfloat16 [8, 2048, 768], P(('rep', 'dp'))
- wq: bfloat16 [2, 768, 768], P(None, 'dp')
- wk: bfloat16 [2, 768, 128], P(None, 'dp')
- wv: bfloat16 [2, 768, 128], P(None, 'dp')
- wo: bfloat16 [2, 768, 768], P(None, 'dp')
- w_gate: bfloat16 [2, 768, 2048], P(None, 'dp')
- w_up: bfloat16 [2, 768, 2048], P(None, 'dp')
- w_down: bfloat16 [2, 2048, 768], P(None, 'dp')
- m_wq: float32 [2, 768, 768], P(None, 'dp')
- m_wk: float32 [2, 768, 128], P(None, 'dp')
- m_wv: float32 [2, 768, 128], P(None, 'dp')
- m_wo: float32 [2, 768, 768], P(None, 'dp')
- m_w_gate: float32 [2, 768, 2048], P(None, 'dp')
- m_w_up: float32 [2, 768, 2048], P(None, 'dp')
- m_w_down: float32 [2, 2048, 768], P(None, 'dp')
- v_wq: float32 [2, 768, 768], P(None, 'dp')
- v_wk: float32 [2, 768, 128], P(None, 'dp')
- v_wv: float32 [2, 768, 128], P(None, 'dp')
- v_wo: float32 [2, 768, 768], P(None, 'dp')
- v_w_gate: float32 [2, 768, 2048], P(None, 'dp')
- v_w_up: float32 [2, 768, 2048], P(None, 'dp')
- v_w_down: float32 [2, 2048, 768], P(None, 'dp')
Outputs:
- output 1: bfloat16 [2, 768, 768], P('rep', 'dp')
- output 2: bfloat16 [2, 768, 128], P('rep', 'dp')
- output 3: bfloat16 [2, 768, 128], P('rep', 'dp')
- output 4: bfloat16 [2, 768, 768], P('rep', 'dp')
- output 5: bfloat16 [2, 768, 2048], P('rep', 'dp')
- output 6: bfloat16 [2, 768, 2048], P('rep', 'dp')
- output 7: bfloat16 [2, 2048, 768], P('rep', 'dp')
- output 8: float32 [2, 768, 768], P('rep', 'dp')
- output 9: float32 [2, 768, 128], P('rep', 'dp')
- output 10: float32 [2, 768, 128], P('rep', 'dp')
- output 11: float32 [2, 768, 768], P('rep', 'dp')
- output 12: float32 [2, 768, 2048], P('rep', 'dp')
- output 13: float32 [2, 768, 2048], P('rep', 'dp')
- output 14: float32 [2, 2048, 768], P('rep', 'dp')
- output 15: float32 [2, 768, 768], P('rep', 'dp')
- output 16: float32 [2, 768, 128], P('rep', 'dp')
- output 17: float32 [2, 768, 128], P('rep', 'dp')
- output 18: float32 [2, 768, 768], P('rep', 'dp')
- output 19: float32 [2, 768, 2048], P('rep', 'dp')
- output 20: float32 [2, 768, 2048], P('rep', 'dp')
- output 21: float32 [2, 2048, 768], P('rep', 'dp')
All inputs are finite; a program needn't handle non-finite values.
Results may differ from the reference program's by a relative error of at most 0.0304.
Values are sent between devices in bfloat16 or wider.
A program may use at most 2 GiB of HBM per device.

```python
import jax
import jax.numpy as jnp
from jax import lax

SEQUENCES = 8
TOKENS = 2048
D = 768
HEADS = 6
KV_HEADS = 1
HEAD = 128
FF = 2048
LAYERS = 2
THETA = 10000
NAMES = ("wq", "wk", "wv", "wo", "w_gate", "w_up", "w_down")
SHAPES = {
    "wq": (LAYERS, D, HEADS * HEAD),
    "wk": (LAYERS, D, KV_HEADS * HEAD),
    "wv": (LAYERS, D, KV_HEADS * HEAD),
    "wo": (LAYERS, HEADS * HEAD, D),
    "w_gate": (LAYERS, D, FF),
    "w_up": (LAYERS, D, FF),
    "w_down": (LAYERS, FF, D),
}


def bump(key, n, height):
    away = (jnp.arange(n, dtype=jnp.int32) - jax.random.randint(key, (), 0, n, jnp.int32)) % n
    return jnp.where(away < n // 8, height, 1.0)


def together(key, own, strength):
    shared = jax.random.normal(key, own.shape[1:], jnp.float32)
    return (own + strength * shared) * lax.rsqrt(1 + strength * strength)


def setup_inputs(seed: int = 0, part: int = 0) -> dict:
    kx, kdy, ka, kb, kz, kf, kh, kl, *keys = jax.random.split(jax.random.key(seed), 8 + 3 * len(NAMES))
    kx, kdy, ka, kb = (jax.random.fold_in(k, part) for k in (kx, kdy, ka, kb))
    kw, km, kv = (keys[i::3] for i in range(3))
    shape = (SEQUENCES, TOKENS, D)
    much_x, much_dy = jax.random.uniform(kz, (2,), jnp.float32, 0.0, 1.0)
    loud = 2.0 ** jax.random.uniform(jax.random.fold_in(kz, 1), (), jnp.float32, -1.0, 2.0)
    layers = 2.0 ** jax.random.uniform(kl, (LAYERS, 1, 1), jnp.float32, -1.0, 1.0)
    times = {"wq": 1.0, "wk": 1.0, "wv": 2.0, "wo": layers, "w_gate": 1.0, "w_up": bump(kh, FF, 4.0), "w_down": layers}
    x = together(ka, jax.random.normal(kx, shape, jnp.float32), much_x) * bump(kf, D, 4.0)
    dy = together(kb, jax.random.normal(kdy, shape, jnp.float32), much_dy)
    drawn = {"x": x.astype(jnp.bfloat16), "dy": (loud * dy * (SEQUENCES * TOKENS) ** -0.5).astype(jnp.bfloat16)}
    for key, name in zip(kw, NAMES, strict=True):
        drawn[name] = (jax.random.normal(key, SHAPES[name], jnp.float32) * SHAPES[name][1] ** -0.5 * times[name]).astype(jnp.bfloat16)
    for key, name in zip(km, NAMES, strict=True):
        drawn[f"m_{name}"] = 0.1 * jax.random.normal(key, SHAPES[name], jnp.float32)
    for key, name in zip(kv, NAMES, strict=True):
        drawn[f"v_{name}"] = jax.random.uniform(key, SHAPES[name], jnp.float32, 0.02, 0.06)
    return drawn


def matmul(a, w):
    return jnp.dot(a, w, preferred_element_type=jnp.float32).astype(jnp.bfloat16)


def normed(h):
    wide = h.astype(jnp.float32)
    scale = lax.rsqrt(jnp.mean(wide**2, -1, keepdims=True) + 1e-6)
    return (wide * scale).astype(jnp.bfloat16)


def turned(t, theta):
    half = t.shape[-1] // 2
    angle = jnp.arange(t.shape[0], dtype=jnp.float32)[:, None] * theta ** (-jnp.arange(half, dtype=jnp.float32) / half)
    cos, sin = jnp.cos(angle)[:, None], jnp.sin(angle)[:, None]
    a, b = t[..., :half].astype(jnp.float32), t[..., half:].astype(jnp.float32)
    return jnp.concatenate([a * cos - b * sin, b * cos + a * sin], -1).astype(jnp.bfloat16)


def seen_by(q, k, v):
    tokens, kv = q.shape[0], k.shape[1]
    q = q.reshape(tokens, kv, -1, q.shape[-1])
    scores = jnp.einsum("tgsd,ugd->gstu", q.astype(jnp.float32), k.astype(jnp.float32)) * q.shape[-1] ** -0.5
    place = jnp.arange(tokens)
    weights = jax.nn.softmax(jnp.where(place[:, None] >= place, scores, -jnp.inf), -1).astype(jnp.bfloat16)
    return jnp.einsum("gstu,ugd->tgsd", weights.astype(jnp.float32), v.astype(jnp.float32)).astype(jnp.bfloat16).reshape(tokens, -1)


def layer(h, w):
    a = normed(h)
    q, k = (turned(matmul(a, w[name]).reshape(h.shape[0], -1, HEAD), THETA) for name in ("wq", "wk"))
    h = h + matmul(seen_by(q, k, matmul(a, w["wv"]).reshape(h.shape[0], -1, HEAD)), w["wo"])
    b = normed(h)
    gate = jnp.dot(b, w["w_gate"], preferred_element_type=jnp.float32)
    up = jnp.dot(b, w["w_up"], preferred_element_type=jnp.float32)
    return h + matmul((jax.nn.silu(gate) * up).astype(jnp.bfloat16), w["w_down"])


def adamw(w, m, v, g):
    m = 0.9 * m + 0.1 * g
    v = 0.95 * v + 0.05 * g * g
    step = m * lax.rsqrt(v + 1e-8) + 0.1 * w
    return (w - 0.02 * step).astype(jnp.bfloat16), m, v


def clipped(gradients, sum_of_squares, count):
    factor = jnp.minimum(1.0, 0.5 * lax.rsqrt(sum_of_squares / count + 1e-30))
    return [g * factor for g in gradients]


def stack(weights, h):
    return lax.scan(lambda h, w: (layer(h, w), None), h, weights)[0]


def reference(x, dy, wq, wk, wv, wo, w_gate, w_up, w_down, m_wq, m_wk, m_wv, m_wo, m_w_gate, m_w_up, m_w_down, v_wq, v_wk, v_wv, v_wo, v_w_gate, v_w_up, v_w_down):
    weights = dict(zip(NAMES, (wq, wk, wv, wo, w_gate, w_up, w_down), strict=True))

    def take(so_far, sequence):
        h, by_y = sequence
        _, back = jax.vjp(stack, weights, h)
        by_weights, by_h = back(by_y)
        return jax.tree.map(lambda total, term: total + term.astype(jnp.float32), so_far, by_weights), by_h

    none_yet = {name: jnp.zeros(w.shape, jnp.float32) for name, w in weights.items()}
    by_weights, by_x = lax.scan(take, none_yet, (x, dy))
    gradients = [by_weights[name].astype(jnp.bfloat16).astype(jnp.float32) for name in NAMES]
    gradients = clipped(gradients, sum(jnp.sum(g * g) for g in gradients), sum(g.size for g in gradients))
    first = (m_wq, m_wk, m_wv, m_wo, m_w_gate, m_w_up, m_w_down)
    second = (v_wq, v_wk, v_wv, v_wo, v_w_gate, v_w_up, v_w_down)
    new = [adamw(weights[name].astype(jnp.float32), m, v, g) for name, m, v, g in zip(NAMES, first, second, gradients, strict=True)]
    return tuple(one[which] for which in range(3) for one in new)
```

```python
import functools

import jax
import jax.numpy as jnp
import numpy as np
from jax import lax
from jax.experimental import pallas as pl
from jax.experimental.pallas import tpu as pltpu
from jax.sharding import PartitionSpec as P

HEAD, HEADS, D, FF = 128, 6, 768, 2048
THETA = 10000
SCALE = HEAD**-0.5
E = SCALE * 1.4426950408889634
NEG = -1e30
HIDDEN = 2 * NEG
EPS = 1e-6
QKV = D + 2 * HEAD
WA = QKV + D
GU = 2 * FF
ROWS, FROWS = D // 8, FF // 8
COARSE = 64
SPLITS = 3
PAIRS = HEADS // 2
B = 512
W = 256

BF, F32 = jnp.bfloat16, jnp.float32
VM = pltpu.VMEM
DMA = pltpu.SemaphoreType.DMA
MESH = pl.DeviceIdType.MESH
ANY = pl.BlockSpec(memory_space=pltpu.HBM)


def _place():
    return lax.axis_index("dp"), lax.axis_index("rep")


def _greet(bits):
    me, rep = _place()
    barrier = pltpu.get_barrier_semaphore()
    for bit in bits:
        pl.semaphore_signal(barrier, inc=1, device_id=(rep, me ^ bit), device_id_type=MESH)
    pl.semaphore_wait(barrier, len(bits))


class _Copy:
    def __init__(self, make):
        self.make = make

    def start(self):
        self.make().start()

    def wait(self):
        self.make().wait()

    def wait_send(self):
        self.make().wait_send()

    def wait_recv(self):
        self.make().wait_recv()


def _local(src, dst, sem):
    return _Copy(lambda: pltpu.make_async_copy(src, dst, sem))


def _remote(src, dst, sems, k, bit):
    me, rep = _place()
    return _Copy(lambda: pltpu.make_async_remote_copy(src_ref=src, dst_ref=dst, send_sem=sems.at[0, k], recv_sem=sems.at[1, k],
                                                      device_id=(rep, me ^ bit), device_id_type=MESH))


def _start(copies):
    for c in copies:
        c.start()


def _wait(copies):
    for c in copies:
        c.wait()


class _Gather:
    def __init__(self, parts, full, sems, local, own=None):
        me, _ = _place()
        rows = parts[0].shape[0]
        half = rows // 2

        def at(dev, first=0, count=rows):
            return full.at[pl.ds(pl.multiple_of(dev * rows + first, 16), count), :]

        def copy(k, bit, dev, first=0, count=rows, src=None):
            return _remote(at(dev, first, count) if src is None else src, at(dev, first, count), sems, k, bit)

        mine = at(me) if own is None else own
        self.loads, col = [], 0
        for k, part in enumerate(parts):
            width = part.shape[1]
            self.loads.append(_local(part, mine.at[:, pl.ds(col, width)], local.at[k]))
            col += width
        self.store = [] if own is None else [_local(own, at(me), local.at[4])]
        self.x, self.y, self.core = (copy(k, bit, me, src=mine) for k, bit in enumerate((4, 2, 1)))
        self.far = [copy(3, 4, me ^ 2, 0, half), copy(4, 2, me ^ 4, half, half)]
        self.near = [copy(5, 1, me ^ 4), copy(6, 1, me ^ 2)]
        self.end = [copy(7, 1, me ^ 6, 0, half), copy(8, 1, me ^ 6, half, half)]

    def load(self):
        _start(self.loads)

    def start(self):
        _wait(self.loads)
        _start([self.x, self.y, self.core] + self.store)

    def forward(self):
        self.x.wait_recv()
        self.y.wait_recv()
        _start(self.far + self.near)

    def last(self):
        for c in self.far:
            c.wait_recv()
        _start(self.end)

    def finish(self):
        for c in [self.core] + self.near + self.end:
            c.wait_recv()
        for c in [self.x, self.y, self.core] + self.far + self.near + self.end:
            c.wait_send()
        _wait(self.store)


def _block(xy, other):
    me, _ = _place()
    return ((me // 2) ^ xy) * 2 + ((me % 2) ^ other)


def _blocks(full, rows, other):
    return [full.at[pl.ds(pl.multiple_of(_block(xy, other) * rows, 16), rows), :] for xy in range(4)]


class _Scatter:
    def __init__(self, keep, send, kept, came, ici, sems, local=None):
        self.kept, self.came, self.ici = kept, came, ici
        self.loads = [_local(keep[b], kept.at[b], local.at[b]) for b in range(4)] if local is not None else []
        self.keep = [kept.at[b] for b in range(4)] if self.loads else keep
        self.core = [_remote(send[b], came.at[b], sems, b, 1) for b in range(4)]
        self.out = [_remote(kept.at[b], ici.at[b - 1], sems, 3 + b, 2 * b) for b in range(1, 4)]

    def start(self):
        for b in (3, 2, 1, 0):
            _start([self.core[b]] + self.loads[b : b + 1])

    def forward(self):
        rows, step = self.came.shape[1], 16
        for b in (3, 2, 1):
            self.core[b].wait_recv()
            _wait(self.loads[b : b + 1])

            def add(i, _):
                at = pl.ds(pl.multiple_of(i * step, step), step)
                self.kept[b, at, :] = (self.keep[b][at, :].astype(F32) + self.came[b, at, :].astype(F32)).astype(BF)

            lax.fori_loop(0, rows // step, add, None)
            self.out[b - 1].start()

    def finish(self, g_ref):
        self.core[0].wait_recv()
        _wait(self.loads[:1])
        for c in self.out:
            c.wait_recv()
        rows, n = g_ref.shape
        step = 16

        def add(i, squares):
            at = pl.ds(pl.multiple_of(i * step, step), step)
            total = self.keep[0][at, :].astype(F32) + self.came[0, at, :].astype(F32)
            for b in range(3):
                total += self.ici[b, at, :].astype(F32)
            g = total.astype(BF)
            g_ref[at, :] = g
            g = g.astype(F32)
            return squares + g[:8] * g[:8] + g[8:] * g[8:]

        squares = lax.fori_loop(0, rows // step, add, jnp.zeros((8, n), F32))
        for c in self.core + self.out:
            c.wait_send()
        return sum(squares[:, c : c + HEAD] for c in range(0, n, HEAD))


def _scatter_scratch(rows, n):
    return [VM((4, rows, n), BF), VM((4, rows, n), BF), VM((3, rows, n), BF), DMA((2, 7)), DMA((4,))]


def _split_out(full, rows, keep, send, sems):
    copies = [_local(src, ref.at[b], sems.at[k, b]) for k, ref in enumerate((keep, send)) for b, src in enumerate(_blocks(full, rows, k))]
    _start(copies)
    return copies


def _dot(a, b, ca, cb):
    return lax.dot_general(a, b, (((ca,), (cb,)), ((), ())), preferred_element_type=F32)


_mm = functools.partial(_dot, ca=1, cb=0)
_mt = functools.partial(_dot, ca=1, cb=1)
_tm = functools.partial(_dot, ca=0, cb=0)


def _at(i, n):
    return pl.ds(pl.multiple_of(i * n, n), n)


def _when(cond, *todo):
    @pl.when(cond)
    def _():
        for do in todo:
            do()


def _loop(n, body):
    def step(i, _):
        body(i)

    lax.fori_loop(0, n, step, None)


def _scale(wide):
    return lax.rsqrt(jnp.mean(wide * wide, -1, keepdims=True) + EPS)


def _norm(wide):
    return (wide * _scale(wide)).astype(BF)


def _norm_back(h, dy, by):
    wide, dy = h.astype(F32), dy.astype(F32)
    scale = _scale(wide)
    back = scale * (dy - wide * (scale * scale * jnp.mean(dy * wide, -1, keepdims=True)))
    return (by.astype(F32) + back.astype(BF).astype(F32)).astype(BF)


def _turn(t, cos, sin):
    t = t.astype(F32)
    return (t * cos + pltpu.roll(t, HEAD // 2, 1) * sin).astype(BF)


def _turn_back(t, cos, sin):
    return (t * cos - pltpu.roll(t, HEAD // 2, 1) * sin).astype(BF)


def _call(body, name, args, specs, outs, out_specs, scratch, flops, talks):
    return pl.pallas_call(
        body,
        in_specs=specs,
        out_specs=out_specs,
        scratch_shapes=scratch,
        out_shape=[jax.ShapeDtypeStruct(*o) for o in outs],
        compiler_params=pltpu.CompilerParams(vmem_limit_bytes=67043328, collective_id=talks, has_side_effects=talks is not None),
        cost_estimate=pl.CostEstimate(flops=flops, transcendentals=0, bytes_accessed=flops // 1000),
        name=name,
    )(*args)


def _pairs(lo, hi, first, steps):
    first(lax.div(lo, PAIRS), 0, 0)

    def body(u, _):
        j, m = lax.div(u, PAIRS), lax.rem(u, PAIRS)
        later = jnp.minimum(u + 1, hi - 1)
        steps(j, 2 * m, 0, lambda: first(j, 2 * m + 1, 1))
        steps(j, 2 * m + 1, 1, lambda: first(lax.div(later, PAIRS), 2 * lax.rem(later, PAIRS), 0))

    lax.fori_loop(lo, hi, body, None)


def _flash_fwd(iq, qh, k_s, vt_s, top_s, mix_s, s_s, p_s, m_s, keep_s):
    top_s[:] = jnp.full(top_s.shape, NEG, F32)
    mix_s[:] = jnp.zeros(mix_s.shape, F32)
    rows = _at(iq, B)

    def run(lo, hi, masked):
        def score(j, n, slot):
            s = _mt(k_s[_at(j, B), :], qh[n, rows, :])
            if masked:
                s = jnp.where(lax.broadcasted_iota(jnp.int32, s.shape, 0) <= lax.broadcasted_iota(jnp.int32, s.shape, 1), s, HIDDEN)
            s_s[slot][:] = s
            m_s[slot][:] = s.max(axis=0, keepdims=True)

        def rest(j, n, slot, meanwhile):
            meanwhile()
            old = top_s[n]
            top = jnp.maximum(old, m_s[slot][:])
            top_s[n] = top
            keep_s[slot][:] = jnp.exp2((old - top) * E)
            for r in range(0, B, HEAD):
                p_s[slot][r : r + HEAD, :] = jnp.exp2((s_s[slot][r : r + HEAD, :] - top) * E).astype(BF)
            mix_s[n] = mix_s[n] * keep_s[slot][:] + _mm(vt_s[:, _at(j, B)], p_s[slot][:])

        _pairs(lo, hi, score, rest)

    run(PAIRS * iq, PAIRS * iq + PAIRS, True)
    _when(iq > 0, lambda: run(0, PAIRS * iq, False))


def _forward(x, near, far, *refs, layers):
    (wq, wk, wv, wo, wg, wu, wd, hm_o, q_o, k_o, v_o, o_o, la_o, s_o, r_o, hid_o, bt_o, h1_o, cos_o, sin_o, wa_o, wgu_o, wd_o,
     h, hm, w_s, wgu_s, wd_s, cos, sin, qh, k_s, v_s, vt_s, o, la, a_s, top_s, mix_s, s0, s1, p0, p1, m0, m1, e0, e1, up_s, dn_s, hid_s, bt_s,
     g_own, d_own, sem, out_sem, a_sem, a_loc, g_sem, g_loc, d_sem, d_loc) = refs
    tokens = h.shape[0]
    blocks = tokens // B
    A = lambda l: _Gather([w.at[l] for w in (wq, wk, wv, wo)], w_s.at[l], a_sem.at[l], a_loc.at[l])
    G = lambda l: _Gather([wg.at[l], wu.at[l]], wgu_o.at[l], g_sem.at[l], g_loc.at[l], g_own)
    N = lambda l: _Gather([wd.at[l]], wd_o.at[l], d_sem.at[l], d_loc.at[l], d_own)

    load = _local(x, h, sem.at[0])
    load.start()
    A(0).load()
    G(0).load()
    N(0).load()
    _greet((1, 2, 4))
    A(0).start()
    near_c, near_s = near[0], near[1]
    for i in range(far.shape[1]):
        far_c, far_s = far[0, i : i + 1, :], far[1, i : i + 1, :]
        rows = slice(i * COARSE, (i + 1) * COARSE)
        cos[rows, :] = far_c * near_c - far_s * near_s
        t = far_s * near_c + far_c * near_s
        sin[rows, :] = jnp.where(lax.broadcasted_iota(jnp.int32, t.shape, 1) < HEAD // 2, -t, t)
    tables = [_local(cos, cos_o, sem.at[1]), _local(sin, sin_o, sem.at[2])]
    _start(tables)
    vt_s[HEAD:, :] = jnp.ones((8, tokens), BF)
    A(0).forward()
    G(0).start()
    N(0).start()
    load.wait()
    A(0).last()
    A(0).finish()

    def project(l, r):
        at = _at(r, B)
        a_s[:] = _norm(h[at, :].astype(F32))
        c, s = cos[at, :], sin[at, :]
        for n in range(HEADS + 2):
            if n % 2 == 0:
                t = _mm(a_s[:], w_s[l, :, n * HEAD : (n + 2) * HEAD]).astype(BF)
            x = t[:, n % 2 * HEAD : (n % 2 + 1) * HEAD]
            if n < HEADS:
                qh[n, at, :] = _turn(x, c, s)
            elif n == HEADS:
                k_s[at, :] = _turn(x, c, s)
            else:
                v_s[at, :] = x
                vt_s[:HEAD, at] = x.T

    def attend(l, iq):
        at = _at(iq, B)
        _when(iq == 2, lambda: G(l).forward())
        _when(iq == 3, lambda: N(l).forward(), lambda: _when(l == 0, lambda: A(1).load()))
        _flash_fwd(iq, qh, k_s, vt_s, top_s, mix_s, (s0, s1), (p0, p1), (m0, m1), (e0, e1))
        lines = []
        for n in range(HEADS):
            total = mix_s[n, HEAD : HEAD + 1, :]
            o[at, n * HEAD : (n + 1) * HEAD] = (mix_s[n, :HEAD, :] * (1 / total)).astype(BF).T
            rest = -(top_s[n] + jnp.log2(total) * (1 / E))
            for _ in range(SPLITS):
                part = rest.astype(BF).astype(F32)
                lines.append(part)
                rest = rest - part
        lines.append(jnp.zeros((HEAD - SPLITS * HEADS, B), F32))
        la[at, :] = jnp.concatenate(lines, 0).astype(BF).T

    def merge(l, r):
        at = _at(r, B)
        out = _mm(o[at, :], w_s[l, :, QKV:]).astype(BF)
        hm[at, :] = (h[at, :].astype(F32) + out.astype(F32)).astype(BF)

    def saved(l, r):
        at, slot = _at(r, W), lax.rem(r, 2)
        pairs = ((up_s.at[slot], s_o.at[l, at, :]), (dn_s.at[slot], r_o.at[l, at, :]), (hid_s.at[slot], hid_o.at[l, at, :]), (bt_s.at[slot], bt_o.at[l, :, at]))
        return [_local(a, b, out_sem.at[slot, i]) for i, (a, b) in enumerate(pairs)]

    def mlp(l, r):
        at, slot = _at(r, W), lax.rem(r, 2)
        @pl.when(l == 0)
        def _():
            _when(r == 2, lambda: A(1).forward(), lambda: G(1).load(), lambda: N(1).load())
            _when(r == 3, lambda: G(1).start(), lambda: N(1).start())
            _when(r == 5, lambda: A(1).last())
            _when(r == 7, lambda: A(1).finish())

        _when(r > 1, lambda: _wait(saved(l, r - 2)))
        b = _norm(hm[at, :].astype(F32))
        bt_s[slot] = b.T
        for c in range(0, FF, W):
            cols = slice(c, c + W)
            gate = _mm(b, wgu_s[:, cols])
            up = _mm(b, wgu_s[:, FF + c : FF + c + W])
            sig = jax.nn.sigmoid(gate)
            silu = gate * sig
            up_s[slot, :, cols] = silu
            dn_s[slot, :, cols] = up * (sig + silu * (1 - sig))
            hid_s[slot, :, cols] = (silu * up).astype(BF)
        _start(saved(l, r))

        @pl.when(l < layers - 1)
        def _():
            out = _mm(hid_s[slot], wd_s[:]).astype(BF)
            h[at, :] = (hm[at, :].astype(F32) + out.astype(F32)).astype(BF)

    def layer(l):
        _loop(blocks, lambda r: project(l, r))
        outs = [_local(a, b.at[l], sem.at[3 + i]) for i, (a, b) in enumerate(((w_s.at[l], wa_o), (qh, q_o), (k_s, k_o), (v_s, v_o)))]
        _start(outs)
        _loop(blocks, lambda iq: attend(l, iq))
        G(l).last()
        N(l).last()
        _when(l == 0, lambda: A(1).start())
        G(l).finish()
        N(l).finish()
        weights = [_local(wgu_o.at[l], wgu_s, sem.at[7]), _local(wd_o.at[l], wd_s, sem.at[8])]
        _start(weights)
        _loop(blocks, lambda r: merge(l, r))
        more = [_local(a, b.at[l], sem.at[9 + i]) for i, (a, b) in enumerate(((hm, hm_o), (o, o_o), (la, la_o)))]
        _start(more)
        _wait(weights)
        _loop(tokens // W, lambda r: mlp(l, r))
        for n in (2, 1):
            _wait(saved(l, tokens // W - n))
        _wait(outs + more)
        _when(l == 0, lambda: _start([_local(h, h1_o, sem.at[0])]))

    _loop(layers, layer)
    _wait(tables + [_local(h, h1_o, sem.at[0])])


def forward(x, weights):
    T, layers = x.shape[0], weights[0].shape[0]
    tables = rotary_tables(T)
    L = lambda *s, t=BF: ((layers, *s), t)
    outs = [L(T, D), L(HEADS, T, HEAD), L(T, HEAD), L(T, HEAD), L(T, D), L(T, HEAD), L(T, FF, t=F32), L(T, FF, t=F32), L(T, FF), L(D, T),
            ((T, D), BF), ((T, HEAD), F32), ((T, HEAD), F32), L(D, WA), L(D, GU), L(FF, D)]
    line = VM((1, B), F32)
    scratch = [VM((T, D), BF), VM((T, D), BF), VM((layers, D, WA), BF), VM((D, GU), BF), VM((FF, D), BF), VM((T, HEAD), F32), VM((T, HEAD), F32),
               VM((HEADS, T, HEAD), BF), VM((T, HEAD), BF), VM((T, HEAD), BF), VM((HEAD + 8, T), BF), VM((T, D), BF), VM((T, HEAD), BF), VM((B, D), BF),
               VM((HEADS, 1, B), F32), VM((HEADS, HEAD + 8, B), F32), VM((B, B), F32), VM((B, B), F32), VM((B, B), BF), VM((B, B), BF),
               line, line, line, line, VM((2, W, FF), F32), VM((2, W, FF), F32), VM((2, W, FF), BF), VM((2, D, W), BF),
               VM((ROWS, GU), BF), VM((FROWS, D), BF), DMA((12,)), DMA((2, 4))] + [DMA((layers, 2, 9)), DMA((layers, 5))] * 3
    small = pl.BlockSpec(memory_space=VM)
    return _call(functools.partial(_forward, layers=layers), "forward", [x, *tables, *weights], [ANY, small, small] + [ANY] * 7, outs,
                 [ANY] * len(outs), scratch, 10**11, 0)


def _mlp_back(*refs, layer, carries):
    hm_i, dy_i, s_i, r_i, hid_i, bt_i, wgu_i, wd_i, *refs = refs
    keep, send = (refs.pop(0), refs.pop(0)) if carries else (None, None)
    dhm_o, kgu, sgu, kd, sd, *refs = refs
    g_o, sq_o = (refs.pop(0), refs.pop(0)) if carries else (None, None)
    hm, dy, up_s, dn_s, hid_s, wgu, wd, g0, g1, bt, dyt, db, sem, part_sem, split_sem, *scatter = refs
    tokens = hm.shape[0]
    blocks, parts = tokens // B, FF // W
    pending = lambda: _Scatter([keep.at[b] for b in range(4)], [send.at[b] for b in range(4)], *scatter)

    def part(c):
        slot, cols = c % 2 if isinstance(c, int) else lax.rem(c, 2), _at(c, W)
        return [_local(a.at[layer, :, cols], b.at[slot], part_sem.at[slot, i]) for i, (a, b) in enumerate(((r_i, dn_s), (s_i, up_s), (hid_i, hid_s)))]

    dys = [_local(dy_i.at[_at(r, B), :], dy.at[_at(r, B), :], sem.at[r]) for r in range(blocks)]
    head = _local(wd_i.at[layer, :W, :], wd.at[:W, :], sem.at[4])
    rest = [_local(wd_i.at[layer, W:, :], wd.at[W:, :], sem.at[5]), _local(bt_i.at[layer], bt, sem.at[6]), _local(wgu_i.at[layer], wgu, sem.at[7])]
    late = _local(hm_i.at[layer], hm, sem.at[8])
    _start([head] + dys[:1] + part(0)[:2] + dys[1:] + rest + part(0)[2:] + part(1) + [late])
    if carries:
        _greet((1, 2, 4, 6))
        pending().start()
    db[:] = jnp.zeros(db.shape, F32)

    def widen(c, slot, r, g):
        rows = slice(r * B, (r + 1) * B)
        t = _mt(dy[rows, :], wd[_at(c, W), :]).astype(BF).astype(F32)
        g[rows, :W] = (t * dn_s[slot, rows, :]).astype(BF)
        g[rows, W:] = (t * up_s[slot, rows, :]).astype(BF)

    head.wait()
    for r in range(blocks):
        dys[r].wait()
        if r == 0:
            _wait(part(0)[:2])
        dyt[:, r * B : (r + 1) * B] = dy[r * B : (r + 1) * B, :].T
        widen(0, 0, r, g0)
    _wait(rest + part(0)[2:])

    def step(c, slot, g, later):
        cols, up = _at(c, W), pl.ds(pl.multiple_of(FF + c * W, W), W)
        after = jnp.minimum(c + 1, parts - 1)
        _when(c + 1 < parts, lambda: _wait(part(c + 1)))
        for r in range(blocks):
            widen(after, 1 - slot, r, later)
        both = jnp.concatenate([wgu[:, cols], wgu[:, up]], 1)
        for r in range(blocks):
            rows = slice(r * B, (r + 1) * B)
            db[rows, :] += _mt(g[rows, :], both)
        dw = _mm(bt[:], g[:]).astype(BF)
        wgu[:, cols] = dw[:, :W]
        wgu[:, up] = dw[:, W:]
        wd[cols, :] = _mm(dyt[:], hid_s[slot]).astype(BF).T
        _when(c + 2 < parts, lambda: _start(part(c + 2)))
        if carries:
            _when(c == 1, lambda: pending().forward())

    def two(u):
        step(2 * u, 0, g0, g1)
        step(2 * u + 1, 1, g1, g0)

    _loop(parts // 2, two)
    copies = _split_out(wgu, ROWS, kgu, sgu, split_sem.at[0]) + _split_out(wd, FROWS, kd, sd, split_sem.at[1])
    late.wait()
    out = lambda r: _local(hm.at[_at(r, B), :], dhm_o.at[_at(r, B), :], sem.at[r])

    def back(r):
        at = _at(r, B)
        hm[at, :] = _norm_back(hm[at, :], db[at, :].astype(BF), dy[at, :])
        out(r).start()

    _loop(blocks, back)
    if carries:
        sq_o[:] = pending().finish(g_o)
    _wait(copies + [out(r) for r in range(blocks)])


WHOLE = pl.BlockSpec(memory_space=VM)


def mlp_back(saved, dy, layer, pending, talks):
    T = dy.shape[0]
    carries = pending is not None
    gu, d = ((4, ROWS, GU), BF), ((4, FROWS, D), BF)
    args = [saved[n] for n in ("hm", "s", "r", "hid", "bt", "wgu", "wd")]
    args.insert(1, dy)
    scratch = [VM((T, D), BF), VM((T, D), BF), VM((2, T, W), F32), VM((2, T, W), F32), VM((2, T, W), BF), VM((D, GU), BF), VM((FF, D), BF),
               VM((T, 2 * W), BF), VM((T, 2 * W), BF), VM((D, T), BF), VM((D, T), BF), VM((T, D), F32), DMA((9,)), DMA((2, 3)), DMA((2, 2, 4))]
    outs, out_specs = [((T, D), BF), gu, gu, d, d], [ANY] * 5
    if carries:
        args += pending
        outs += [((ROWS, WA), BF), ((8, HEAD), F32)]
        out_specs += [WHOLE, WHOLE]
        scratch += _scatter_scratch(ROWS, WA)
    return _call(functools.partial(_mlp_back, layer=layer, carries=carries), "mlp_back", args, [ANY] * len(args), outs, out_specs, scratch,
                 4 * 10**10, talks)


def _flash_back(iq, qh, qt, doh, dot, la, dl, zs, k_s, v_s, dq, dkt, dvt, p_s, x_s):
    rows = _at(iq, B)

    def run(lo, hi, masked):
        def weigh(j, n, slot):
            keys = _at(j, B)
            s = _mt(jnp.concatenate([qh[n, rows, :], la[rows, :]], 1), jnp.concatenate([k_s[keys, :], zs[n]], 1))
            d = _mt(jnp.concatenate([doh[n, rows, :], dl[rows, :]], 1), jnp.concatenate([v_s[keys, :], zs[n]], 1))
            for e in range(0, B, HEAD):
                cols = slice(e, e + HEAD)
                p = jnp.exp2(s[:, cols] * E)
                if masked:
                    p = jnp.where(lax.broadcasted_iota(jnp.int32, p.shape, 0) >= e + lax.broadcasted_iota(jnp.int32, p.shape, 1), p, 0.0)
                p_s[slot][:, cols] = p.astype(BF)
                x_s[slot][:, cols] = (p * d[:, cols]).astype(BF)

        def rest(j, n, slot, meanwhile):
            keys = _at(j, B)
            dvt[:, keys] += _mm(dot[n, :, rows], p_s[slot][:])
            dkt[:, keys] += _mm(qt[n, :, rows], x_s[slot][:])
            dq[n] += _mm(x_s[slot][:], k_s[keys, :])
            meanwhile()

        _pairs(lo, hi, weigh, rest)

    run(PAIRS * iq, PAIRS * iq + PAIRS, True)
    _when(iq > 0, lambda: run(0, PAIRS * iq, False))


def _attn_back(*refs, layer, count):
    first = layer == 0
    dhm_i, h_i, q_i, k_i, v_i, o_i, la_i, cos_i, sin_i, wa_i, kgu, sgu, kd, sd, *refs = refs
    if first:
        sq_a, sq_b, ggu_o, gd_o, ga_o, factor_o, *refs = refs
    else:
        ggu_o, gd_o, sq_o, dh_o, keep_o, send_o, *refs = refs
    (dhm, h, qh, k_s, v_s, o, la, cos, sin, wa, doh, dqkv, a_s, qt, dot, dl, zs, dq, dkt, dvt, p0, p1, x0, x1, dn_s, sem, split_sem, *refs) = refs
    scatter_gu, scatter_d, refs = refs[:5], refs[5:10], refs[10:]
    tokens = h.shape[0]
    blocks = tokens // B
    pending = lambda: [_Scatter([a.at[b] for b in range(4)], [c.at[b] for b in range(4)], *s) for a, c, s in ((kgu, sgu, scatter_gu), (kd, sd, scatter_d))]

    def piece(i, a, b):
        return _local(a, b, sem.at[i])

    wo = piece(0, wa_i.at[layer, :, pl.ds(QKV, D)], wa.at[:, pl.ds(QKV, D)])
    groups = []
    for r in range(blocks):
        at = _at(r, B)
        pairs = ((dhm_i.at[at, :], dhm.at[at, :]), (q_i.at[layer, :, at, :], qh.at[:, at, :]), (o_i.at[layer, at, :], o.at[at, :]))
        groups.append([piece(1 + 3 * r + i, a, b) for i, (a, b) in enumerate(pairs)])
    pairs = ((la_i.at[layer], la), (k_i.at[layer], k_s), (v_i.at[layer], v_s), (h_i, h), (cos_i, cos), (sin_i, sin),
             (wa_i.at[layer, :, pl.ds(0, QKV)], wa.at[:, pl.ds(0, QKV)]))
    late = [piece(1 + 3 * blocks + i, a, b) for i, (a, b) in enumerate(pairs)]
    _start([wo] + sum(groups, []) + late)
    _greet(range(1, 8) if first else (1, 2, 4, 6))
    for s in pending():
        s.start()
    dkt[:] = jnp.zeros(dkt.shape, F32)
    dvt[:] = jnp.zeros(dvt.shape, F32)
    lane = lax.broadcasted_iota(jnp.int32, (B, HEAD), 1)
    for n in range(HEADS):
        zs[n] = ((lane >= SPLITS * n) & (lane < SPLITS * (n + 1))).astype(F32).astype(BF)
    wo.wait()

    def lead(r):
        at = _at(r, B)
        do = _mt(dhm[at, :], wa[:, QKV:]).astype(BF)
        means = jnp.zeros(lane.shape, F32)
        for n in range(HEADS):
            cols = slice(n * HEAD, (n + 1) * HEAD)
            by = do[:, cols]
            doh[n, at, :] = by
            dot[n, :, at] = by.T
            qt[n, :, at] = qh[n, at, :].T
            rest = -jnp.sum(by.astype(F32) * o[at, cols].astype(F32), -1, keepdims=True)
            for i in range(SPLITS):
                part = rest.astype(BF).astype(F32)
                means = jnp.where(lane == SPLITS * n + i, part, means)
                rest = rest - part
        dl[at, :] = means.astype(BF)

    def begin(r):
        for k in range(blocks):
            _when(r == k, lambda: _wait(groups[k]))
        lead(r)

    _loop(blocks, begin)
    wa[:, QKV:] = _tm(o[:], dhm[:]).astype(BF)
    _wait(late)
    for s in pending():
        s.forward()

    def attend(g):
        iq = blocks - 1 - g
        at = _at(iq, B)
        dq[:] = jnp.zeros(dq.shape, F32)
        _flash_back(iq, qh, qt, doh, dot, la, dl, zs, k_s, v_s, dq, dkt, dvt, (p0, p1), (x0, x1))
        c, s = cos[at, :], sin[at, :]
        _loop(HEADS, lambda n: dqkv.__setitem__((at, _at(n, HEAD)), _turn_back(dq[n] * SCALE, c, s)))
        dqkv[at, D : D + HEAD] = _turn_back((dkt[:, at] * SCALE).T, c, s)
        dqkv[at, D + HEAD :] = dvt[:, at].T.astype(BF)
        a_s[at, :] = _norm(h[at, :].astype(F32))

    _loop(blocks, attend)
    dw = lambda: wa.__setitem__((slice(None), slice(0, QKV)), _tm(a_s[:], dqkv[:]).astype(BF))
    if first:
        dw()
        came, ici, own_sem, mine, all_s, all_sem = refs
        own = _Scatter(_blocks(wa, ROWS, 0), _blocks(wa, ROWS, 1), scatter_gu[0].at[:, :, pl.ds(0, WA)], came, ici, own_sem)
        own.start()
        gu, d = pending()
        squares = gu.finish(ggu_o) + d.finish(gd_o) + sq_a[:] + sq_b[:]
        own.forward()
        mine[:] = own.finish(ga_o) + squares
        me, _ = _place()
        copies = [_remote(mine, all_s.at[me], all_sem, r, r) for r in range(1, 8)]
        _start(copies)
        all_s[me] = mine[:]
        _wait(copies)
        total = jnp.sum(jnp.sum(jnp.sum(all_s[:], axis=0), axis=1, keepdims=True), axis=0, keepdims=True)
        factor_o[:] = jnp.broadcast_to(jnp.minimum(1.0, 0.5 * lax.rsqrt(total / count + 1e-30)), factor_o.shape)
    else:
        out = lambda r: _local(h.at[_at(r, B), :], dh_o.at[_at(r, B), :], split_sem.at[2, r])

        def back(r):
            at = _at(r, B)
            dn_s[:] = _mt(dqkv[at, :], wa[:, :QKV]).astype(BF)
            h[at, :] = _norm_back(h[at, :], dn_s[:], dhm[at, :])
            out(r).start()

        _loop(blocks, back)
        dw()
        copies = _split_out(wa, ROWS, keep_o, send_o, split_sem)
        gu, d = pending()
        sq_o[:] = gu.finish(ggu_o) + d.finish(gd_o)
        _wait(copies + [out(r) for r in range(blocks)])


def attn_back(saved, dhm, h, layer, pending, squares, count, talks):
    T = h.shape[0]
    args = [dhm, h] + [saved[n] for n in ("q", "k", "v", "o", "la", "cos", "sin", "wa")] + [*pending, *squares]
    specs = [ANY] * (10 + len(pending)) + [WHOLE] * len(squares)
    dw, small = ((4, ROWS, WA), BF), ((8, HEAD), F32)
    outs, out_specs = [((ROWS, GU), BF), ((FROWS, D), BF)], [WHOLE, WHOLE]
    tile = VM((B, B), BF)
    scratch = [VM((T, D), BF), VM((T, D), BF), VM((HEADS, T, HEAD), BF), VM((T, HEAD), BF), VM((T, HEAD), BF), VM((T, D), BF), VM((T, HEAD), BF),
               VM((T, HEAD), F32), VM((T, HEAD), F32), VM((D, WA), BF), VM((HEADS, T, HEAD), BF), VM((T, QKV), BF), VM((T, D), BF),
               VM((HEADS, HEAD, T), BF), VM((HEADS, HEAD, T), BF), VM((T, HEAD), BF), VM((HEADS, B, HEAD), BF), VM((HEADS, B, HEAD), F32),
               VM((HEAD, T), F32), VM((HEAD, T), F32), tile, tile, tile, tile, VM((B, D), BF), DMA((20,)), DMA((3, 4)),
               *_scatter_scratch(ROWS, GU), *_scatter_scratch(FROWS, D)]
    if layer == 0:
        outs += [((ROWS, WA), BF), small]
        out_specs += [WHOLE, WHOLE]
        scratch += [VM((4, ROWS, WA), BF), VM((3, ROWS, WA), BF), DMA((2, 7)), VM((8, HEAD), F32), VM((8, 8, HEAD), F32), DMA((2, 8))]
    else:
        outs += [small, ((T, D), BF), dw, dw]
        out_specs += [WHOLE, ANY, ANY, ANY]
    return _call(functools.partial(_attn_back, layer=layer, count=count), "attn_back", args, specs, outs, out_specs, scratch, 5 * 10**10, talks)


def _adamw(*refs, cuts):
    factor = refs[0][0:1, 0:1]
    grads, refs = refs[1:7], refs[7:]
    w_in, m_in, v_in, w_out, m_out, v_out = (refs[i : i + 7] for i in range(0, 42, 7))
    for layer in range(2):

        @pl.when(pl.program_id(0) == layer)
        def _():
            for i, (which, a, b) in enumerate(cuts):
                g = grads[3 * layer + which][:, a:b].astype(F32) * factor
                m = 0.9 * m_in[i][0] + 0.1 * g
                v = 0.95 * v_in[i][0] + 0.05 * g * g
                w = w_in[i][0].astype(F32)
                step = m * lax.rsqrt(v + 1e-8) + 0.1 * w
                w_out[i][0] = (w - 0.02 * step).astype(BF)
                m_out[i][0] = m
                v_out[i][0] = v


def adamw(factor, grads, weights, m, v):
    cuts = ((0, 0, D), (0, D, D + HEAD), (0, D + HEAD, QKV), (0, QKV, WA), (1, 0, FF), (1, FF, GU), (2, 0, D))
    blocks = [pl.BlockSpec((1, t.shape[1] // 2, t.shape[2]), lambda n, s: (n, s, 0)) for t in weights]

    def grad(n, t):
        return pl.BlockSpec((t.shape[0] // 2, t.shape[1]), lambda l, s: (jnp.where(l == n, s, 1 - n), 0))

    flat = [(n, g) for n, layer in enumerate(grads) for g in layer]
    return pl.pallas_call(
        functools.partial(_adamw, cuts=cuts),
        grid=(2, 2),
        in_specs=[pl.BlockSpec((8, HEAD), lambda n, s: (0, 0))] + [grad(n, g) for n, g in flat] + blocks * 3,
        out_specs=blocks * 3,
        out_shape=[jax.ShapeDtypeStruct(t.shape, BF) for t in weights] + [jax.ShapeDtypeStruct(t.shape, F32) for t in weights] * 2,
        compiler_params=pltpu.CompilerParams(dimension_semantics=("arbitrary", "arbitrary"), vmem_limit_bytes=67043328),
        cost_estimate=pl.CostEstimate(flops=10**8, transcendentals=0, bytes_accessed=35 * 10**6),
        name="adamw",
    )(factor, *[g for _, g in flat], *weights, *m, *v)


def rotary_tables(tokens):
    half = HEAD // 2
    rate = THETA ** (-np.arange(half, dtype=np.float64) / half)

    def table(places):
        angle = np.concatenate([places[:, None] * rate] * 2, 1)
        return jnp.asarray(np.stack([np.cos(angle), np.sin(angle)]), F32)

    return table(np.arange(COARSE)), table(np.arange(0, tokens, COARSE))


def solution(mesh):
    def step(x, dy, *arrays):
        weights, m, v = (arrays[i : i + 7] for i in (0, 7, 14))
        x, dy = x[0], dy[0]
        names = ("hm", "q", "k", "v", "o", "la", "s", "r", "hid", "bt", "h1", "cos", "sin", "wa", "wgu", "wd")
        saved = dict(zip(names, forward(x, weights)))
        count = 8 * sum(w.size for w in weights)
        by_hm, *mlp1 = mlp_back(saved, dy, 1, None, None)
        ggu1, gd1, sq_a, by_h, *attn1 = attn_back(saved, by_hm, saved["h1"], 1, mlp1, [], count, 1)
        by_hm, *mlp0, ga1, sq_b = mlp_back(saved, by_h, 0, attn1, 2)
        ggu0, gd0, ga0, factor = attn_back(saved, by_hm, x, 0, mlp0, [sq_a, sq_b], count, 3)
        return tuple(adamw(factor, [[ga0, ggu0, gd0], [ga1, ggu1, gd1]], weights, m, v))

    states, cut = P(("rep", "dp"), None, None), P(None, "dp", None)
    return jax.shard_map(
        step,
        mesh=mesh,
        in_specs=(states, states) + (cut,) * 21,
        out_specs=(P("rep", "dp", None),) * 21,
        check_vma=False,
    )
```

```python
import functools
import itertools

import jax
import jax.numpy as jnp
import numpy as np
from jax import lax
from jax.experimental import pallas as pl
from jax.experimental.pallas import tpu as pltpu
from jax.sharding import PartitionSpec as P

HEAD, HEADS, D, FF = 128, 6, 768, 2048
THETA = 10000
SCALE = HEAD**-0.5
E = SCALE * 1.4426950408889634
NEG = -1e30
HIDDEN = 2 * NEG
EPS = 1e-6
QKV = D + 2 * HEAD
WA = QKV + D
GU = 2 * FF
ROWS, FROWS = D // 8, FF // 8
COARSE = 64
SPLITS = 3
PAIRS = HEADS // 2
B = 512
H = B // 2
W = 256
X, Y, CORE = 4, 2, 1
AROUND = (CORE, Y, X, X ^ Y)

BF, F32 = jnp.bfloat16, jnp.float32
VM = pltpu.VMEM
DMA = pltpu.SemaphoreType.DMA
MESH = pl.DeviceIdType.MESH
ANY = pl.BlockSpec(memory_space=pltpu.HBM)


def _place():
    return lax.axis_index("dp"), lax.axis_index("rep")


def _greet(bits):
    me, rep = _place()
    barrier = pltpu.get_barrier_semaphore()
    for bit in bits:
        pl.semaphore_signal(barrier, inc=1, device_id=(rep, me ^ bit), device_id_type=MESH)
    pl.semaphore_wait(barrier, len(bits))


class _Copy:
    def __init__(self, make):
        self.make = make

    def start(self):
        self.make().start()

    def wait(self):
        self.make().wait()

    def wait_send(self):
        self.make().wait_send()

    def wait_recv(self):
        self.make().wait_recv()


def _local(src, dst, sem):
    return _Copy(lambda: pltpu.make_async_copy(src, dst, sem))


def _remote(src, dst, sems, k, bit):
    me, rep = _place()
    return _Copy(lambda: pltpu.make_async_remote_copy(src_ref=src, dst_ref=dst, send_sem=sems.at[0, k], recv_sem=sems.at[1, k],
                                                      device_id=(rep, me ^ bit), device_id_type=MESH))


def _start(copies):
    for c in copies:
        c.start()


def _wait(copies):
    for c in copies:
        c.wait()


class _Gather:
    def __init__(self, parts, full, sems, local, own=None):
        me, _ = _place()
        rows = parts[0].shape[0]
        half = rows // 2

        def at(dev, first=0, count=rows):
            return full.at[pl.ds(pl.multiple_of(dev * rows + first, 16), count), :]

        ids = itertools.count()

        def copy(bit, dev, first=0, count=rows, src=None):
            return _remote(at(dev, first, count) if src is None else src, at(dev, first, count), sems, next(ids), bit)

        mine = at(me) if own is None else own
        self.loads, col = [], 0
        for k, part in enumerate(parts):
            width = part.shape[1]
            self.loads.append(_local(part, mine.at[:, pl.ds(col, width)], local.at[k]))
            col += width
        self.store = [] if own is None else [_local(own, at(me), local.at[4])]
        self.x, self.y, self.core = (copy(bit, me, src=mine) for bit in (X, Y, CORE))
        self.far = [copy(X, me ^ Y, count=half), copy(Y, me ^ X, half, half)]
        self.near = [copy(CORE, me ^ X), copy(CORE, me ^ Y)]
        self.end = [copy(CORE, me ^ X ^ Y, count=half), copy(CORE, me ^ X ^ Y, half, half)]

    def load(self):
        _start(self.loads)

    def start(self):
        _wait(self.loads)
        _start([self.x, self.y, self.core] + self.store)

    def forward(self):
        self.x.wait_recv()
        self.y.wait_recv()
        _start(self.far + self.near)

    def last(self):
        for c in self.far:
            c.wait_recv()
        _start(self.end)

    def finish(self):
        for c in [self.core] + self.near + self.end:
            c.wait_recv()
        for c in [self.x, self.y, self.core] + self.far + self.near + self.end:
            c.wait_send()
        _wait(self.store)


def _block(xy, other):
    me, _ = _place()
    return ((me // 2) ^ xy) * 2 + ((me % 2) ^ other)


def _blocks(full, rows, other):
    return [full.at[pl.ds(pl.multiple_of(_block(xy, other) * rows, 16), rows), :] for xy in range(4)]


class _Scatter:
    def __init__(self, keep, send, kept, came, ici, sems, local=None):
        self.kept, self.came, self.ici = kept, came, ici
        self.loads = [_local(keep[b], kept.at[b], local.at[b]) for b in range(4)] if local is not None else []
        self.keep = [kept.at[b] for b in range(4)] if self.loads else keep
        self.core = [_remote(send[b], came.at[b], sems, b, 1) for b in range(4)]
        self.out = [_remote(kept.at[b], ici.at[b - 1], sems, 3 + b, 2 * b) for b in range(1, 4)]

    def start(self):
        for b in (3, 2, 1, 0):
            _start([self.core[b]] + self.loads[b : b + 1])

    def forward(self):
        rows, step = self.came.shape[1], 16
        for b in (3, 2, 1):
            self.core[b].wait_recv()
            _wait(self.loads[b : b + 1])

            def add(i, _):
                at = pl.ds(pl.multiple_of(i * step, step), step)
                self.kept[b, at, :] = (self.keep[b][at, :].astype(F32) + self.came[b, at, :].astype(F32)).astype(BF)

            lax.fori_loop(0, rows // step, add, None)
            self.out[b - 1].start()

    def finish(self, g_ref):
        self.core[0].wait_recv()
        _wait(self.loads[:1])
        for c in self.out:
            c.wait_recv()
        rows, n = g_ref.shape
        step = 16

        def add(i, squares):
            at = pl.ds(pl.multiple_of(i * step, step), step)
            total = self.keep[0][at, :].astype(F32) + self.came[0, at, :].astype(F32)
            for b in range(3):
                total += self.ici[b, at, :].astype(F32)
            g = total.astype(BF)
            g_ref[at, :] = g
            g = g.astype(F32)
            return squares + g[:8] * g[:8] + g[8:] * g[8:]

        squares = lax.fori_loop(0, rows // step, add, jnp.zeros((8, n), F32))
        for c in self.core + self.out:
            c.wait_send()
        return sum(squares[:, c : c + HEAD] for c in range(0, n, HEAD))


def _scatter_scratch(rows, n):
    return [VM((4, rows, n), BF), VM((4, rows, n), BF), VM((3, rows, n), BF), DMA((2, 7)), DMA((4,))]


def _split_out(full, rows, keep, send, sems):
    copies = [_local(src, ref.at[b], sems.at[k, b]) for k, ref in enumerate((keep, send)) for b, src in enumerate(_blocks(full, rows, k))]
    _start(copies)
    return copies


def _dot(a, b, ca, cb):
    return lax.dot_general(a, b, (((ca,), (cb,)), ((), ())), preferred_element_type=F32)


_mm = functools.partial(_dot, ca=1, cb=0)
_mt = functools.partial(_dot, ca=1, cb=1)
_tm = functools.partial(_dot, ca=0, cb=0)


def _at(i, n):
    return pl.ds(pl.multiple_of(i * n, n), n)


def _when(cond, *todo):
    @pl.when(cond)
    def _():
        for do in todo:
            do()


def _loop(n, body):
    def step(i, _):
        body(i)

    lax.fori_loop(0, n, step, None)


def _scale(wide):
    return lax.rsqrt(jnp.mean(wide * wide, -1, keepdims=True) + EPS)


def _norm(wide):
    return (wide * _scale(wide)).astype(BF)


def _norm_back(h, dy, by):
    wide, dy = h.astype(F32), dy.astype(F32)
    scale = _scale(wide)
    back = scale * (dy - wide * (scale * scale * jnp.mean(dy * wide, -1, keepdims=True)))
    return (by.astype(F32) + back.astype(BF).astype(F32)).astype(BF)


def _turn(t, cos, sin, times=1):
    t = t.astype(F32)
    return ((t * cos + pltpu.roll(t, HEAD // 2, 1) * sin) * times).astype(BF)


def _turn_back(t, cos, sin):
    return (t * cos - pltpu.roll(t, HEAD // 2, 1) * sin).astype(BF)


def _call(body, name, args, specs, outs, out_specs, scratch, flops, talks):
    return pl.pallas_call(
        body,
        in_specs=specs,
        out_specs=out_specs,
        scratch_shapes=scratch,
        out_shape=[jax.ShapeDtypeStruct(*o) for o in outs],
        compiler_params=pltpu.CompilerParams(vmem_limit_bytes=67043328, collective_id=talks, has_side_effects=talks is not None),
        cost_estimate=pl.CostEstimate(flops=flops, transcendentals=0, bytes_accessed=flops // 1000),
        name=name,
    )(*args)


def _pairs(hi, first, steps):
    first(0, 0, 0)

    def body(u):
        j, m = lax.div(u, PAIRS), lax.rem(u, PAIRS)
        later = jnp.minimum(u + 1, hi - 1)
        first(j, 2 * m + 1, 1)
        steps(j, 2 * m, 0)
        first(lax.div(later, PAIRS), 2 * lax.rem(later, PAIRS), 0)
        steps(j, 2 * m + 1, 1)

    _loop(hi, body)


def _halves(first, steps):
    first(0, 1, 0)

    def body(m):
        first(m, 0, 1)
        steps(m, 1, 0)
        first(jnp.minimum(m + 1, PAIRS - 1), 1, 0)
        steps(m, 0, 1)

    _loop(PAIRS, body)


def _hidden(shape, later, queries):
    return lax.broadcasted_iota(jnp.int32, shape, 1 - queries) - later > lax.broadcasted_iota(jnp.int32, shape, queries)


def _flash_fwd(iq, qh, k_s, vt_s, top_s, mix_s, s_s, m_s):
    def mix(s, top, cols, start, count):
        got = []
        for r in range(0, count, W):
            p = jnp.exp2(s[r : r + W, cols] - top).astype(BF)
            got.append(_mm(vt_s[:, pl.ds(pl.multiple_of(start + r, W), W)], p))
        return sum(got)

    def score_half(m, half, slot):
        rows, keys = pl.ds(pl.multiple_of(iq * B + half * H, H), H), pl.ds(pl.multiple_of(iq * B, B), H + half * H)
        s = _mt(k_s[keys, :], jnp.concatenate([qh[2 * m, rows, :], qh[2 * m + 1, rows, :]], 0))
        hide = _hidden((H, H), 0, 1)
        for i in range(2):
            cols, last = slice(i * H, (i + 1) * H), slice(half * H, (half + 1) * H)
            t = jnp.where(hide, HIDDEN, s[last, cols])
            top = t.max(axis=0, keepdims=True)
            s_s[slot][last, cols] = t
            if half:
                s_s[slot][:H, cols] = s[:H, cols]
                top = jnp.maximum(top, s[:H, cols].max(axis=0, keepdims=True))
            m_s[slot][:, cols] = top

    def rest_half(m, half, slot):
        for i in range(2):
            cols, to = slice(i * H, (i + 1) * H), slice(half * H, (half + 1) * H)
            top = m_s[slot][:, cols]
            top_s[2 * m + i, :, to] = top
            mix_s[2 * m + i, :, to] = mix(s_s[slot], top, cols, iq * B, H + half * H)

    _halves(score_half, rest_half)

    @pl.when(iq > 0)
    def _():
        rows = _at(iq, B)

        def score(j, n, slot):
            s = _mt(k_s[_at(j, B), :], qh[n, rows, :])
            s_s[slot][:] = s
            m_s[slot][:] = s.max(axis=0, keepdims=True)

        def rest(j, n, slot):
            old = top_s[n]
            top = jnp.maximum(old, m_s[slot][:])
            top_s[n] = top
            keep = jnp.exp2(old - top)
            for c in range(0, B, W):
                cols = slice(c, c + W)
                mix_s[n, :, cols] = mix_s[n, :, cols] * keep[:, cols] + mix(s_s[slot], top[:, cols], cols, j * B, B)

        _pairs(PAIRS * iq, score, rest)


def _forward(x, near, far, *refs, layers):
    (wq, wk, wv, wo, wg, wu, wd, hm_o, q_o, k_o, v_o, o_o, la_o, s_o, r_o, hid_o, bt_o, h1_o, cos_o, sin_o, wa_o, wgu_o, wd_o,
     h, hm, w_s, wgu_s, wd_s, cos, sin, qh, k_s, v_s, vt_s, o, la, a_s, top_s, mix_s, s0, s1, m0, m1, up_s, dn_s, hid, bt_s,
     g_own, d_own, sem, out_sem, a_sem, a_loc, b_sem, b_loc, g_sem, g_loc, d_sem, d_loc) = refs
    tokens = h.shape[0]
    blocks = tokens // B
    A = lambda l: _Gather([w.at[l] for w in (wq, wk, wv)], w_s.at[l, :, pl.ds(0, QKV)], a_sem.at[l], a_loc.at[l])
    O = lambda l: _Gather([wo.at[l]], w_s.at[l, :, pl.ds(QKV, D)], b_sem.at[l], b_loc.at[l])
    G = lambda l: _Gather([wg.at[l], wu.at[l]], wgu_o.at[l], g_sem.at[l], g_loc.at[l], g_own)
    N = lambda l: _Gather([wd.at[l]], wd_o.at[l], d_sem.at[l], d_loc.at[l], d_own)

    load = _local(x, h, sem.at[0])
    load.start()
    for g in (A, O, G, N):
        g(0).load()
    _greet((CORE, Y, X))
    A(0).start()
    O(0).start()
    near_c, near_s = near[0], near[1]
    for i in range(far.shape[1]):
        far_c, far_s = far[0, i : i + 1, :], far[1, i : i + 1, :]
        rows = slice(i * COARSE, (i + 1) * COARSE)
        cos[rows, :] = far_c * near_c - far_s * near_s
        t = far_s * near_c + far_c * near_s
        sin[rows, :] = jnp.where(lax.broadcasted_iota(jnp.int32, t.shape, 1) < HEAD // 2, -t, t)
    tables = [_local(cos, cos_o, sem.at[1]), _local(sin, sin_o, sem.at[2])]
    _start(tables)
    _wait(tables)
    vt_s[HEAD:, :] = jnp.ones((8, tokens), BF)
    A(0).forward()
    G(0).start()
    load.wait()
    A(0).last()
    A(0).finish()

    def project(l, r):
        at = _at(r, B)
        a_s[:] = _norm(h[at, :].astype(F32))
        c, s = cos[at, :], sin[at, :]
        columns = lambda m: _mm(a_s[:], w_s[l, :, m * W : (m + 1) * W]).astype(BF)
        ahead = columns(0)
        for m in range(PAIRS + 1):
            t = ahead
            if m < PAIRS:
                ahead = columns(m + 1)
            left, right = t[:, :HEAD], t[:, HEAD:]
            if m < PAIRS:
                qh[2 * m, at, :] = _turn(left, c, s, E)
                qh[2 * m + 1, at, :] = _turn(right, c, s, E)
            else:
                k_s[at, :] = _turn(left, c, s)
                v_s[at, :] = right
                vt_s[:HEAD, at] = right.T

    def attend(l, iq):
        at = _at(iq, B)
        _when(iq == blocks - 1, lambda: G(l).forward(), lambda: N(l).start(), lambda: _when(l == 0, lambda: O(0).last()))
        _flash_fwd(iq, qh, k_s, vt_s, top_s, mix_s, (s0, s1), (m0, m1))
        lines = []
        for n in range(HEADS):
            total = mix_s[n, HEAD : HEAD + 1, :]
            o[at, n * HEAD : (n + 1) * HEAD] = (mix_s[n, :HEAD, :] * (1 / total)).astype(BF).T
            rest = -(top_s[n] + jnp.log2(total))
            for _ in range(SPLITS):
                part = rest.astype(BF).astype(F32)
                lines.append(part)
                rest = rest - part
        lines.append(jnp.zeros((HEAD - SPLITS * HEADS, B), F32))
        la[at, :] = jnp.concatenate(lines, 0).astype(BF).T

    def merge(l, r):
        at = _at(r, B)
        _when(r == 1, lambda: G(l).last())
        out = _mm(o[at, :], w_s[l, :, QKV:]).astype(BF)
        hm[at, :] = (h[at, :].astype(F32) + out.astype(F32)).astype(BF)

    def saved(l, r):
        at, slot = _at(r, W), lax.rem(r, 2)
        pairs = ((up_s.at[slot], s_o.at[l, at, :]), (dn_s.at[slot], r_o.at[l, at, :]), (bt_s.at[slot], bt_o.at[l, :, at]), (hid.at[at, :], hid_o.at[l, at, :]))
        return [_local(a, b, out_sem.at[slot, i]) for i, (a, b) in enumerate(pairs)]

    wide = _local(wd_o.at[0], wd_s, sem.at[1])

    def widen(l, r):
        at, slot = _at(r, W), lax.rem(r, 2)
        _when(r == 2, lambda: N(l).forward(), lambda: _when(l == 0, lambda: A(1).start(), lambda: O(1).start()))
        _when(r == 5, lambda: N(l).last())
        _when(r == 7, lambda: N(l).finish())
        _when((l == 0) & (r == 7), lambda: wide.start(), *[lambda g=g: g(1).load() for g in (G, N)])
        _when(r > 1, lambda: _wait(saved(l, r - 2)))
        b = _norm(hm[at, :].astype(F32))
        bt_s[slot] = b.T
        ahead = None
        for c in range(0, FF + W, W):
            now = ahead
            if c < FF:
                ahead = _mm(b, wgu_s[:, c : c + W]), _mm(b, wgu_s[:, FF + c : FF + c + W])
            if now is not None:
                cols = slice(c - W, c)
                gate, up = now
                sig = jax.nn.sigmoid(gate)
                silu = gate * sig
                up_s[slot, :, cols] = silu
                dn_s[slot, :, cols] = up * (sig + silu * (1 - sig))
                hid[at, cols] = (silu * up).astype(BF)
        _start(saved(l, r))

    def narrow(r):
        at = _at(r, B)
        _when(r == 0, *[lambda g=g: g(1).forward() for g in (A, O)], lambda: G(1).start())
        _when(r == blocks - 1, lambda: A(1).last(), lambda: O(1).last())
        out = _mm(hid[at, :], wd_s[:]).astype(BF)
        h[at, :] = (hm[at, :].astype(F32) + out.astype(F32)).astype(BF)

    def layer(l):
        _loop(blocks, lambda r: project(l, r))
        pairs = ((qh, q_o), (k_s, k_o), (v_s, v_o), (w_s.at[l], wa_o), (hm, hm_o), (o, o_o), (la, la_o))
        outs = [_local(a, b.at[l], sem.at[3 + i]) for i, (a, b) in enumerate(pairs)]
        _start(outs[:3])
        _when(l == 0, lambda: O(0).forward())
        _loop(blocks, lambda iq: attend(l, iq))
        _when(l == 0, lambda: O(0).finish(), *[lambda g=g: g(1).load() for g in (A, O)])
        _loop(blocks, lambda r: merge(l, r))
        G(l).finish()
        fetch = _local(wgu_o.at[l], wgu_s, sem.at[2])
        fetch.start()
        fetch.wait()
        _start(outs[3:])
        _loop(tokens // W, lambda r: widen(l, r))

        @pl.when(l == 0)
        def _():
            wide.wait()
            _loop(blocks, narrow)
            A(1).finish()
            O(1).finish()

        for n in (2, 1):
            _wait(saved(l, tokens // W - n))
        _wait(outs)
        _when(l == 0, lambda: _start([_local(h, h1_o, sem.at[0])]))

    _loop(layers, layer)
    _wait([_local(h, h1_o, sem.at[0])])


def forward(x, weights):
    T, layers = x.shape[0], weights[0].shape[0]
    tables = rotary_tables(T)
    L = lambda *s, t=BF: ((layers, *s), t)
    outs = [L(T, D), L(HEADS, T, HEAD), L(T, HEAD), L(T, HEAD), L(T, D), L(T, HEAD), L(T, FF, t=F32), L(T, FF, t=F32), L(T, FF), L(D, T),
            ((T, D), BF), ((T, HEAD), F32), ((T, HEAD), F32), L(D, WA), L(D, GU), L(FF, D)]
    line = VM((1, B), F32)
    scratch = [VM((T, D), BF), VM((T, D), BF), VM((layers, D, WA), BF), VM((D, GU), BF), VM((FF, D), BF), VM((T, HEAD), F32), VM((T, HEAD), F32),
               VM((HEADS, T, HEAD), BF), VM((T, HEAD), BF), VM((T, HEAD), BF), VM((HEAD + 8, T), BF), VM((T, D), BF), VM((T, HEAD), BF), VM((B, D), BF),
               VM((HEADS, 1, B), F32), VM((HEADS, HEAD + 8, B), F32), VM((B, B), F32), VM((B, B), F32), line, line, VM((2, W, FF), F32), VM((2, W, FF), F32), VM((T, FF), BF), VM((2, D, W), BF),
               VM((ROWS, GU), BF), VM((FROWS, D), BF), DMA((10,)), DMA((2, 4))] + [DMA((layers, 2, 9)), DMA((layers, 5))] * 4
    small = pl.BlockSpec(memory_space=VM)
    return _call(functools.partial(_forward, layers=layers), "forward", [x, *tables, *weights], [ANY, small, small] + [ANY] * 7, outs,
                 [ANY] * len(outs), scratch, 10**11, 0)


def _mlp_back(*refs, layer, carries):
    hm_i, dy_i, s_i, r_i, hid_i, bt_i, wgu_i, wd_i, *refs = refs
    if carries:
        keep, send, dhm_o, kgu, sgu, kd, sd, g_o, sq_o, *refs = refs
    else:
        dhm_o, kgu, sgu, kd, sd, *refs = refs
    hm, dy, up_s, dn_s, hid_s, wgu, wd, g0, g1, bt, dyt, db, sem, part_sem, split_sem, *scatter = refs
    tokens = hm.shape[0]
    blocks, parts = tokens // B, FF // W
    pending = lambda: _Scatter([keep.at[b] for b in range(4)], [send.at[b] for b in range(4)], *scatter)

    def early(c):
        slot, cols = lax.rem(c, 2), _at(c, W)
        pairs = ((wd_i.at[layer, cols, :], wd.at[cols, :]), (r_i.at[layer, :, cols], dn_s.at[slot]), (s_i.at[layer, :, cols], up_s.at[slot]))
        return [_local(a, b, part_sem.at[slot, i]) for i, (a, b) in enumerate(pairs)]

    def rest(c):
        slot, cols, up = lax.rem(c, 2), _at(c, W), pl.ds(pl.multiple_of(FF + c * W, W), W)
        pairs = ((hid_i.at[layer, :, cols], hid_s.at[slot]), (wgu_i.at[layer, :, cols], wgu.at[:, cols]), (wgu_i.at[layer, :, up], wgu.at[:, up]))
        return [_local(a, b, part_sem.at[slot, 3 + i]) for i, (a, b) in enumerate(pairs)]

    dys = [_local(dy_i.at[_at(r, B), :], dy.at[_at(r, B), :], sem.at[r]) for r in range(blocks)]
    flip = _local(bt_i.at[layer], bt, sem.at[4])
    late = _local(hm_i.at[layer], hm, sem.at[5])
    _start(dys[:1] + early(0) + dys[1:] + [flip] + rest(0) + early(1) + [late])
    if carries:
        _greet(AROUND)
        pending().start()
    db[:] = jnp.zeros(db.shape, F32)

    def widen(c, slot, r, g):
        rows = slice(r * B, (r + 1) * B)
        t = _mt(dy[rows, :], wd[_at(c, W), :]).astype(BF).astype(F32)
        g[rows, :W] = (t * dn_s[slot, rows, :]).astype(BF)
        g[rows, W:] = (t * up_s[slot, rows, :]).astype(BF)

    for r in range(blocks):
        dys[r].wait()
        if r == 0:
            _wait(early(0))
        dyt[:, r * B : (r + 1) * B] = dy[r * B : (r + 1) * B, :].T
        widen(0, 0, r, g0)
    flip.wait()

    def step(c, slot, g, later):
        cols, up = _at(c, W), pl.ds(pl.multiple_of(FF + c * W, W), W)
        after = jnp.minimum(c + 1, parts - 1)
        _when(c + 2 < parts, lambda: _start(early(c + 2)))
        _when(c + 1 < parts, lambda: _start(rest(c + 1)), lambda: _wait(early(c + 1)))
        _wait(rest(c))
        for r in range(blocks):
            widen(after, 1 - slot, r, later)
        both = jnp.concatenate([wgu[:, cols], wgu[:, up]], 1)
        for r in range(blocks):
            rows = slice(r * B, (r + 1) * B)
            db[rows, :] += _mt(g[rows, :], both)
        dw = _mm(bt[:], g[:]).astype(BF)
        wgu[:, cols] = dw[:, :W]
        wgu[:, up] = dw[:, W:]
        wd[cols, :] = _mm(dyt[:], hid_s[slot]).astype(BF).T
        if carries:
            _when(c == 1, lambda: pending().forward())

    def two(u):
        step(2 * u, 0, g0, g1)
        step(2 * u + 1, 1, g1, g0)

    _loop(parts // 2, two)
    copies = _split_out(wgu, ROWS, kgu, sgu, split_sem.at[0]) + _split_out(wd, FROWS, kd, sd, split_sem.at[1])
    late.wait()
    out = lambda r: _local(hm.at[_at(r, B), :], dhm_o.at[_at(r, B), :], sem.at[r])

    def back(r):
        at = _at(r, B)
        hm[at, :] = _norm_back(hm[at, :], db[at, :].astype(BF), dy[at, :])
        out(r).start()

    _loop(blocks, back)
    if carries:
        sq_o[:] = pending().finish(g_o)
    _wait(copies + [out(r) for r in range(blocks)])


WHOLE = pl.BlockSpec(memory_space=VM)


def mlp_back(saved, dy, layer, pending, talks):
    T = dy.shape[0]
    carries = pending is not None
    gu, d = ((4, ROWS, GU), BF), ((4, FROWS, D), BF)
    args = [saved[n] for n in ("hm", "s", "r", "hid", "bt", "wgu", "wd")]
    args.insert(1, dy)
    scratch = [VM((T, D), BF), VM((T, D), BF), VM((2, T, W), F32), VM((2, T, W), F32), VM((2, T, W), BF), VM((D, GU), BF), VM((FF, D), BF),
               VM((T, 2 * W), BF), VM((T, 2 * W), BF), VM((D, T), BF), VM((D, T), BF), VM((T, D), F32), DMA((6,)), DMA((2, 6)), DMA((2, 2, 4))]
    outs, out_specs = [((T, D), BF), gu, gu, d, d], [ANY] * 5
    if carries:
        args += pending
        outs += [((ROWS, WA), BF), ((8, HEAD), F32)]
        out_specs += [WHOLE, WHOLE]
        scratch += _scatter_scratch(ROWS, WA)
    return _call(functools.partial(_mlp_back, layer=layer, carries=carries), "mlp_back", args, [ANY] * len(args), outs, out_specs, scratch,
                 4 * 10**10, talks)


def _flash_back(iq, qh, qt, doh, dot, la, dl, zs, k_s, v_s, dq, dkt, dvt, p_s, x_s):
    def give(slot, count, s, d, edge=B):
        for e in range(0, count, HEAD):
            cols = slice(e, e + HEAD)
            for r in range(0, B, H):
                rows = slice(r, r + H)
                p = jnp.exp2(s[rows, cols])
                if e >= edge:
                    p = jnp.where(_hidden(p.shape, edge - e, 0), 0.0, p)
                p_s[slot][rows, cols] = p.astype(BF)
                x_s[slot][rows, cols] = (p * d[rows, cols]).astype(BF)

    def weigh_half(m, half, slot):
        rows, keys = pl.ds(pl.multiple_of(iq * B + half * H, H), H), pl.ds(pl.multiple_of(iq * B, B), H + half * H)
        pair = (2 * m, 2 * m + 1)
        q = jnp.concatenate([jnp.concatenate([qh[n, rows, :], la[rows, :] * zs[n, :H, :]], 1) for n in pair], 0)
        do = jnp.concatenate([jnp.concatenate([doh[n, rows, :], dl[rows, :] * zs[n, :H, :]], 1) for n in pair], 0)
        z = zs[HEADS, : H + half * H, :]
        s = _mt(q, jnp.concatenate([k_s[keys, :], z], 1))
        d = _mt(do, jnp.concatenate([v_s[keys, :], z], 1))
        give(slot, H + half * H, s, d, half * H)

    def rest_half(m, half, slot):
        rows, keys = pl.ds(pl.multiple_of(iq * B + half * H, H), H), pl.ds(pl.multiple_of(iq * B, B), H + half * H)
        pair = (2 * m, 2 * m + 1)
        p, x = p_s[slot][:, : H + half * H], x_s[slot][:, : H + half * H]
        dvt[:, keys] += _mm(jnp.concatenate([dot[n, :, rows] for n in pair], 1), p)
        dkt[:, keys] += _mm(jnp.concatenate([qt[n, :, rows] for n in pair], 1), x)
        g = _mm(x, k_s[keys, :])
        for i, n in enumerate(pair):
            dq[n, half * H : (half + 1) * H, :] = g[i * H : (i + 1) * H, :]

    _halves(weigh_half, rest_half)

    @pl.when(iq > 0)
    def _():
        rows = _at(iq, B)

        def weigh(j, n, slot):
            keys = _at(j, B)
            s = _mt(jnp.concatenate([qh[n, rows, :], la[rows, :]], 1), jnp.concatenate([k_s[keys, :], zs[n]], 1))
            d = _mt(jnp.concatenate([doh[n, rows, :], dl[rows, :]], 1), jnp.concatenate([v_s[keys, :], zs[n]], 1))
            give(slot, B, s, d)

        def rest(j, n, slot):
            keys = _at(j, B)
            dvt[:, keys] += _mm(dot[n, :, rows], p_s[slot][:])
            dkt[:, keys] += _mm(qt[n, :, rows], x_s[slot][:])
            dq[n] += _mm(x_s[slot][:], k_s[keys, :])

        _pairs(PAIRS * iq, weigh, rest)


def _attn_back(*refs, layer, count):
    first = layer == 0
    dhm_i, h_i, q_i, k_i, v_i, o_i, la_i, cos_i, sin_i, wa_i, kgu, sgu, kd, sd, *refs = refs
    if first:
        sq_a, sq_b, ggu_o, gd_o, ga_o, factor_o, *refs = refs
    else:
        ggu_o, gd_o, sq_o, dh_o, keep_o, send_o, *refs = refs
    (dhm, h, qh, k_s, v_s, o, la, cos, sin, wa, doh, dqkv, a_s, qt, dot, dl, zs, dq, dkt, dvt, p0, p1, x0, x1, dn_s, sem, split_sem, *refs) = refs
    scatter_gu, scatter_d, refs = refs[:5], refs[5:10], refs[10:]
    tokens = h.shape[0]
    blocks = tokens // B
    pending = lambda: [_Scatter([a.at[b] for b in range(4)], [c.at[b] for b in range(4)], *s) for a, c, s in ((kgu, sgu, scatter_gu), (kd, sd, scatter_d))]

    def piece(i, a, b):
        return _local(a, b, sem.at[i])

    wo = piece(0, wa_i.at[layer, :, pl.ds(QKV, D)], wa.at[:, pl.ds(QKV, D)])
    groups = []
    for r in range(blocks):
        at = _at(r, B)
        pairs = ((dhm_i.at[at, :], dhm.at[at, :]), (q_i.at[layer, :, at, :], qh.at[:, at, :]), (o_i.at[layer, at, :], o.at[at, :]))
        groups.append([piece(1 + 3 * r + i, a, b) for i, (a, b) in enumerate(pairs)])
    pairs = ((la_i.at[layer], la), (k_i.at[layer], k_s), (v_i.at[layer], v_s), (h_i, h), (cos_i, cos), (sin_i, sin),
             (wa_i.at[layer, :, pl.ds(0, QKV)], wa.at[:, pl.ds(0, QKV)]))
    late = [piece(1 + 3 * blocks + i, a, b) for i, (a, b) in enumerate(pairs)]
    _start([wo] + sum(groups, []) + late)
    _greet(range(1, 8) if first else AROUND)
    for s in pending():
        s.start()
    dkt[:] = jnp.zeros(dkt.shape, F32)
    dvt[:] = jnp.zeros(dvt.shape, F32)
    lane = lax.broadcasted_iota(jnp.int32, (B, HEAD), 1)
    for n in range(HEADS):
        zs[n] = ((lane >= SPLITS * n) & (lane < SPLITS * (n + 1))).astype(F32).astype(BF)
    zs[HEADS] = (lane < SPLITS * HEADS).astype(F32).astype(BF)
    wo.wait()

    def lead(r):
        at = _at(r, B)
        columns = lambda m: _mt(dhm[at, :], wa[m * W : (m + 1) * W, QKV:]).astype(BF)
        ahead = columns(0)
        means = jnp.zeros(lane.shape, F32)
        for n in range(HEADS):
            if n % 2 == 0:
                do = ahead
                if n + 2 < HEADS:
                    ahead = columns(n // 2 + 1)
            by = do[:, n % 2 * HEAD : (n % 2 + 1) * HEAD]
            doh[n, at, :] = by
            dot[n, :, at] = by.T
            qt[n, :, at] = qh[n, at, :].T
            rest = -jnp.sum(by.astype(F32) * o[at, n * HEAD : (n + 1) * HEAD].astype(F32), -1, keepdims=True)
            for i in range(SPLITS):
                part = rest.astype(BF).astype(F32)
                means = jnp.where(lane == SPLITS * n + i, part, means)
                rest = rest - part
        dl[at, :] = means.astype(BF)

    def begin(r):
        for k in range(blocks):
            _when(r == k, lambda: _wait(groups[k]))
        lead(r)

    _loop(blocks, begin)
    wa[:, QKV:] = _tm(o[:], dhm[:]).astype(BF)
    if first:
        own = [_Scatter(*[_blocks(wa.at[:, cols], ROWS, k) for k in range(2)], *s) for cols, s in
               ((pl.ds(QKV, D), refs[:4]), (pl.ds(0, QKV), [scatter_gu[0].at[:, :, pl.ds(0, QKV)], *refs[4:7]]))]
        own[0].start()
    _wait(late)
    for s in pending():
        s.forward()

    def attend(g):
        iq = blocks - 1 - g
        at = _at(iq, B)
        if first:
            _when(g == 1, lambda: own[0].forward())
        _flash_back(iq, qh, qt, doh, dot, la, dl, zs, k_s, v_s, dq, dkt, dvt, (p0, p1), (x0, x1))
        c, s = cos[at, :], sin[at, :]
        _loop(HEADS, lambda n: dqkv.__setitem__((at, _at(n, HEAD)), _turn_back(dq[n] * SCALE, c, s)))
        dqkv[at, D : D + HEAD] = _turn_back((dkt[:, at] * (SCALE / E)).T, c, s)
        dqkv[at, D + HEAD :] = dvt[:, at].T.astype(BF)
        a_s[at, :] = _norm(h[at, :].astype(F32))

    _loop(blocks, attend)
    dw = lambda: wa.__setitem__((slice(None), slice(0, QKV)), _tm(a_s[:], dqkv[:]).astype(BF))
    if first:
        dw()
        mine, all_s, all_sem = refs[7:]
        own[1].start()
        gu, d = pending()
        squares = gu.finish(ggu_o) + d.finish(gd_o) + sq_a[:] + sq_b[:]
        own[1].forward()
        squares += own[0].finish(ga_o.at[:, pl.ds(QKV, D)])
        mine[:] = own[1].finish(ga_o.at[:, pl.ds(0, QKV)]) + squares
        me, _ = _place()
        copies = [_remote(mine, all_s.at[me], all_sem, r, r) for r in range(1, 8)]
        _start(copies)
        all_s[me] = mine[:]
        _wait(copies)
        total = jnp.sum(jnp.sum(jnp.sum(all_s[:], axis=0), axis=1, keepdims=True), axis=0, keepdims=True)
        factor_o[:] = jnp.broadcast_to(jnp.minimum(1.0, 0.5 * lax.rsqrt(total / count + 1e-30)), factor_o.shape)
    else:
        out = lambda r: _local(h.at[_at(r, B), :], dh_o.at[_at(r, B), :], split_sem.at[2, r])

        def back(r):
            at = _at(r, B)
            dn_s[:] = _mt(dqkv[at, :], wa[:, :QKV]).astype(BF)
            h[at, :] = _norm_back(h[at, :], dn_s[:], dhm[at, :])
            out(r).start()

        _loop(blocks, back)
        dw()
        copies = _split_out(wa, ROWS, keep_o, send_o, split_sem)
        gu, d = pending()
        sq_o[:] = gu.finish(ggu_o) + d.finish(gd_o)
        _wait(copies + [out(r) for r in range(blocks)])


def attn_back(saved, dhm, h, layer, pending, squares, count, talks):
    T = h.shape[0]
    args = [dhm, h] + [saved[n] for n in ("q", "k", "v", "o", "la", "cos", "sin", "wa")] + [*pending, *squares]
    specs = [ANY] * (10 + len(pending)) + [WHOLE] * len(squares)
    dw, small = ((4, ROWS, WA), BF), ((8, HEAD), F32)
    outs, out_specs = [((ROWS, GU), BF), ((FROWS, D), BF)], [WHOLE, WHOLE]
    tile = VM((B, B), BF)
    scratch = [VM((T, D), BF), VM((T, D), BF), VM((HEADS, T, HEAD), BF), VM((T, HEAD), BF), VM((T, HEAD), BF), VM((T, D), BF), VM((T, HEAD), BF),
               VM((T, HEAD), F32), VM((T, HEAD), F32), VM((D, WA), BF), VM((HEADS, T, HEAD), BF), VM((T, QKV), BF), VM((T, D), BF),
               VM((HEADS, HEAD, T), BF), VM((HEADS, HEAD, T), BF), VM((T, HEAD), BF), VM((HEADS + 1, B, HEAD), BF), VM((HEADS, B, HEAD), F32),
               VM((HEAD, T), F32), VM((HEAD, T), F32), tile, tile, tile, tile, VM((B, D), BF), DMA((20,)), DMA((3, 4)),
               *_scatter_scratch(ROWS, GU), *_scatter_scratch(FROWS, D)]
    if layer == 0:
        outs += [((ROWS, WA), BF), small]
        out_specs += [WHOLE, WHOLE]
        scratch += [VM((4, ROWS, D), BF)]
        for width in (D, QKV):
            scratch += [VM((4, ROWS, width), BF), VM((3, ROWS, width), BF), DMA((2, 7))]
        scratch += [VM((8, HEAD), F32), VM((8, 8, HEAD), F32), DMA((2, 8))]
    else:
        outs += [small, ((T, D), BF), dw, dw]
        out_specs += [WHOLE, ANY, ANY, ANY]
    return _call(functools.partial(_attn_back, layer=layer, count=count), "attn_back", args, specs, outs, out_specs, scratch, 5 * 10**10, talks)


def _adamw(*refs, layers):
    factor_ref, *refs = refs
    groups = [list(itertools.islice(refs, i, i + n)) for i, n in ((0, 3 * layers), (3 * layers, 21), (3 * layers + 21, 21), (3 * layers + 42, 21))]
    grads, given, out, held = groups
    g_held, load_sem, grad_sem, store_sem = refs[3 * layers + 63 :][: 3 * layers], *refs[-3:]
    factor = factor_ref[:1, :1]
    where = [(which, sum(widths[:i]), width) for which, widths in enumerate(((D, HEAD, HEAD, D), (FF, FF), (D,))) for i, width in enumerate(widths)]
    fetch = [_local(a, b, grad_sem.at[i]) for i, (a, b) in enumerate(zip(grads, g_held))]

    def moves(layer, i):
        trio = range(i, 21, 7)
        return ([_local(given[k].at[layer], held[k].at[layer], load_sem.at[layer, k]) for k in trio],
                [_local(held[k].at[layer], out[k].at[layer], store_sem.at[layer, k]) for k in trio])

    every = [(layer, i) for layer in range(layers) for i in range(7)]
    for layer, i in every:
        if where[i][1] == 0:
            fetch[3 * layer + where[i][0]].start()
        _start(moves(layer, i)[0])
    for layer, i in every:
        which, start, width = where[i]
        if start == 0:
            fetch[3 * layer + which].wait()
        loads, stores = moves(layer, i)
        _wait(loads)
        w_ref, m_ref, v_ref = (held[k].at[layer] for k in range(i, 21, 7))
        g_ref = g_held[3 * layer + which]

        def step(r):
            at = _at(r, 16)
            g = g_ref[at, start : start + width].astype(F32) * factor
            m = 0.9 * m_ref[at, :] + 0.1 * g
            v = 0.95 * v_ref[at, :] + 0.05 * g * g
            w = w_ref[at, :].astype(F32)
            w_ref[at, :] = (w - 0.02 * (m * lax.rsqrt(v + 1e-8) + 0.1 * w)).astype(BF)
            m_ref[at, :] = m
            v_ref[at, :] = v

        _loop(g_ref.shape[0] // 16, step)
        _start(stores)
    for layer, i in every:
        _wait(moves(layer, i)[1])


def adamw(factor, grads, weights, m, v):
    layers = len(grads)
    flat, given = sum(grads, []), [*weights, *m, *v]
    whole = lambda a: VM(a.shape, a.dtype)
    return _call(functools.partial(_adamw, layers=layers), "adamw", [factor, *flat, *given], [WHOLE] + [ANY] * (len(flat) + len(given)),
                 [(a.shape, a.dtype) for a in given], [ANY] * len(given),
                 [whole(a) for a in given + flat] + [DMA((layers, 21)), DMA((len(flat),)), DMA((layers, 21))], 10**9, None)


def rotary_tables(tokens):
    half = HEAD // 2
    rate = THETA ** (-np.arange(half, dtype=np.float64) / half)

    def table(places):
        angle = np.concatenate([places[:, None] * rate] * 2, 1)
        return jnp.asarray(np.stack([np.cos(angle), np.sin(angle)]), F32)

    return table(np.arange(COARSE)), table(np.arange(0, tokens, COARSE))


def solution(mesh):
    def step(x, dy, *arrays):
        weights, m, v = (arrays[i : i + 7] for i in (0, 7, 14))
        x, dy = x[0], dy[0]
        names = ("hm", "q", "k", "v", "o", "la", "s", "r", "hid", "bt", "h1", "cos", "sin", "wa", "wgu", "wd")
        saved = dict(zip(names, forward(x, weights)))
        count = 8 * sum(w.size for w in weights)
        by_hm, *mlp1 = mlp_back(saved, dy, 1, None, None)
        ggu1, gd1, sq_a, by_h, *attn1 = attn_back(saved, by_hm, saved["h1"], 1, mlp1, [], count, 1)
        by_hm, *mlp0, ga1, sq_b = mlp_back(saved, by_h, 0, attn1, 2)
        ggu0, gd0, ga0, factor = attn_back(saved, by_hm, x, 0, mlp0, [sq_a, sq_b], count, 3)
        return tuple(adamw(factor, [[ga0, ggu0, gd0], [ga1, ggu1, gd1]], weights, m, v))

    states, cut = P(("rep", "dp"), None, None), P(None, "dp", None)
    return jax.shard_map(
        step,
        mesh=mesh,
        in_specs=(states, states) + (cut,) * 21,
        out_specs=(P("rep", "dp", None),) * 21,
        check_vma=False,
    )
```

```python
import functools
import itertools

import jax
import jax.numpy as jnp
import numpy as np
from jax import lax
from jax.experimental import pallas as pl
from jax.experimental.pallas import tpu as pltpu
from jax.sharding import PartitionSpec as P

HEAD, HEADS, D, FF = 128, 6, 768, 2048
THETA = 10000
SCALE = HEAD**-0.5
E = SCALE * 1.4426950408889634
NEG = -1e30
HIDDEN = 2 * NEG
EPS = 1e-6
QKV = D + 2 * HEAD
WA = QKV + D
GU = 2 * FF
ROWS, FROWS = D // 8, FF // 8
COARSE = 64
SPLITS = 3
PAIRS = HEADS // 2
B = 512
H = B // 2
STEP = 16
W = 256
FIRST, LAST = range(2)
HALF = FF // 2
X, Y, CORE = 4, 2, 1
AROUND = (CORE, Y, X, X ^ Y)

BF, F32 = jnp.bfloat16, jnp.float32
VM = pltpu.VMEM
DMA = pltpu.SemaphoreType.DMA
MESH = pl.DeviceIdType.MESH
ANY = pl.BlockSpec(memory_space=pltpu.HBM)


def _place():
    return lax.axis_index("dp"), lax.axis_index("rep")


def _greet(bits):
    me, rep = _place()
    barrier = pltpu.get_barrier_semaphore()
    for bit in bits:
        pl.semaphore_signal(barrier, inc=1, device_id=(rep, me ^ bit), device_id_type=MESH)
    pl.semaphore_wait(barrier, len(bits))


class _Copy:
    def __init__(self, make):
        self.make = make

    def start(self):
        self.make().start()

    def wait(self):
        self.make().wait()

    def wait_send(self):
        self.make().wait_send()

    def wait_recv(self):
        self.make().wait_recv()


def _local(src, dst, sem):
    return _Copy(lambda: pltpu.make_async_copy(src, dst, sem))


def _remote(src, dst, sems, k, bit):
    me, rep = _place()
    return _Copy(lambda: pltpu.make_async_remote_copy(src_ref=src, dst_ref=dst, send_sem=sems.at[0, k], recv_sem=sems.at[1, k],
                                                      device_id=(rep, me ^ bit), device_id_type=MESH))


def _start(copies):
    for c in copies:
        c.start()


def _wait(copies):
    for c in copies:
        c.wait()


class _Gather:
    def __init__(self, parts, full, sems, local, own=None):
        me, _ = _place()
        rows = parts[0].shape[0]
        half = rows // 2

        def at(dev, first=0, count=rows):
            return full.at[pl.ds(pl.multiple_of(dev * rows + first, 16), count), :]

        ids = itertools.count()

        def copy(bit, dev, first=0, count=rows, src=None):
            return _remote(at(dev, first, count) if src is None else src, at(dev, first, count), sems, next(ids), bit)

        mine = at(me) if own is None else own
        self.loads, col = [], 0
        for k, part in enumerate(parts):
            width = part.shape[1]
            self.loads.append(_local(part, mine.at[:, pl.ds(col, width)], local.at[k]))
            col += width
        self.store = [] if own is None else [_local(own, at(me), local.at[4])]
        self.x, self.y, self.core = (copy(bit, me, src=mine) for bit in (X, Y, CORE))
        self.far = [copy(X, me ^ Y, count=half), copy(Y, me ^ X, half, half)]
        self.near = [copy(CORE, me ^ X), copy(CORE, me ^ Y)]
        self.end = [copy(CORE, me ^ X ^ Y, count=half), copy(CORE, me ^ X ^ Y, half, half)]

    def load(self):
        _start(self.loads)

    def start(self):
        _wait(self.loads)
        _start([self.x, self.y, self.core] + self.store)

    def forward(self):
        self.x.wait_recv()
        self.y.wait_recv()
        _start(self.far + self.near)

    def last(self):
        for c in self.far:
            c.wait_recv()
        _start(self.end)

    def early(self):
        for c in [self.core] + self.near:
            c.wait_recv()
        _wait(self.store)

    def late(self):
        for c in self.end:
            c.wait_recv()
        for c in [self.x, self.y, self.core] + self.far + self.near + self.end:
            c.wait_send()

    def finish(self):
        self.early()
        self.late()


def _block(xy, other):
    me, _ = _place()
    return ((me // 2) ^ xy) * 2 + ((me % 2) ^ other)


def _blocks(full, rows, other):
    return [full.at[pl.ds(pl.multiple_of(_block(xy, other) * rows, 16), rows), :] for xy in range(4)]


class _Scatter:
    def __init__(self, keep, send, kept, came, ici, sems, local=None):
        self.kept, self.came, self.ici = kept, came, ici
        self.loads = [_local(keep[b], kept.at[b], local.at[b]) for b in range(4)] if local is not None else []
        self.keep = [kept.at[b] for b in range(4)] if self.loads else keep
        ids = itertools.count()
        self.core = [_remote(send[b], came.at[b], sems, next(ids), CORE) for b in range(4)]
        half = came.shape[1] // 2
        self.ways = ((pl.ds(0, half), X, 2, Y, 1), (pl.ds(half, half), Y, 1, X, 2))
        self.first = [_remote(kept.at[b, at, :], ici.at[k, at, :], sems, next(ids), bit) for at, bit, near, _, _ in self.ways for k, b in enumerate((near, 3))]
        self.second = [_remote(kept.at[b, at, :], ici.at[2, at, :], sems, next(ids), bit) for at, _, _, bit, b in self.ways]

    def start(self):
        for b in (3, 2, 1, 0):
            _start([self.core[b]] + self.loads[b : b + 1])

    def _add(self, out, start, rows, *terms):
        def add(i):
            at = pl.ds(pl.multiple_of(start + i * STEP, STEP), STEP)
            out[at, :] = sum(t[at, :].astype(F32) for t in terms).astype(BF)

        _loop(rows // STEP, add)

    def forward(self):
        for b in (3, 2, 1):
            self.core[b].wait_recv()
            _wait(self.loads[b : b + 1])
            self._add(self.kept.at[b], 0, self.came.shape[1], self.keep[b], self.came.at[b])
        _start(self.first)

    def pass_on(self):
        half = self.came.shape[1] // 2
        for i, way in enumerate(self.ways):
            self.first[2 * i + 1].wait_recv()
            self._add(self.kept.at[way[-1]], i * half, half, self.kept.at[way[-1]], self.ici.at[1])
            self.second[i].start()

    def finish(self, g_ref):
        self.core[0].wait_recv()
        _wait(self.loads[:1])
        for c in self.first[::2] + self.second:
            c.wait_recv()
        self._add(g_ref, 0, g_ref.shape[0], self.keep[0], self.came.at[0], self.ici.at[0], self.ici.at[2])

        def square(i, squares):
            g = g_ref[_at(i, STEP), :].astype(F32)
            return squares + g[:8] * g[:8] + g[8:] * g[8:]

        squares = lax.fori_loop(0, g_ref.shape[0] // STEP, square, jnp.zeros((8, g_ref.shape[1]), F32))
        for c in self.core + self.first + self.second:
            c.wait_send()
        return sum(squares[:, c : c + HEAD] for c in range(0, g_ref.shape[1], HEAD))


def _scatter_scratch(rows, n):
    return [VM((4, rows, n), BF), VM((4, rows, n), BF), VM((3, rows, n), BF), DMA((2, 10)), DMA((4,))]


def _split_out(full, rows, keep, send, sems):
    copies = [_local(src, ref.at[b], sems.at[k, b]) for k, ref in enumerate((keep, send)) for b, src in enumerate(_blocks(full, rows, k))]
    _start(copies)
    return copies


def _dot(a, b, ca, cb):
    return lax.dot_general(a, b, (((ca,), (cb,)), ((), ())), preferred_element_type=F32)


_mm = functools.partial(_dot, ca=1, cb=0)
_mt = functools.partial(_dot, ca=1, cb=1)
_tm = functools.partial(_dot, ca=0, cb=0)


def _at(i, n):
    return pl.ds(pl.multiple_of(i * n, n), n)


def _when(cond, *todo):
    @pl.when(cond)
    def _():
        for do in todo:
            do()


def _loop(n, body):
    def step(i, _):
        body(i)

    lax.fori_loop(0, n, step, None)


def _scale(wide):
    return lax.rsqrt(jnp.mean(wide * wide, -1, keepdims=True) + EPS)


def _norm_to(out, to, h, at):
    wide = h[at, :].astype(F32)
    out[to, :] = (wide * _scale(wide)).astype(BF)


def _norm_back(h, dy, by):
    wide, dy = h.astype(F32), dy.astype(F32)
    scale = _scale(wide)
    back = scale * (dy - wide * (scale * scale * jnp.mean(dy * wide, -1, keepdims=True)))
    return (by.astype(F32) + back.astype(BF).astype(F32)).astype(BF)


def _turn(t, cos, sin, times=1):
    t = t.astype(F32)
    return ((t * cos + pltpu.roll(t, HEAD // 2, 1) * sin) * times).astype(BF)


def _turn_back(t, cos, sin):
    return (t * cos - pltpu.roll(t, HEAD // 2, 1) * sin).astype(BF)


def _call(body, name, args, specs, outs, out_specs, scratch, flops, talks):
    return pl.pallas_call(
        body,
        in_specs=specs,
        out_specs=out_specs,
        scratch_shapes=scratch,
        out_shape=[jax.ShapeDtypeStruct(*o) for o in outs],
        compiler_params=pltpu.CompilerParams(vmem_limit_bytes=67043328, collective_id=talks, has_side_effects=talks is not None),
        cost_estimate=pl.CostEstimate(flops=flops, transcendentals=0, bytes_accessed=flops // 1000),
        name=name,
    )(*args)


def _pairs(hi, first, steps):
    first(0, 0, 0)

    def body(u):
        j, m = lax.div(u, PAIRS), lax.rem(u, PAIRS)
        later = jnp.minimum(u + 1, hi - 1)
        first(j, 2 * m + 1, 1)
        steps(j, 2 * m, 0)
        first(lax.div(later, PAIRS), 2 * lax.rem(later, PAIRS), 0)
        steps(j, 2 * m + 1, 1)

    _loop(hi, body)


def _halves(first, steps):
    first(0, 1, 0)

    def body(m):
        first(m, 0, 1)
        steps(m, 1, 0)
        first(jnp.minimum(m + 1, PAIRS - 1), 1, 0)
        steps(m, 0, 1)

    _loop(PAIRS, body)


def _hidden(shape, later, queries):
    return lax.broadcasted_iota(jnp.int32, shape, 1 - queries) - later > lax.broadcasted_iota(jnp.int32, shape, queries)


def _flash_fwd(iq, qh, k_s, vt_s, top_s, mix_s, s_s, m_s):
    def mix(s, top, cols, start, count):
        got = []
        for r in range(0, count, W):
            p = jnp.exp2(s[r : r + W, cols] - top).astype(BF)
            got.append(_mm(vt_s[:, pl.ds(pl.multiple_of(start + r, W), W)], p))
        return sum(got)

    def score_half(m, half, slot):
        rows, keys = pl.ds(pl.multiple_of(iq * B + half * H, H), H), pl.ds(pl.multiple_of(iq * B, B), H + half * H)
        s = _mt(k_s[keys, :], jnp.concatenate([qh[2 * m, rows, :], qh[2 * m + 1, rows, :]], 0))
        hide = _hidden((H, H), 0, 1)
        for i in range(2):
            cols, last = slice(i * H, (i + 1) * H), slice(half * H, (half + 1) * H)
            t = jnp.where(hide, HIDDEN, s[last, cols])
            top = t.max(axis=0, keepdims=True)
            s_s[slot][last, cols] = t
            if half:
                s_s[slot][:H, cols] = s[:H, cols]
                top = jnp.maximum(top, s[:H, cols].max(axis=0, keepdims=True))
            m_s[slot][:, cols] = top

    def rest_half(m, half, slot):
        for i in range(2):
            cols, to = slice(i * H, (i + 1) * H), slice(half * H, (half + 1) * H)
            top = m_s[slot][:, cols]
            top_s[2 * m + i, :, to] = top
            mix_s[2 * m + i, :, to] = mix(s_s[slot], top, cols, iq * B, H + half * H)

    _halves(score_half, rest_half)

    @pl.when(iq > 0)
    def _():
        rows = _at(iq, B)

        def score(j, n, slot):
            s = _mt(k_s[_at(j, B), :], qh[n, rows, :])
            s_s[slot][:] = s
            m_s[slot][:] = s.max(axis=0, keepdims=True)

        def rest(j, n, slot):
            old = top_s[n]
            top = jnp.maximum(old, m_s[slot][:])
            top_s[n] = top
            keep = jnp.exp2(old - top)
            for c in range(0, B, W):
                cols = slice(c, c + W)
                mix_s[n, :, cols] = mix_s[n, :, cols] * keep[:, cols] + mix(s_s[slot], top[:, cols], cols, j * B, B)

        _pairs(PAIRS * iq, score, rest)


def _forward(x, near, far, *refs, layers):
    (wq, wk, wv, wo, wg, wu, wd, hm_o, q_o, k_o, v_o, o_o, la_o, s_o, r_o, hid_o, bt_o, h1_o, cos_o, sin_o, wa_o, wgu_o, wd_o,
     h, hm, w_s, wgu_s, wd_s, cos, sin, qh, k_s, v_s, vt_s, o, la, a_s, top_s, mix_s, s0, s1, m0, m1, up_s, dn_s, hid, bt_s,
     g_own, d_own, sem, out_sem, load_sem, a_sem, a_loc, b_sem, b_loc, g_sem, g_loc, d_sem, d_loc) = refs
    tokens = h.shape[0]
    blocks = tokens // B
    A = lambda l: _Gather([w.at[l] for w in (wq, wk, wv)], w_s.at[l, :, pl.ds(0, QKV)], a_sem.at[l], a_loc.at[l])
    O = lambda l: _Gather([wo.at[l]], w_s.at[l, :, pl.ds(QKV, D)], b_sem.at[l], b_loc.at[l])
    G = lambda l: _Gather([wg.at[l], wu.at[l]], wgu_o.at[l], g_sem.at[l], g_loc.at[l], g_own)
    N = lambda l: _Gather([wd.at[l]], wd_o.at[l], d_sem.at[l], d_loc.at[l], d_own)

    load = _local(x, h, sem.at[0])
    load.start()
    for g in (A, O, G, N):
        g(0).load()
    _greet((CORE, Y, X))
    A(FIRST).start()
    O(FIRST).start()
    near_c, near_s = near[0], near[1]
    for i in range(far.shape[1]):
        far_c, far_s = far[0, i : i + 1, :], far[1, i : i + 1, :]
        rows = slice(i * COARSE, (i + 1) * COARSE)
        cos[rows, :] = far_c * near_c - far_s * near_s
        t = far_s * near_c + far_c * near_s
        sin[rows, :] = jnp.where(lax.broadcasted_iota(jnp.int32, t.shape, 1) < HEAD // 2, -t, t)
    tables = [_local(cos, cos_o, sem.at[1]), _local(sin, sin_o, sem.at[2])]
    _start(tables)
    _wait(tables)
    vt_s[HEAD:, :] = jnp.ones((8, tokens), BF)
    A(FIRST).forward()
    G(FIRST).start()
    load.wait()
    A(FIRST).last()
    A(FIRST).finish()

    def project(l, r):
        at = _at(r, B)
        _norm_to(a_s, slice(None), h, at)
        c, s = cos[at, :], sin[at, :]
        columns = lambda m: _mm(a_s[:], w_s[l, :, m * W : (m + 1) * W]).astype(BF)
        ahead = columns(0)
        for m in range(PAIRS + 1):
            t = ahead
            if m < PAIRS:
                ahead = columns(m + 1)
            left, right = t[:, :HEAD], t[:, HEAD:]
            if m < PAIRS:
                qh[2 * m, at, :] = _turn(left, c, s, E)
                qh[2 * m + 1, at, :] = _turn(right, c, s, E)
            else:
                k_s[at, :] = _turn(left, c, s)
                v_s[at, :] = right
                vt_s[:HEAD, at] = right.T

    def attend(l, iq):
        at = _at(iq, B)
        _when((l == FIRST) & (iq == 3), lambda: G(FIRST).forward(), lambda: N(FIRST).start(), lambda: O(FIRST).last())
        _when((l == LAST) & (iq == 2), lambda: G(LAST).forward())
        _when((l == LAST) & (iq == 3), lambda: N(LAST).forward())
        _flash_fwd(iq, qh, k_s, vt_s, top_s, mix_s, (s0, s1), (m0, m1))
        lines = []
        for n in range(HEADS):
            total = mix_s[n, HEAD : HEAD + 1, :]
            o[at, n * HEAD : (n + 1) * HEAD] = (mix_s[n, :HEAD, :] * (1 / total)).astype(BF).T
            rest = -(top_s[n] + jnp.log2(total))
            for _ in range(SPLITS):
                part = rest.astype(BF).astype(F32)
                lines.append(part)
                rest = rest - part
        lines.append(jnp.zeros((HEAD - SPLITS * HEADS, B), F32))
        la[at, :] = jnp.concatenate(lines, 0).astype(BF).T

    def merge(l, r):
        at = _at(r, B)
        _when((l == FIRST) & (r == 1), lambda: G(FIRST).last())
        out = _mm(o[at, :], w_s[l, :, QKV:]).astype(BF)
        hm[at, :] = (h[at, :].astype(F32) + out.astype(F32)).astype(BF)

    def saved(i):
        slot, at, cols, quarter = lax.rem(i, 2), _at(lax.div(i, 2), B), _at(lax.rem(i, 2), HALF), _at(i, H)
        pairs = ((up_s.at[slot], s_o.at[at, cols]), (dn_s.at[slot], r_o.at[at, cols]), (bt_s.at[slot], bt_o.at[:, quarter]), (hid.at[at, cols], hid_o.at[at, cols]))
        return [_local(a, b, out_sem.at[slot, i]) for i, (a, b) in enumerate(pairs)]

    wide = _local(wd_o.at[FIRST], wd_s, sem.at[1])

    def widen(i):
        half, at = lax.rem(i, 2), _at(lax.div(i, 2), B)
        _when(i == 1, lambda: A(LAST).start(), lambda: O(LAST).start(), lambda: G(LAST).load())
        _when(i == 2, lambda: N(FIRST).forward())
        _when(i == 5, lambda: A(LAST).forward(), lambda: O(LAST).forward())
        _when(i == 6, lambda: G(LAST).start(), lambda: N(FIRST).last())
        _when(i == 7, lambda: N(FIRST).finish(), lambda: wide.start(), lambda: N(LAST).load())
        _when(i > 1, lambda: _wait(saved(i - 2)))

        @pl.when(half == 0)
        def _():
            _norm_to(a_s, slice(None), hm, at)

        bt_s[half] = a_s[_at(half, H), :].T
        ahead = None
        for c in range(0, HALF + W, W):
            now = ahead
            if c < HALF:
                at_gate, at_up = (pl.ds(pl.multiple_of(half * HALF + k + c, W), W) for k in (0, FF))
                ahead = _mm(a_s[:], wgu_s[:, at_gate]), _mm(a_s[:], wgu_s[:, at_up])
            if now is not None:
                cols = slice(c - W, c)
                gate, up = now
                sig = jax.nn.sigmoid(gate)
                silu = gate * sig
                up_s[half, :, cols] = silu
                dn_s[half, :, cols] = up * (sig + silu * (1 - sig))
                hid[at, pl.ds(pl.multiple_of(half * HALF + c - W, W), W)] = (silu * up).astype(BF)
        _start(saved(i))

    def narrow(r):
        at = _at(r, B)
        _when(r == 0, lambda: A(LAST).last(), lambda: O(LAST).last())
        _when(r == 1, lambda: N(LAST).start())
        out = _mm(hid[at, :], wd_s[:]).astype(BF)
        h[at, :] = (hm[at, :].astype(F32) + out.astype(F32)).astype(BF)

    def layer(l):
        _loop(blocks, lambda r: project(l, r))
        pairs = ((qh, q_o), (k_s, k_o), (v_s, v_o), (w_s.at[l], wa_o), (o, o_o), (la, la_o), (hm, hm_o))
        outs = [_local(a, b.at[l], sem.at[3 + i]) for i, (a, b) in enumerate(pairs)]
        _start(outs[:3])
        _when(l == FIRST, lambda: O(FIRST).forward())
        _loop(blocks, lambda iq: attend(l, iq))
        me, _ = _place()
        fetch = [_local(wgu_o.at[FIRST, at, :], wgu_s.at[at, :], load_sem.at[r]) for r, at in enumerate([_at(me ^ r, ROWS) for r in range(8)])]

        @pl.when(l == FIRST)
        def _():
            G(FIRST).early()
            _start(fetch[:6])
            O(FIRST).finish()
            A(LAST).load()
            O(LAST).load()

        _when(l == LAST, lambda: G(LAST).last(), lambda: _start(outs[3:6]))
        _loop(blocks, lambda r: merge(l, r))
        _when(l == LAST, lambda: N(LAST).last())
        _start(outs[6:])

        @pl.when(l == FIRST)
        def _():
            G(FIRST).late()
            _start(fetch[6:])
            _wait(fetch)
            _start(outs[3:6])
            _loop(2 * blocks, widen)
            wide.wait()
            _loop(blocks, narrow)
            A(LAST).finish()
            O(LAST).finish()
            for n in (2, 1):
                _wait(saved(2 * blocks - n))

        _wait(outs)
        _when(l == FIRST, lambda: _start([_local(h, h1_o, sem.at[0])]))

    _loop(layers, layer)
    G(LAST).finish()
    N(LAST).finish()
    _wait([_local(h, h1_o, sem.at[0])])


def forward(x, weights):
    T, layers = x.shape[0], weights[0].shape[0]
    tables = rotary_tables(T)
    L = lambda *s, t=BF: ((layers, *s), t)
    outs = [L(T, D), L(HEADS, T, HEAD), L(T, HEAD), L(T, HEAD), L(T, D), L(T, HEAD), ((T, FF), F32), ((T, FF), F32), ((T, FF), BF), ((D, T), BF),
            ((T, D), BF), ((T, HEAD), F32), ((T, HEAD), F32), L(D, WA), L(D, GU), L(FF, D)]
    line = VM((1, B), F32)
    scratch = [VM((T, D), BF), VM((T, D), BF), VM((layers, D, WA), BF), VM((D, GU), BF), VM((FF, D), BF), VM((T, HEAD), F32), VM((T, HEAD), F32),
               VM((HEADS, T, HEAD), BF), VM((T, HEAD), BF), VM((T, HEAD), BF), VM((HEAD + 8, T), BF), VM((T, D), BF), VM((T, HEAD), BF), VM((B, D), BF),
               VM((HEADS, 1, B), F32), VM((HEADS, HEAD + 8, B), F32), VM((B, B), F32), VM((B, B), F32), line, line, VM((2, B, HALF), F32), VM((2, B, HALF), F32), VM((T, FF), BF), VM((2, D, H), BF),
               VM((ROWS, GU), BF), VM((FROWS, D), BF), DMA((10,)), DMA((2, 4)), DMA((8,))] + [DMA((layers, 2, 9)), DMA((layers, 5))] * 4
    small = pl.BlockSpec(memory_space=VM)
    return _call(functools.partial(_forward, layers=layers), "forward", [x, *tables, *weights], [ANY, small, small] + [ANY] * 7, outs,
                 [ANY] * len(outs), scratch, 10**11, 0)


def _mlp_back(*refs, layer, last):
    hm_i, dy_i, wgu_i, wd_i, *refs = refs
    if last:
        dhm_o, kgu, sgu, kd, sd, b_s, *refs = refs
    else:
        s_i, r_i, hid_i, bt_i, keep, send, dhm_o, kgu, sgu, kd, sd, g_o, sq_o, up_s, dn_s, *refs = refs
    hm, dy, hid_s, wgu, wd, g0, g1, bt, dyt, db, sem, part_sem, split_sem, *scatter = refs
    tokens = hm.shape[0]
    blocks, parts = tokens // B, FF // W
    pending = lambda: _Scatter([keep.at[b] for b in range(4)], [send.at[b] for b in range(4)], *scatter)

    def columns(c):
        return _at(c, W), pl.ds(pl.multiple_of(FF + c * W, W), W)

    def weights(c):
        cols, up = columns(c)
        return [(wgu_i.at[layer, :, cols], wgu.at[:, cols]), (wgu_i.at[layer, :, up], wgu.at[:, up])]

    def early(c):
        slot, cols = lax.rem(c, 2), _at(c, W)
        pairs = [(wd_i.at[layer, cols, :], wd.at[cols, :])]
        pairs += weights(c) if last else [(r_i.at[:, cols], dn_s.at[slot]), (s_i.at[:, cols], up_s.at[slot])]
        return [_local(a, b, part_sem.at[slot, i]) for i, (a, b) in enumerate(pairs)]

    def rest(c):
        slot, cols = lax.rem(c, 2), _at(c, W)
        pairs = [] if last else [(hid_i.at[:, cols], hid_s.at[slot]), *weights(c)]
        return [_local(a, b, part_sem.at[slot, 3 + i]) for i, (a, b) in enumerate(pairs)]

    spans = [_at(r, B) for r in range(blocks)]
    dys = [_local(dy_i.at[at, :], dy.at[at, :], sem.at[r]) for r, at in enumerate(spans)]
    hms = [_local(hm_i.at[layer, at, :], hm.at[at, :], sem.at[blocks + r]) for r, at in enumerate(spans)]
    flip = [] if last else [_local(bt_i, bt, sem.at[2 * blocks])]
    if last:
        _start(hms[:1] + dys[:1] + early(0) + [c for pair in zip(hms[1:], dys[1:]) for c in pair] + early(1))
    else:
        _start(dys[:1] + early(0) + dys[1:] + flip + rest(0) + early(1) + hms)
        _greet(AROUND)
        pending().start()
    db[:] = jnp.zeros(db.shape, F32)

    def widen(c, slot, r, g):
        rows = slice(r * B, (r + 1) * B)
        if last:
            gate, up = (_mm(b_s[rows, :], wgu[:, cols]) for cols in columns(c))
        t = _mt(dy[rows, :], wd[_at(c, W), :]).astype(BF).astype(F32)
        if last:
            sig = jax.nn.sigmoid(gate)
            silu = gate * sig
            hid_s[slot, rows, :] = (silu * up).astype(BF)
            slope = up * (sig + silu * (1 - sig))
        else:
            silu, slope = up_s[slot, rows, :], dn_s[slot, rows, :]
        g[rows, :W] = (t * slope).astype(BF)
        g[rows, W:] = (t * silu).astype(BF)

    for r in range(blocks + 1):
        if r < blocks:
            rows = slice(r * B, (r + 1) * B)
            _wait(hms[r : r + last] + dys[r : r + 1])
            if r == 0:
                _wait(early(0))
            if last:
                _norm_to(b_s, rows, hm, rows)
                bt[:, rows] = b_s[rows, :].T
            dyt[:, rows] = dy[rows, :].T
        if r > 0:
            widen(0, 0, r - 1, g0)
    _wait(flip)

    def step(c, slot, g, later):
        cols, up = columns(c)
        after = jnp.minimum(c + 1, parts - 1)
        _when(c + 2 < parts, lambda: _start(early(c + 2)))
        _when(c + 1 < parts, lambda: _start(rest(c + 1)), lambda: _wait(early(c + 1)))
        _wait(rest(c))
        for r in range(blocks):
            widen(after, 1 - slot, r, later)
        both = jnp.concatenate([wgu[:, cols], wgu[:, up]], 1)
        for r in range(blocks):
            rows = slice(r * B, (r + 1) * B)
            db[rows, :] += _mt(g[rows, :], both)
        dw = _mm(bt[:], g[:]).astype(BF)
        wgu[:, cols] = dw[:, :W]
        wgu[:, up] = dw[:, W:]
        wd[cols, :] = _mm(dyt[:], hid_s[slot]).astype(BF).T
        if not last:
            _when(c == 1, lambda: pending().forward())
            _when(c == 4, lambda: pending().pass_on())

    def two(u):
        step(2 * u, 0, g0, g1)
        step(2 * u + 1, 1, g1, g0)

    _loop(parts // 2, two)
    copies = _split_out(wgu, ROWS, kgu, sgu, split_sem.at[0]) + _split_out(wd, FROWS, kd, sd, split_sem.at[1])
    if not last:
        _wait(hms)
    out = lambda r: _local(hm.at[_at(r, B), :], dhm_o.at[_at(r, B), :], sem.at[r])

    def back(r):
        at = _at(r, B)
        hm[at, :] = _norm_back(hm[at, :], db[at, :].astype(BF), dy[at, :])
        out(r).start()

    _loop(blocks, back)
    if not last:
        sq_o[:] = pending().finish(g_o)
    _wait(copies + [out(r) for r in range(blocks)])


WHOLE = pl.BlockSpec(memory_space=VM)


def mlp_back(saved, dy, layer, pending, talks):
    T = dy.shape[0]
    last = pending is None
    gu, d = ((4, ROWS, GU), BF), ((4, FROWS, D), BF)
    args = [saved["hm"], dy, saved["wgu"], saved["wd"]]
    outs, out_specs = [((T, D), BF), gu, gu, d, d], [ANY] * 5
    scratch = [VM((T, D), BF), VM((T, D), BF), VM((2, T, W), BF), VM((D, GU), BF), VM((FF, D), BF), VM((T, 2 * W), BF), VM((T, 2 * W), BF),
               VM((D, T), BF), VM((D, T), BF), VM((T, D), F32), DMA((9,)), DMA((2, 6)), DMA((2, 2, 4))]
    if last:
        scratch = [VM((T, D), BF)] + scratch
    else:
        args += [saved[n] for n in ("s", "r", "hid", "bt")] + pending
        outs += [((ROWS, WA), BF), ((8, HEAD), F32)]
        out_specs += [WHOLE, WHOLE]
        scratch = [VM((2, T, W), F32), VM((2, T, W), F32)] + scratch + _scatter_scratch(ROWS, WA)
    return _call(functools.partial(_mlp_back, layer=layer, last=last), "mlp_back", args, [ANY] * len(args), outs, out_specs, scratch, 4 * 10**10, talks)


def _flash_back(iq, qh, qt, doh, dot, la, dl, zs, k_s, v_s, dq, dkt, dvt, p_s, x_s):
    def give(slot, count, s, d, edge=B):
        for e in range(0, count, HEAD):
            cols = slice(e, e + HEAD)
            for r in range(0, B, H):
                rows = slice(r, r + H)
                p = jnp.exp2(s[rows, cols])
                if e >= edge:
                    p = jnp.where(_hidden(p.shape, edge - e, 0), 0.0, p)
                p_s[slot][rows, cols] = p.astype(BF)
                x_s[slot][rows, cols] = (p * d[rows, cols]).astype(BF)

    def weigh_half(m, half, slot):
        rows, keys = pl.ds(pl.multiple_of(iq * B + half * H, H), H), pl.ds(pl.multiple_of(iq * B, B), H + half * H)
        pair = (2 * m, 2 * m + 1)
        q = jnp.concatenate([jnp.concatenate([qh[n, rows, :], la[rows, :] * zs[n, :H, :]], 1) for n in pair], 0)
        do = jnp.concatenate([jnp.concatenate([doh[n, rows, :], dl[rows, :] * zs[n, :H, :]], 1) for n in pair], 0)
        z = zs[HEADS, : H + half * H, :]
        s = _mt(q, jnp.concatenate([k_s[keys, :], z], 1))
        d = _mt(do, jnp.concatenate([v_s[keys, :], z], 1))
        give(slot, H + half * H, s, d, half * H)

    def rest_half(m, half, slot):
        rows, keys = pl.ds(pl.multiple_of(iq * B + half * H, H), H), pl.ds(pl.multiple_of(iq * B, B), H + half * H)
        pair = (2 * m, 2 * m + 1)
        p, x = p_s[slot][:, : H + half * H], x_s[slot][:, : H + half * H]
        dvt[:, keys] += _mm(jnp.concatenate([dot[n, :, rows] for n in pair], 1), p)
        dkt[:, keys] += _mm(jnp.concatenate([qt[n, :, rows] for n in pair], 1), x)
        g = _mm(x, k_s[keys, :])
        for i, n in enumerate(pair):
            dq[n, half * H : (half + 1) * H, :] = g[i * H : (i + 1) * H, :]

    _halves(weigh_half, rest_half)

    @pl.when(iq > 0)
    def _():
        rows = _at(iq, B)

        def weigh(j, n, slot):
            keys = _at(j, B)
            s = _mt(jnp.concatenate([qh[n, rows, :], la[rows, :]], 1), jnp.concatenate([k_s[keys, :], zs[n]], 1))
            d = _mt(jnp.concatenate([doh[n, rows, :], dl[rows, :]], 1), jnp.concatenate([v_s[keys, :], zs[n]], 1))
            give(slot, B, s, d)

        def rest(j, n, slot):
            keys = _at(j, B)
            dvt[:, keys] += _mm(dot[n, :, rows], p_s[slot][:])
            dkt[:, keys] += _mm(qt[n, :, rows], x_s[slot][:])
            dq[n] += _mm(x_s[slot][:], k_s[keys, :])

        _pairs(PAIRS * iq, weigh, rest)


def _attn_back(*refs, layer, count):
    first = layer == FIRST
    dhm_i, h_i, q_i, k_i, v_i, o_i, la_i, cos_i, sin_i, wa_i, kgu, sgu, kd, sd, *refs = refs
    if first:
        sq_a, sq_b, ggu_o, gd_o, ga_o, factor_o, *refs = refs
    else:
        ggu_o, gd_o, sq_o, dh_o, keep_o, send_o, *refs = refs
    (dhm, h, qh, k_s, v_s, o, la, cos, sin, wa, doh, dqkv, a_s, qt, dot, dl, zs, dq, dkt, dvt, p0, p1, x0, x1, sem, split_sem, *refs) = refs
    scatter_gu, scatter_d, refs = refs[:5], refs[5:10], refs[10:]
    tokens = h.shape[0]
    blocks = tokens // B
    pending = lambda: [_Scatter([a.at[b] for b in range(4)], [c.at[b] for b in range(4)], *s) for a, c, s in ((kgu, sgu, scatter_gu), (kd, sd, scatter_d))]

    def piece(i, a, b):
        return _local(a, b, sem.at[i])

    wo = piece(0, wa_i.at[layer, :, pl.ds(QKV, D)], wa.at[:, pl.ds(QKV, D)])
    groups = []
    for r in range(blocks):
        at = _at(r, B)
        pairs = ((dhm_i.at[at, :], dhm.at[at, :]), (q_i.at[layer, :, at, :], qh.at[:, at, :]), (o_i.at[layer, at, :], o.at[at, :]))
        groups.append([piece(1 + 3 * r + i, a, b) for i, (a, b) in enumerate(pairs)])
    pairs = ((la_i.at[layer], la), (k_i.at[layer], k_s), (v_i.at[layer], v_s), (h_i, h), (cos_i, cos), (sin_i, sin),
             (wa_i.at[layer, :, pl.ds(0, QKV)], wa.at[:, pl.ds(0, QKV)]))
    late = [piece(1 + 3 * blocks + i, a, b) for i, (a, b) in enumerate(pairs)]
    _start([wo] + sum(groups, []) + late)
    _greet(range(1, 8) if first else AROUND)
    for s in pending():
        s.start()
    dkt[:] = jnp.zeros(dkt.shape, F32)
    dvt[:] = jnp.zeros(dvt.shape, F32)
    lane = lax.broadcasted_iota(jnp.int32, (B, HEAD), 1)
    for n in range(HEADS):
        zs[n] = ((lane >= SPLITS * n) & (lane < SPLITS * (n + 1))).astype(F32).astype(BF)
    zs[HEADS] = (lane < SPLITS * HEADS).astype(F32).astype(BF)
    wo.wait()

    def lead(r):
        at = _at(r, B)
        columns = lambda m: _mt(dhm[at, :], wa[m * W : (m + 1) * W, QKV:]).astype(BF)
        ahead = columns(0)
        means = jnp.zeros(lane.shape, F32)
        for n in range(HEADS):
            if n % 2 == 0:
                do = ahead
                if n + 2 < HEADS:
                    ahead = columns(n // 2 + 1)
            by = do[:, n % 2 * HEAD : (n % 2 + 1) * HEAD]
            doh[n, at, :] = by
            dot[n, :, at] = by.T
            qt[n, :, at] = qh[n, at, :].T
            rest = -jnp.sum(by.astype(F32) * o[at, n * HEAD : (n + 1) * HEAD].astype(F32), -1, keepdims=True)
            for i in range(SPLITS):
                part = rest.astype(BF).astype(F32)
                means = jnp.where(lane == SPLITS * n + i, part, means)
                rest = rest - part
        dl[at, :] = means.astype(BF)

    def begin(r):
        for k in range(blocks):
            _when(r == k, lambda: _wait(groups[k]))
        lead(r)

    _loop(blocks, begin)
    for s in pending():
        s.forward()
    wa[:, QKV:] = _tm(o[:], dhm[:]).astype(BF)
    if first:
        own = [_Scatter(*[_blocks(wa.at[:, cols], ROWS, k) for k in range(2)], *s) for cols, s in
               ((pl.ds(QKV, D), refs[:4]), (pl.ds(0, QKV), [scatter_gu[0].at[:, :, pl.ds(0, QKV)], *refs[4:7]]))]
        own[0].start()
    _wait(late)

    def attend(g):
        iq = blocks - 1 - g
        at = _at(iq, B)
        _when(g == 2, *[lambda s=s: s.pass_on() for s in pending()])
        if first:
            _when(g == 1, lambda: own[0].forward())
            _when(g == 2, lambda: own[0].pass_on())
        _flash_back(iq, qh, qt, doh, dot, la, dl, zs, k_s, v_s, dq, dkt, dvt, (p0, p1), (x0, x1))
        c, s = cos[at, :], sin[at, :]

        def turn(m):
            for n in (2 * m, 2 * m + 1):
                dqkv[at, _at(n, HEAD)] = _turn_back(dq[n] * SCALE, c, s)

        _loop(PAIRS, turn)
        dqkv[at, D : D + HEAD] = _turn_back((dkt[:, at] * (SCALE / E)).T, c, s)
        dqkv[at, D + HEAD :] = dvt[:, at].T.astype(BF)
        _norm_to(a_s, at, h, at)

    _loop(blocks, attend)
    dw = lambda: wa.__setitem__((slice(None), slice(0, QKV)), _tm(a_s[:], dqkv[:]).astype(BF))
    if first:
        dw()
        mine, all_s, all_sem = refs[7:]
        own[1].start()
        gu, d = pending()
        squares = gu.finish(ggu_o) + d.finish(gd_o) + sq_a[:] + sq_b[:]
        own[1].forward()
        own[1].pass_on()
        squares += own[0].finish(ga_o.at[:, pl.ds(QKV, D)])
        mine[:] = own[1].finish(ga_o.at[:, pl.ds(0, QKV)]) + squares
        me, _ = _place()
        copies = [_remote(mine, all_s.at[me], all_sem, r, r) for r in range(1, 8)]
        _start(copies)
        all_s[me] = mine[:]
        _wait(copies)
        total = jnp.sum(jnp.sum(jnp.sum(all_s[:], axis=0), axis=1, keepdims=True), axis=0, keepdims=True)
        factor_o[:] = jnp.broadcast_to(jnp.minimum(1.0, 0.5 * lax.rsqrt(total / count + 1e-30)), factor_o.shape)
    else:
        out = lambda r: _local(h.at[_at(r, B), :], dh_o.at[_at(r, B), :], split_sem.at[2, r])

        def back(r):
            at = _at(r, B)
            o[at, :] = _mt(dqkv[at, :], wa[:, :QKV]).astype(BF)
            h[at, :] = _norm_back(h[at, :], o[at, :], dhm[at, :])
            out(r).start()

        _loop(blocks, back)
        dw()
        copies = _split_out(wa, ROWS, keep_o, send_o, split_sem)
        gu, d = pending()
        sq_o[:] = gu.finish(ggu_o) + d.finish(gd_o)
        _wait(copies + [out(r) for r in range(blocks)])


def attn_back(saved, dhm, h, layer, pending, squares, count, talks):
    T = h.shape[0]
    args = [dhm, h] + [saved[n] for n in ("q", "k", "v", "o", "la", "cos", "sin", "wa")] + [*pending, *squares]
    specs = [ANY] * (10 + len(pending)) + [WHOLE] * len(squares)
    dw, small = ((4, ROWS, WA), BF), ((8, HEAD), F32)
    outs, out_specs = [((ROWS, GU), BF), ((FROWS, D), BF)], [WHOLE, WHOLE]
    tile = VM((B, B), BF)
    scratch = [VM((T, D), BF), VM((T, D), BF), VM((HEADS, T, HEAD), BF), VM((T, HEAD), BF), VM((T, HEAD), BF), VM((T, D), BF), VM((T, HEAD), BF),
               VM((T, HEAD), F32), VM((T, HEAD), F32), VM((D, WA), BF), VM((HEADS, T, HEAD), BF), VM((T, QKV), BF), VM((T, D), BF),
               VM((HEADS, HEAD, T), BF), VM((HEADS, HEAD, T), BF), VM((T, HEAD), BF), VM((HEADS + 1, B, HEAD), BF), VM((HEADS, B, HEAD), F32),
               VM((HEAD, T), F32), VM((HEAD, T), F32), tile, tile, tile, tile, DMA((20,)), DMA((3, 4)),
               *_scatter_scratch(ROWS, GU), *_scatter_scratch(FROWS, D)]
    if layer == FIRST:
        outs += [((ROWS, WA), BF), small]
        out_specs += [WHOLE, WHOLE]
        scratch.append(VM((4, ROWS, D), BF))
        for width in (D, QKV):
            scratch += [VM((4, ROWS, width), BF), VM((3, ROWS, width), BF), DMA((2, 10))]
        scratch += [VM((8, HEAD), F32), VM((8, 8, HEAD), F32), DMA((2, 8))]
    else:
        outs += [small, ((T, D), BF), dw, dw]
        out_specs += [WHOLE, ANY, ANY, ANY]
    return _call(functools.partial(_attn_back, layer=layer, count=count), "attn_back", args, specs, outs, out_specs, scratch, 5 * 10**10, talks)


TRIOS = range(21)


def _adamw(*refs, layers):
    refs = iter(refs)
    take = lambda count: list(itertools.islice(refs, count))
    (factor_ref,) = take(1)
    grads = take(3 * layers)
    given, out, held = (take(len(TRIOS)) for _ in range(3))
    g_held = take(len(grads))
    load_sem, grad_sem, store_sem = refs
    factor = factor_ref[:1, :1]
    where = [(which, sum(widths[:i]), width) for which, widths in enumerate(((D, HEAD, HEAD, D), (FF, FF), (D,))) for i, width in enumerate(widths)]
    fetch = [_local(a, b, grad_sem.at[i]) for i, (a, b) in enumerate(zip(grads, g_held))]

    def moves(layer, i):
        trio = TRIOS[i::7]
        return ([_local(given[k].at[layer], held[k].at[layer], load_sem.at[layer, k]) for k in trio],
                [_local(held[k].at[layer], out[k].at[layer], store_sem.at[layer, k]) for k in trio])

    every = [(layer, i) for layer in range(layers) for i in range(7)]
    for layer, i in every:
        if where[i][1] == 0:
            fetch[3 * layer + where[i][0]].start()
        _start(moves(layer, i)[0])
    for layer, i in every:
        which, start, width = where[i]
        if start == 0:
            fetch[3 * layer + which].wait()
        loads, stores = moves(layer, i)
        _wait(loads)
        w_ref, m_ref, v_ref = (held[k].at[layer] for k in TRIOS[i::7])
        g_ref = g_held[3 * layer + which]

        def step(r):
            at = _at(r, 16)
            g = g_ref[at, start : start + width].astype(F32) * factor
            m = 0.9 * m_ref[at, :] + 0.1 * g
            v = 0.95 * v_ref[at, :] + 0.05 * g * g
            w = w_ref[at, :].astype(F32)
            w_ref[at, :] = (w - 0.02 * (m * lax.rsqrt(v + 1e-8) + 0.1 * w)).astype(BF)
            m_ref[at, :] = m
            v_ref[at, :] = v

        _loop(g_ref.shape[0] // 16, step)
        _start(stores)
    for layer, i in every:
        _wait(moves(layer, i)[1])


def adamw(factor, grads, weights, m, v):
    layers = len(grads)
    flat, given = sum(grads, []), [*weights, *m, *v]
    whole = lambda a: VM(a.shape, a.dtype)
    return _call(functools.partial(_adamw, layers=layers), "adamw", [factor, *flat, *given], [WHOLE] + [ANY] * (len(flat) + len(given)),
                 [(a.shape, a.dtype) for a in given], [ANY] * len(given),
                 [whole(a) for a in given + flat] + [DMA((layers, len(given))), DMA((len(flat),)), DMA((layers, len(given)))], 10**9, None)


def rotary_tables(tokens):
    half = HEAD // 2
    rate = THETA ** (-np.arange(half, dtype=np.float64) / half)

    def table(places):
        angle = np.concatenate([places[:, None] * rate] * 2, 1)
        return jnp.asarray(np.stack([np.cos(angle), np.sin(angle)]), F32)

    return table(np.arange(COARSE)), table(np.arange(0, tokens, COARSE))


def solution(mesh):
    def step(x, dy, *arrays):
        weights, m, v = (arrays[i : i + 7] for i in (0, 7, 14))
        x, dy = x[0], dy[0]
        names = ("hm", "q", "k", "v", "o", "la", "s", "r", "hid", "bt", "h1", "cos", "sin", "wa", "wgu", "wd")
        saved = dict(zip(names, forward(x, weights)))
        count = 8 * sum(w.size for w in weights)
        by_hm, *mlp1 = mlp_back(saved, dy, LAST, None, None)
        ggu1, gd1, sq_a, by_h, *attn1 = attn_back(saved, by_hm, saved["h1"], LAST, mlp1, [], count, 1)
        by_hm, *mlp0, ga1, sq_b = mlp_back(saved, by_h, FIRST, attn1, 2)
        ggu0, gd0, ga0, factor = attn_back(saved, by_hm, x, FIRST, mlp0, [sq_a, sq_b], count, 3)
        return tuple(adamw(factor, [[ga0, ggu0, gd0], [ga1, ggu1, gd1]], weights, m, v))

    states, cut = P(("rep", "dp"), None, None), P(None, "dp", None)
    return jax.shard_map(
        step,
        mesh=mesh,
        in_specs=(states, states) + (cut,) * 21,
        out_specs=(P("rep", "dp", None),) * 21,
        check_vma=False,
    )
```

```python
import functools
import itertools

import jax
import jax.numpy as jnp
import numpy as np
from jax import lax
from jax.experimental import pallas as pl
from jax.experimental.pallas import tpu as pltpu
from jax.sharding import PartitionSpec as P

HEAD, HEADS, D, FF = 128, 6, 768, 2048
THETA = 10000
SCALE = HEAD**-0.5
E = SCALE * 1.4426950408889634
NEG = -1e30
HIDDEN = NEG + NEG
EPS = 1e-6
QKV = D + 2 * HEAD
WA = QKV + D
GU = 2 * FF
ROWS, FROWS = D // 8, FF // 8
COARSE = 64
SPLITS = 3
PAIRS = HEADS // 2
B = 512
H = B // 2
STEP = 16
W = 256
FIRST, LAST = range(2)
HALF = FF // 2
X, Y, CORE = 4, 2, 1
AROUND = (CORE, Y, X, X ^ Y)

BF, F32 = jnp.bfloat16, jnp.float32
VM = pltpu.VMEM
DMA = pltpu.SemaphoreType.DMA
MESH = pl.DeviceIdType.MESH
ANY = pl.BlockSpec(memory_space=pltpu.HBM)


def _place():
    return lax.axis_index("dp"), lax.axis_index("rep")


def _greet(bits):
    me, rep = _place()
    barrier = pltpu.get_barrier_semaphore()
    for bit in bits:
        pl.semaphore_signal(barrier, inc=1, device_id=(rep, me ^ bit), device_id_type=MESH)
    pl.semaphore_wait(barrier, len(bits))


class _Copy:
    def __init__(self, make):
        self.make = make

    def start(self):
        self.make().start()

    def wait(self):
        self.make().wait()

    def wait_send(self):
        self.make().wait_send()

    def wait_recv(self):
        self.make().wait_recv()


def _local(src, dst, sem):
    return _Copy(lambda: pltpu.make_async_copy(src, dst, sem))


def _remote(src, dst, sems, k, bit):
    me, rep = _place()
    return _Copy(lambda: pltpu.make_async_remote_copy(src_ref=src, dst_ref=dst, send_sem=sems.at[0, k], recv_sem=sems.at[1, k],
                                                      device_id=(rep, me ^ bit), device_id_type=MESH))


def _start(copies):
    for c in copies:
        c.start()


def _wait(copies):
    for c in copies:
        c.wait()


class _Gather:
    def __init__(self, parts, full, sems, local, own=None):
        me, _ = _place()
        rows = parts[0].shape[0]
        half = rows // 2

        def at(dev, first=0, count=rows):
            return full.at[pl.ds(pl.multiple_of(dev * rows + first, 16), count), :]

        ids = itertools.count()

        def copy(bit, dev, first=0, count=rows, src=None):
            return _remote(at(dev, first, count) if src is None else src, at(dev, first, count), sems, next(ids), bit)

        mine = at(me) if own is None else own
        self.loads, col = [], 0
        for k, part in enumerate(parts):
            width = part.shape[1]
            self.loads.append(_local(part, mine.at[:, pl.ds(col, width)], local.at[k]))
            col += width
        self.store = [] if own is None else [_local(own, at(me), local.at[4])]
        self.x, self.y, self.core = (copy(bit, me, src=mine) for bit in (X, Y, CORE))
        self.far = [copy(X, me ^ Y, count=half), copy(Y, me ^ X, half, half)]
        self.near = [copy(CORE, me ^ X), copy(CORE, me ^ Y)]
        self.end = [copy(CORE, me ^ X ^ Y, count=half), copy(CORE, me ^ X ^ Y, half, half)]

    def load(self):
        _start(self.loads)

    def start(self):
        _wait(self.loads)
        _start([self.x, self.y, self.core] + self.store)

    def forward(self):
        self.x.wait_recv()
        self.y.wait_recv()
        _start(self.far + self.near)

    def last(self):
        for c in self.far:
            c.wait_recv()
        _start(self.end)

    def early(self):
        for c in [self.core] + self.near:
            c.wait_recv()
        _wait(self.store)

    def late(self):
        for c in self.end:
            c.wait_recv()
        for c in [self.x, self.y, self.core] + self.far + self.near + self.end:
            c.wait_send()

    def finish(self):
        self.early()
        self.late()


def _block(xy, other):
    me, _ = _place()
    return ((me // 2) ^ xy) * 2 + ((me % 2) ^ other)


def _blocks(full, rows, other):
    return [full.at[pl.ds(pl.multiple_of(_block(xy, other) * rows, 16), rows), :] for xy in range(4)]


class _Scatter:
    def __init__(self, keep, send, kept, came, ici, sems, local=None):
        self.kept, self.came, self.ici = kept, came, ici
        self.loads = [_local(keep[b], kept.at[b], local.at[b]) for b in range(4)] if local is not None else []
        self.keep = [kept.at[b] for b in range(4)] if self.loads else keep
        ids = itertools.count()
        self.core = [_remote(send[b], came.at[b], sems, next(ids), CORE) for b in range(4)]
        half = came.shape[1] // 2
        self.ways = ((pl.ds(0, half), X, 2, Y, 1), (pl.ds(half, half), Y, 1, X, 2))
        self.first = [_remote(kept.at[b, at, :], ici.at[k, at, :], sems, next(ids), bit) for at, bit, near, _, _ in self.ways for k, b in enumerate((near, 3))]
        self.second = [_remote(kept.at[b, at, :], ici.at[2, at, :], sems, next(ids), bit) for at, _, _, bit, b in self.ways]

    def start(self):
        for b in (3, 2, 1, 0):
            _start([self.core[b]] + self.loads[b : b + 1])

    def _add(self, out, start, rows, *terms):
        def add(i):
            at = pl.ds(pl.multiple_of(start + i * STEP, STEP), STEP)
            out[at, :] = sum(t[at, :].astype(F32) for t in terms).astype(BF)

        _loop(rows // STEP, add)

    def forward(self):
        for b in (3, 2, 1):
            self.core[b].wait_recv()
            _wait(self.loads[b : b + 1])
            self._add(self.kept.at[b], 0, self.came.shape[1], self.keep[b], self.came.at[b])
        _start(self.first)

    def pass_on(self):
        half = self.came.shape[1] // 2
        for i, way in enumerate(self.ways):
            self.first[2 * i + 1].wait_recv()
            self._add(self.kept.at[way[-1]], i * half, half, self.kept.at[way[-1]], self.ici.at[1])
            self.second[i].start()

    def finish(self, g_ref):
        self.core[0].wait_recv()
        _wait(self.loads[:1])
        for c in self.first[::2] + self.second:
            c.wait_recv()
        self._add(g_ref, 0, g_ref.shape[0], self.keep[0], self.came.at[0], self.ici.at[0], self.ici.at[2])

        def square(i, squares):
            g = g_ref[_at(i, STEP), :].astype(F32)
            return squares + g[:8] * g[:8] + g[8:] * g[8:]

        squares = lax.fori_loop(0, g_ref.shape[0] // STEP, square, jnp.zeros((8, g_ref.shape[1]), F32))
        for c in self.core + self.first + self.second:
            c.wait_send()
        return sum(squares[:, c : c + HEAD] for c in range(0, g_ref.shape[1], HEAD))


def _scatter_scratch(rows, n):
    return [VM((4, rows, n), BF), VM((4, rows, n), BF), VM((3, rows, n), BF), DMA((2, 10)), DMA((4,))]


def _split_out(full, rows, keep, send, sems):
    copies = [_local(src, ref.at[b], sems.at[k, b]) for k, ref in enumerate((keep, send)) for b, src in enumerate(_blocks(full, rows, k))]
    _start(copies)
    return copies


def _dot(a, b, ca, cb):
    return lax.dot_general(a, b, (((ca,), (cb,)), ((), ())), preferred_element_type=F32)


_mm = functools.partial(_dot, ca=1, cb=0)
_mt = functools.partial(_dot, ca=1, cb=1)
_tm = functools.partial(_dot, ca=0, cb=0)


def _at(i, n):
    return pl.ds(pl.multiple_of(i * n, n), n)


def _when(cond, *todo):
    @pl.when(cond)
    def _():
        for do in todo:
            do()


def _loop(n, body):
    def step(i, _):
        body(i)

    lax.fori_loop(0, n, step, None)


def _scale(wide):
    return lax.rsqrt(jnp.mean(wide * wide, -1, keepdims=True) + EPS)


def _norm_to(out, to, h, at):
    wide = h[at, :].astype(F32)
    out[to, :] = (wide * _scale(wide)).astype(BF)


def _norm_back(h, dy, by):
    wide, dy = h.astype(F32), dy.astype(F32)
    scale = _scale(wide)
    back = scale * (dy - wide * (scale * scale * jnp.mean(dy * wide, -1, keepdims=True)))
    return (by.astype(F32) + back.astype(BF).astype(F32)).astype(BF)


def _turn(t, cos, sin, times=1):
    t = t.astype(F32)
    return ((t * cos + pltpu.roll(t, HEAD // 2, 1) * sin) * times).astype(BF)


def _turn_back(t, cos, sin):
    return (t * cos - pltpu.roll(t, HEAD // 2, 1) * sin).astype(BF)


def _call(body, name, args, specs, outs, out_specs, scratch, flops, talks):
    return pl.pallas_call(
        body,
        in_specs=specs,
        out_specs=out_specs,
        scratch_shapes=scratch,
        out_shape=[jax.ShapeDtypeStruct(*o) for o in outs],
        compiler_params=pltpu.CompilerParams(vmem_limit_bytes=67043328, collective_id=talks, has_side_effects=talks is not None),
        cost_estimate=pl.CostEstimate(flops=flops, transcendentals=0, bytes_accessed=flops // 1000),
        name=name,
    )(*args)


def _pairs(hi, first, steps):
    first(0, 0, 0)

    def body(u):
        j, m = lax.div(u, PAIRS), lax.rem(u, PAIRS)
        later = jnp.minimum(u + 1, hi - 1)
        first(j, 2 * m + 1, 1)
        steps(j, 2 * m, 0)
        first(lax.div(later, PAIRS), 2 * lax.rem(later, PAIRS), 0)
        steps(j, 2 * m + 1, 1)

    _loop(hi, body)


def _halves(first, steps):
    first(0, 1, 0)

    def body(m):
        first(m, 0, 1)
        steps(m, 1, 0)
        first(jnp.minimum(m + 1, PAIRS - 1), 1, 0)
        steps(m, 0, 1)

    _loop(PAIRS, body)


def _hidden(shape, later, queries):
    return lax.broadcasted_iota(jnp.int32, shape, 1 - queries) - later > lax.broadcasted_iota(jnp.int32, shape, queries)


def _flash_fwd(iq, qh, k_s, vt_s, top_s, mix_s, s_s, m_s):
    def mix(s, top, cols, start, count):
        got = []
        for r in range(0, count, W):
            p = jnp.exp2(s[r : r + W, cols] - top).astype(BF)
            got.append(_mm(vt_s[:, pl.ds(pl.multiple_of(start + r, W), W)], p))
        return sum(got)

    def score_half(m, half, slot):
        rows, keys = pl.ds(pl.multiple_of(iq * B + half * H, H), H), pl.ds(pl.multiple_of(iq * B, B), H + half * H)
        s = _mt(k_s[keys, :], jnp.concatenate([qh[2 * m, rows, :], qh[2 * m + 1, rows, :]], 0))
        hide = _hidden((H, H), 0, 1)
        for i in range(2):
            cols, last = slice(i * H, (i + 1) * H), slice(half * H, (half + 1) * H)
            t = jnp.where(hide, HIDDEN, s[last, cols])
            top = t.max(axis=0, keepdims=True)
            s_s[slot][last, cols] = t
            if half:
                s_s[slot][:H, cols] = s[:H, cols]
                top = jnp.maximum(top, s[:H, cols].max(axis=0, keepdims=True))
            m_s[slot][:, cols] = top

    def rest_half(m, half, slot):
        for i in range(2):
            cols, to = slice(i * H, (i + 1) * H), slice(half * H, (half + 1) * H)
            top = m_s[slot][:, cols]
            top_s[2 * m + i, :, to] = top
            mix_s[2 * m + i, :, to] = mix(s_s[slot], top, cols, iq * B, H + half * H)

    _halves(score_half, rest_half)

    @pl.when(iq > 0)
    def _():
        rows = _at(iq, B)

        def score(j, n, slot):
            s = _mt(k_s[_at(j, B), :], qh[n, rows, :])
            s_s[slot][:] = s
            m_s[slot][:] = s.max(axis=0, keepdims=True)

        def rest(j, n, slot):
            old = top_s[n]
            top = jnp.maximum(old, m_s[slot][:])
            top_s[n] = top
            keep = jnp.exp2(old - top)
            for c in range(0, B, W):
                cols = slice(c, c + W)
                mix_s[n, :, cols] = mix_s[n, :, cols] * keep[:, cols] + mix(s_s[slot], top[:, cols], cols, j * B, B)

        _pairs(PAIRS * iq, score, rest)


def _forward(x, near, far, *refs, layers):
    (wq, wk, wv, wo, wg, wu, wd, a_o, hm_o, q_o, k_o, v_o, o_o, la_o, s_o, r_o, hid_o, bt_o, h1_o, cos_o, sin_o, wa_o, wgu_o, wd_o,
     h, hm, w_s, wgu_s, wd_s, cos, sin, qh, k_s, v_s, vt_s, o, la, a_s, top_s, mix_s, s0, s1, m0, m1, up_s, dn_s, hid, bt_s,
     g_own, d_own, sem, out_sem, load_sem, a_sem, a_loc, k_sem, k_loc, b_sem, b_loc, g_sem, g_loc, d_sem, d_loc) = refs
    tokens = h.shape[0]
    blocks = tokens // B
    A = lambda l: _Gather([wq.at[l, :, pl.ds(0, B)]], w_s.at[l, :, pl.ds(0, B)], a_sem.at[l], a_loc.at[l])
    K = lambda l: _Gather([wq.at[l, :, pl.ds(B, W)], wk.at[l], wv.at[l]], w_s.at[l, :, pl.ds(B, B)], k_sem.at[l], k_loc.at[l])
    O = lambda l: _Gather([wo.at[l]], w_s.at[l, :, pl.ds(QKV, D)], b_sem.at[l], b_loc.at[l])
    G = lambda l: _Gather([wg.at[l], wu.at[l]], wgu_o.at[l], g_sem.at[l], g_loc.at[l], g_own)
    N = lambda l: _Gather([wd.at[l]], wd_o.at[l], d_sem.at[l], d_loc.at[l], d_own)

    load = _local(x, h, sem.at[0])
    load.start()
    for g in (A, K, O, G, N):
        g(FIRST).load()
    _greet((CORE, Y, X))
    A(FIRST).start()
    K(FIRST).start()
    near_c, near_s = near[0], near[1]
    for i in range(far.shape[1]):
        far_c, far_s = far[0, i : i + 1, :], far[1, i : i + 1, :]
        rows = slice(i * COARSE, (i + 1) * COARSE)
        cos[rows, :] = far_c * near_c - far_s * near_s
        t = far_s * near_c + far_c * near_s
        sin[rows, :] = jnp.where(lax.broadcasted_iota(jnp.int32, t.shape, 1) < HEAD // 2, -t, t)
    tables = [_local(cos, cos_o, sem.at[1]), _local(sin, sin_o, sem.at[2])]
    _start(tables)
    _wait(tables)
    vt_s[HEAD:, :] = jnp.ones((8, tokens), BF)
    A(FIRST).forward()
    K(FIRST).forward()
    O(FIRST).start()
    G(FIRST).start()
    load.wait()
    A(FIRST).last()
    K(FIRST).last()
    A(FIRST).finish()

    def project(l, r, start):
        at = _at(r, B)
        if not start:
            _norm_to(o, at, h, at)
        c, s = cos[at, :], sin[at, :]
        columns = lambda m: _mm(o[at, :], w_s[l, :, m * W : (m + 1) * W]).astype(BF)
        ahead = columns(start)
        for m in (start, start + 1):
            t = ahead
            if m == start:
                ahead = columns(m + 1)
            left, right = t[:, :HEAD], t[:, HEAD:]
            if m < PAIRS:
                qh[2 * m, at, :] = _turn(left, c, s, E)
                qh[2 * m + 1, at, :] = _turn(right, c, s, E)
            else:
                k_s[at, :] = _turn(left, c, s)
                v_s[at, :] = right
                vt_s[:HEAD, at] = right.T

    normed = lambda l: _local(o, a_o.at[l], sem.at[2])

    def attend(l, iq):
        at = _at(iq, B)
        _when((l == FIRST) & (iq == 3), lambda: G(FIRST).forward(), lambda: N(FIRST).start(), lambda: O(FIRST).last())
        _when((l == LAST) & (iq == 2), lambda: G(LAST).forward())
        _when((l == LAST) & (iq == 3), lambda: N(LAST).forward())
        _flash_fwd(iq, qh, k_s, vt_s, top_s, mix_s, (s0, s1), (m0, m1))
        _when(iq == 0, lambda: normed(l).wait())
        lines = []
        for n in range(HEADS):
            total = mix_s[n, HEAD : HEAD + 1, :]
            o[at, n * HEAD : (n + 1) * HEAD] = (mix_s[n, :HEAD, :] * (1 / total)).astype(BF).T
            rest = -(top_s[n] + jnp.log2(total))
            for _ in range(SPLITS):
                part = rest.astype(BF).astype(F32)
                lines.append(part)
                rest = rest - part
        lines.append(jnp.zeros((HEAD - SPLITS * HEADS, B), F32))
        la[at, :] = jnp.concatenate(lines, 0).astype(BF).T

    def merge(l, r):
        at = _at(r, B)
        _when((l == FIRST) & (r == 1), lambda: G(FIRST).last())
        out = _mm(o[at, :], w_s[l, :, QKV:]).astype(BF)
        hm[at, :] = (h[at, :].astype(F32) + out.astype(F32)).astype(BF)

    def saved(i):
        slot, at, cols, quarter = lax.rem(i, 2), _at(lax.div(i, 2), B), _at(lax.rem(i, 2), HALF), _at(i, H)
        pairs = ((up_s.at[slot], s_o.at[at, cols]), (dn_s.at[slot], r_o.at[at, cols]), (bt_s.at[slot], bt_o.at[:, quarter]), (hid.at[at, cols], hid_o.at[at, cols]))
        return [_local(a, b, out_sem.at[slot, i]) for i, (a, b) in enumerate(pairs)]

    wide = _local(wd_o.at[FIRST], wd_s, sem.at[1])

    def widen(i):
        half, at = lax.rem(i, 2), _at(lax.div(i, 2), B)
        trio = lambda do: [lambda g=g: do(g(LAST)) for g in (A, K, O)]
        _when(i == 1, lambda: N(FIRST).forward(), *trio(_Gather.start), lambda: G(LAST).load())
        _when(i == 4, lambda: N(FIRST).last())
        _when(i == 6, lambda: N(FIRST).finish(), lambda: wide.start(), lambda: N(LAST).load())
        _when(i == 7, *trio(_Gather.forward), lambda: G(LAST).start())
        _when(i > 1, lambda: _wait(saved(i - 2)))

        @pl.when(half == 0)
        def _():
            _norm_to(a_s, slice(None), hm, at)

        bt_s[half] = a_s[_at(half, H), :].T
        ahead = None
        for c in range(0, HALF + W, W):
            now = ahead
            if c < HALF:
                at_gate, at_up = (pl.ds(pl.multiple_of(half * HALF + k + c, W), W) for k in (0, FF))
                ahead = _mm(a_s[:], wgu_s[:, at_gate]), _mm(a_s[:], wgu_s[:, at_up])
            if now is not None:
                cols = slice(c - W, c)
                gate, up = now
                sig = jax.nn.sigmoid(gate)
                silu = gate * sig
                up_s[half, :, cols] = silu
                dn_s[half, :, cols] = up * (sig + silu * (1 - sig))
                hid[at, pl.ds(pl.multiple_of(half * HALF + c - W, W), W)] = (silu * up).astype(BF)
        _start(saved(i))

    def narrow(r):
        at = _at(r, B)
        _when(r == 2, *[lambda g=g: g(LAST).last() for g in (A, K, O)], lambda: N(LAST).start())
        out = _mm(hid[at, :], wd_s[:]).astype(BF)
        h[at, :] = (hm[at, :].astype(F32) + out.astype(F32)).astype(BF)

    def layer(l):
        _loop(blocks, lambda r: project(l, r, 0))
        _when(l == FIRST, lambda: K(FIRST).finish())
        _start([normed(l)])
        _loop(blocks, lambda r: project(l, r, 2))
        pairs = ((qh, q_o), (k_s, k_o), (v_s, v_o), (w_s.at[l], wa_o), (o, o_o), (la, la_o), (hm, hm_o))
        outs = [_local(a, b.at[l], sem.at[3 + i]) for i, (a, b) in enumerate(pairs)]
        _start(outs[:3])
        _when(l == FIRST, lambda: O(FIRST).forward())
        _loop(blocks, lambda iq: attend(l, iq))
        me, _ = _place()
        fetch = [_local(wgu_o.at[FIRST, at, :], wgu_s.at[at, :], load_sem.at[r]) for r, at in enumerate([_at(me ^ r, ROWS) for r in range(8)])]

        @pl.when(l == FIRST)
        def _():
            G(FIRST).early()
            _start(fetch[:6])
            O(FIRST).finish()
            for g in (A, K, O):
                g(LAST).load()

        _when(l == LAST, lambda: G(LAST).last(), lambda: _start(outs[3:6]))
        _loop(blocks, lambda r: merge(l, r))
        _when(l == LAST, lambda: N(LAST).last())
        _start(outs[6:])

        @pl.when(l == FIRST)
        def _():
            G(FIRST).late()
            _start(fetch[6:])
            _wait(fetch)
            _start(outs[3:6])
            _loop(2 * blocks, widen)
            wide.wait()
            _loop(blocks, narrow)
            for g in (A, K, O):
                g(LAST).finish()
            for n in (2, 1):
                _wait(saved(2 * blocks - n))

        _wait(outs)
        _when(l == FIRST, lambda: _start([_local(h, h1_o, sem.at[0])]))

    _loop(layers, layer)
    G(LAST).finish()
    N(LAST).finish()
    _wait([_local(h, h1_o, sem.at[0])])


def forward(x, weights):
    T, layers = x.shape[0], weights[0].shape[0]
    tables = rotary_tables(T)
    L = lambda *s, t=BF: ((layers, *s), t)
    outs = [L(T, D), L(T, D), L(HEADS, T, HEAD), L(T, HEAD), L(T, HEAD), L(T, D), L(T, HEAD), ((T, FF), F32), ((T, FF), F32), ((T, FF), BF), ((D, T), BF),
            ((T, D), BF), ((T, HEAD), F32), ((T, HEAD), F32), L(D, WA), L(D, GU), L(FF, D)]
    line = VM((1, B), F32)
    scratch = [VM((T, D), BF), VM((T, D), BF), VM((layers, D, WA), BF), VM((D, GU), BF), VM((FF, D), BF), VM((T, HEAD), F32), VM((T, HEAD), F32),
               VM((HEADS, T, HEAD), BF), VM((T, HEAD), BF), VM((T, HEAD), BF), VM((HEAD + 8, T), BF), VM((T, D), BF), VM((T, HEAD), BF), VM((B, D), BF),
               VM((HEADS, 1, B), F32), VM((HEADS, HEAD + 8, B), F32), VM((B, B), F32), VM((B, B), F32), line, line, VM((2, B, HALF), F32), VM((2, B, HALF), F32), VM((T, FF), BF), VM((2, D, H), BF),
               VM((ROWS, GU), BF), VM((FROWS, D), BF), DMA((10,)), DMA((2, 4)), DMA((8,))] + [DMA((layers, 2, 9)), DMA((layers, 5))] * 5
    small = pl.BlockSpec(memory_space=VM)
    return _call(functools.partial(_forward, layers=layers), "forward", [x, *tables, *weights], [ANY, small, small] + [ANY] * 7, outs,
                 [ANY] * len(outs), scratch, 10**11, 0)


def _mlp_back(*refs, layer, last):
    hm_i, dy_i, wgu_i, wd_i, *refs = refs
    if last:
        dhm_o, kgu, sgu, kd, sd, b_s, *refs = refs
    else:
        s_i, r_i, hid_i, bt_i, keep, send, dhm_o, kgu, sgu, kd, sd, g_o, sq_o, up_s, dn_s, *refs = refs
    hm, dy, hid_s, wgu, wd, g0, g1, bt, dyt, db, sem, part_sem, split_sem, *scatter = refs
    tokens = hm.shape[0]
    blocks, parts = tokens // B, FF // W
    pending = lambda: _Scatter([keep.at[b] for b in range(4)], [send.at[b] for b in range(4)], *scatter)

    def columns(c):
        return _at(c, W), pl.ds(pl.multiple_of(FF + c * W, W), W)

    def weights(c):
        cols, up = columns(c)
        return [(wgu_i.at[layer, :, cols], wgu.at[:, cols]), (wgu_i.at[layer, :, up], wgu.at[:, up])]

    def early(c):
        slot, cols = lax.rem(c, 2), _at(c, W)
        pairs = [(wd_i.at[layer, cols, :], wd.at[cols, :])]
        pairs += weights(c) if last else [(r_i.at[:, cols], dn_s.at[slot]), (s_i.at[:, cols], up_s.at[slot])]
        return [_local(a, b, part_sem.at[slot, i]) for i, (a, b) in enumerate(pairs)]

    def rest(c):
        slot, cols = lax.rem(c, 2), _at(c, W)
        pairs = [] if last else [(hid_i.at[:, cols], hid_s.at[slot]), *weights(c)]
        return [_local(a, b, part_sem.at[slot, 3 + i]) for i, (a, b) in enumerate(pairs)]

    spans = [_at(r, B) for r in range(blocks)]
    dys = [_local(dy_i.at[at, :], dy.at[at, :], sem.at[r]) for r, at in enumerate(spans)]
    hms = [_local(hm_i.at[layer, at, :], hm.at[at, :], sem.at[blocks + r]) for r, at in enumerate(spans)]
    flip = [] if last else [_local(bt_i, bt, sem.at[2 * blocks])]
    if last:
        _start(hms[:1] + dys[:1] + early(0) + [c for pair in zip(hms[1:], dys[1:]) for c in pair] + early(1))
    else:
        _start(dys[:1] + early(0) + dys[1:] + flip + rest(0) + early(1) + hms)
        _greet(AROUND)
        pending().start()
    db[:] = jnp.zeros(db.shape, F32)

    def widen(c, slot, r, g):
        rows = slice(r * B, (r + 1) * B)
        if last:
            gate, up = (_mm(b_s[rows, :], wgu[:, cols]) for cols in columns(c))
        t = _mt(dy[rows, :], wd[_at(c, W), :]).astype(BF).astype(F32)
        if last:
            sig = jax.nn.sigmoid(gate)
            silu = gate * sig
            hid_s[slot, rows, :] = (silu * up).astype(BF)
            slope = up * (sig + silu * (1 - sig))
        else:
            silu, slope = up_s[slot, rows, :], dn_s[slot, rows, :]
        g[rows, :W] = (t * slope).astype(BF)
        g[rows, W:] = (t * silu).astype(BF)

    for r in range(blocks + 1):
        if r < blocks:
            rows = slice(r * B, (r + 1) * B)
            _wait([*hms[r : r + last], dys[r]])
            if r == 0:
                _wait(early(0))
            if last:
                _norm_to(b_s, rows, hm, rows)
                bt[:, rows] = b_s[rows, :].T
            dyt[:, rows] = dy[rows, :].T
        if r > 0:
            widen(0, 0, r - 1, g0)
    _wait(flip)

    def step(c, slot, g, later):
        cols, up = columns(c)
        after = jnp.minimum(c + 1, parts - 1)
        _when(c + 2 < parts, lambda: _start(early(c + 2)))
        _when(c + 1 < parts, lambda: _start(rest(c + 1)), lambda: _wait(early(c + 1)))
        _wait(rest(c))
        for r in range(blocks):
            widen(after, 1 - slot, r, later)
        both = jnp.concatenate([wgu[:, cols], wgu[:, up]], 1)
        for r in range(blocks):
            rows = slice(r * B, (r + 1) * B)
            db[rows, :] += _mt(g[rows, :], both)
        dw = _mm(bt[:], g[:]).astype(BF)
        wgu[:, cols] = dw[:, :W]
        wgu[:, up] = dw[:, W:]
        wd[cols, :] = _mm(dyt[:], hid_s[slot]).astype(BF).T
        if not last:
            _when(c == 1, lambda: pending().forward())
            _when(c == 4, lambda: pending().pass_on())

    def two(u):
        step(2 * u, 0, g0, g1)
        step(2 * u + 1, 1, g1, g0)

    _loop(parts // 2, two)
    copies = _split_out(wgu, ROWS, kgu, sgu, split_sem.at[0]) + _split_out(wd, FROWS, kd, sd, split_sem.at[1])
    if not last:
        _wait(hms)
    out = lambda r: _local(hm.at[_at(r, B), :], dhm_o.at[_at(r, B), :], sem.at[r])

    def back(r):
        at = _at(r, B)
        hm[at, :] = _norm_back(hm[at, :], db[at, :].astype(BF), dy[at, :])
        out(r).start()

    _loop(blocks, back)
    if not last:
        sq_o[:] = pending().finish(g_o)
    _wait(copies + [out(r) for r in range(blocks)])


WHOLE = pl.BlockSpec(memory_space=VM)


def mlp_back(saved, dy, layer, pending, talks):
    T = dy.shape[0]
    last = pending is None
    gu, d = ((4, ROWS, GU), BF), ((4, FROWS, D), BF)
    args = [saved["hm"], dy, saved["wgu"], saved["wd"]]
    outs, out_specs = [((T, D), BF), gu, gu, d, d], [ANY] * 5
    scratch = [VM((T, D), BF), VM((T, D), BF), VM((2, T, W), BF), VM((D, GU), BF), VM((FF, D), BF), VM((T, 2 * W), BF), VM((T, 2 * W), BF),
               VM((D, T), BF), VM((D, T), BF), VM((T, D), F32), DMA((9,)), DMA((2, 6)), DMA((2, 2, 4))]
    if last:
        scratch = [VM((T, D), BF)] + scratch
    else:
        args += [saved[n] for n in ("s", "r", "hid", "bt")] + pending
        outs += [((ROWS, WA), BF), ((8, HEAD), F32)]
        out_specs += [WHOLE, WHOLE]
        scratch = [VM((2, T, W), F32), VM((2, T, W), F32)] + scratch + _scatter_scratch(ROWS, WA)
    return _call(functools.partial(_mlp_back, layer=layer, last=last), "mlp_back", args, [ANY] * len(args), outs, out_specs, scratch, 4 * 10**10, talks)


def _flash_back(iq, qh, qt, doh, dot, la, dl, zs, k_s, v_s, dq, dkt, dvt, p_s, x_s):
    def give(slot, count, s, d, edge=B):
        for e in range(0, count, HEAD):
            cols = slice(e, e + HEAD)
            for r in range(0, B, H):
                rows = slice(r, r + H)
                p = jnp.exp2(s[rows, cols])
                if e >= edge:
                    p = jnp.where(_hidden(p.shape, edge - e, 0), 0.0, p)
                p_s[slot][rows, cols] = p.astype(BF)
                x_s[slot][rows, cols] = (p * d[rows, cols]).astype(BF)

    def weigh_half(m, half, slot):
        rows, keys = pl.ds(pl.multiple_of(iq * B + half * H, H), H), pl.ds(pl.multiple_of(iq * B, B), H + half * H)
        pair = (2 * m, 2 * m + 1)
        q = jnp.concatenate([jnp.concatenate([qh[n, rows, :], la[rows, :] * zs[n, :H, :]], 1) for n in pair], 0)
        do = jnp.concatenate([jnp.concatenate([doh[n, rows, :], dl[rows, :] * zs[n, :H, :]], 1) for n in pair], 0)
        z = zs[HEADS, : H + half * H, :]
        s = _mt(q, jnp.concatenate([k_s[keys, :], z], 1))
        d = _mt(do, jnp.concatenate([v_s[keys, :], z], 1))
        give(slot, H + half * H, s, d, half * H)

    def rest_half(m, half, slot):
        rows, keys = pl.ds(pl.multiple_of(iq * B + half * H, H), H), pl.ds(pl.multiple_of(iq * B, B), H + half * H)
        pair = (2 * m, 2 * m + 1)
        p, x = p_s[slot][:, : H + half * H], x_s[slot][:, : H + half * H]
        dvt[:, keys] += _mm(jnp.concatenate([dot[n, :, rows] for n in pair], 1), p)
        dkt[:, keys] += _mm(jnp.concatenate([qt[n, :, rows] for n in pair], 1), x)
        g = _mm(x, k_s[keys, :])
        for i, n in enumerate(pair):
            dq[n, half * H : (half + 1) * H, :] = g[i * H : (i + 1) * H, :]

    _halves(weigh_half, rest_half)

    @pl.when(iq > 0)
    def _():
        rows = _at(iq, B)

        def weigh(j, n, slot):
            keys = _at(j, B)
            s = _mt(jnp.concatenate([qh[n, rows, :], la[rows, :]], 1), jnp.concatenate([k_s[keys, :], zs[n]], 1))
            d = _mt(jnp.concatenate([doh[n, rows, :], dl[rows, :]], 1), jnp.concatenate([v_s[keys, :], zs[n]], 1))
            give(slot, B, s, d)

        def rest(j, n, slot):
            keys = _at(j, B)
            dvt[:, keys] += _mm(dot[n, :, rows], p_s[slot][:])
            dkt[:, keys] += _mm(qt[n, :, rows], x_s[slot][:])
            dq[n] += _mm(x_s[slot][:], k_s[keys, :])

        _pairs(PAIRS * iq, weigh, rest)


def _attn_back(*refs, layer, count):
    first = layer == FIRST
    dhm_i, h_i, a_i, q_i, k_i, v_i, o_i, la_i, cos_i, sin_i, wa_i, kgu, sgu, kd, sd, *refs = refs
    if first:
        sq_a, sq_b, ggu_o, gd_o, ga_o, factor_o, *refs = refs
    else:
        ggu_o, gd_o, sq_o, dh_o, keep_o, send_o, *refs = refs
    (dhm, h, qh, k_s, v_s, o, la, cos, sin, wa, doh, dqkv, a_s, qt, dot, dl, zs, dq, dkt, dvt, p0, p1, x0, x1, sem, split_sem, *refs) = refs
    scatter_gu, scatter_d, refs = refs[:5], refs[5:10], refs[10:]
    tokens = h.shape[0]
    blocks = tokens // B
    pending = lambda: [_Scatter([a.at[b] for b in range(4)], [c.at[b] for b in range(4)], *s) for a, c, s in ((kgu, sgu, scatter_gu), (kd, sd, scatter_d))]

    def piece(i, a, b):
        return _local(a, b, sem.at[i])

    wo = piece(0, wa_i.at[layer, :, pl.ds(QKV, D)], wa.at[:, pl.ds(QKV, D)])
    groups = []
    for r in range(blocks):
        at = _at(r, B)
        pairs = ((dhm_i.at[at, :], dhm.at[at, :]), (q_i.at[layer, :, at, :], qh.at[:, at, :]), (o_i.at[layer, at, :], o.at[at, :]))
        groups.append([piece(1 + 3 * r + i, a, b) for i, (a, b) in enumerate(pairs)])
    pairs = [(la_i.at[layer], la), (k_i.at[layer], k_s), (v_i.at[layer], v_s), (cos_i, cos), (sin_i, sin), (a_i.at[layer], a_s)]
    if not first:
        pairs += [(h_i, h), (wa_i.at[layer, :, pl.ds(0, QKV)], wa.at[:, pl.ds(0, QKV)])]
    late = [piece(1 + 3 * blocks + i, a, b) for i, (a, b) in enumerate(pairs)]
    _start([wo] + sum(groups, []) + late)
    _greet(range(1, 8) if first else AROUND)
    for s in pending():
        s.start()
    dkt[:] = jnp.zeros(dkt.shape, F32)
    dvt[:] = jnp.zeros(dvt.shape, F32)
    lane = lax.broadcasted_iota(jnp.int32, (1, HEAD), 1)
    for n in range(HEADS + 1):
        ours = lax.div(lane, SPLITS) == n if n < HEADS else lane < SPLITS * HEADS
        zs[n] = jnp.broadcast_to(ours.astype(F32).astype(BF), (B, HEAD))
    wo.wait()

    def lead(r):
        at = _at(r, B)
        columns = lambda m: _mt(dhm[at, :], wa[m * W : (m + 1) * W, QKV:]).astype(BF)
        ahead = columns(0)
        means = jnp.zeros((B, HEAD), F32)
        for n in range(HEADS):
            if n % 2 == 0:
                do = ahead
                if n + 2 < HEADS:
                    ahead = columns(n // 2 + 1)
            by = do[:, n % 2 * HEAD : (n % 2 + 1) * HEAD]
            doh[n, at, :] = by
            dot[n, :, at] = by.T
            qt[n, :, at] = qh[n, at, :].T
            mean = jnp.sum(by.astype(F32) * o[at, n * HEAD : (n + 1) * HEAD].astype(F32), -1, keepdims=True)
            means = jnp.where(lax.div(lane, SPLITS) == n, -mean, means)
        high = means.astype(BF).astype(F32)
        middle = (means - high).astype(BF).astype(F32)
        parts = jnp.where(lax.rem(lane, SPLITS) == 1, middle, means - high - middle)
        dl[at, :] = jnp.where(lax.rem(lane, SPLITS) == 0, high, parts).astype(BF)

    def begin(r):
        for k in range(blocks):
            _when(r == k, lambda: _wait(groups[k]))
        lead(r)

    _loop(blocks, begin)
    for s in pending():
        s.forward()
    wa[:, QKV:] = _tm(o[:], dhm[:]).astype(BF)
    if first:
        own = [_Scatter(*[_blocks(wa.at[:, cols], ROWS, k) for k in range(2)], *s) for cols, s in
               ((pl.ds(QKV, D), refs[:4]), (pl.ds(0, QKV), [scatter_gu[0].at[:, :, pl.ds(0, QKV)], *refs[4:7]]))]
        own[0].start()
    _wait(late)

    def attend(g):
        iq = blocks - 1 - g
        at = _at(iq, B)
        _when(g == 2, *[lambda s=s: s.pass_on() for s in pending()])
        if first:
            _when(g == 1, lambda: own[0].forward())
            _when(g == 2, lambda: own[0].pass_on())
        _flash_back(iq, qh, qt, doh, dot, la, dl, zs, k_s, v_s, dq, dkt, dvt, (p0, p1), (x0, x1))
        c, s = cos[at, :], sin[at, :]

        def turn(m):
            for n in (2 * m, 2 * m + 1):
                dqkv[at, _at(n, HEAD)] = _turn_back(dq[n] * SCALE, c, s)

        _loop(PAIRS, turn)
        dqkv[at, D : D + HEAD] = _turn_back((dkt[:, at] * (SCALE / E)).T, c, s)
        dqkv[at, D + HEAD :] = dvt[:, at].T.astype(BF)

    _loop(blocks, attend)
    dw = lambda: wa.__setitem__((slice(None), slice(0, QKV)), _tm(a_s[:], dqkv[:]).astype(BF))
    if first:
        dw()
        mine, all_s, all_sem = refs[7:]
        own[1].start()
        gu, d = pending()
        squares = gu.finish(ggu_o) + d.finish(gd_o) + sq_a[:] + sq_b[:]
        own[1].forward()
        squares += own[0].finish(ga_o.at[:, pl.ds(QKV, D)])
        own[1].pass_on()
        mine[:] = own[1].finish(ga_o.at[:, pl.ds(0, QKV)]) + squares
        me, _ = _place()
        copies = [_remote(mine, all_s.at[me], all_sem, r, r) for r in range(1, 8)]
        _start(copies)
        all_s[me] = mine[:]
        _wait(copies)
        total = jnp.sum(jnp.sum(jnp.sum(all_s[:], axis=0), axis=1, keepdims=True), axis=0, keepdims=True)
        factor_o[:] = jnp.broadcast_to(jnp.minimum(1.0, 0.5 * lax.rsqrt(total / count + 1e-30)), factor_o.shape)
    else:
        out = lambda r: _local(h.at[_at(r, B), :], dh_o.at[_at(r, B), :], split_sem.at[2, r])

        def back(r):
            at = _at(r, B)
            o[at, :] = _mt(dqkv[at, :], wa[:, :QKV]).astype(BF)
            h[at, :] = _norm_back(h[at, :], o[at, :], dhm[at, :])
            out(r).start()

        _loop(blocks, back)
        dw()
        copies = _split_out(wa, ROWS, keep_o, send_o, split_sem)
        gu, d = pending()
        sq_o[:] = gu.finish(ggu_o) + d.finish(gd_o)
        _wait(copies + [out(r) for r in range(blocks)])


def attn_back(saved, dhm, h, layer, pending, squares, count, talks):
    T = h.shape[0]
    args = [dhm, h] + [saved[n] for n in ("a", "q", "k", "v", "o", "la", "cos", "sin", "wa")] + [*pending, *squares]
    specs = [ANY] * (11 + len(pending)) + [WHOLE] * len(squares)
    dw, small = ((4, ROWS, WA), BF), ((8, HEAD), F32)
    outs, out_specs = [((ROWS, GU), BF), ((FROWS, D), BF)], [WHOLE, WHOLE]
    tile = VM((B, B), BF)
    scratch = [VM((T, D), BF), VM((T, D), BF), VM((HEADS, T, HEAD), BF), VM((T, HEAD), BF), VM((T, HEAD), BF), VM((T, D), BF), VM((T, HEAD), BF),
               VM((T, HEAD), F32), VM((T, HEAD), F32), VM((D, WA), BF), VM((HEADS, T, HEAD), BF), VM((T, QKV), BF), VM((T, D), BF),
               VM((HEADS, HEAD, T), BF), VM((HEADS, HEAD, T), BF), VM((T, HEAD), BF), VM((HEADS + 1, B, HEAD), BF), VM((HEADS, B, HEAD), F32),
               VM((HEAD, T), F32), VM((HEAD, T), F32), tile, tile, tile, tile, DMA((21,)), DMA((3, 4)),
               *_scatter_scratch(ROWS, GU), *_scatter_scratch(FROWS, D)]
    if layer == FIRST:
        outs += [((ROWS, WA), BF), small]
        out_specs += [WHOLE, WHOLE]
        scratch.append(VM((4, ROWS, D), BF))
        for width in (D, QKV):
            scratch += [VM((4, ROWS, width), BF), VM((3, ROWS, width), BF), DMA((2, 10))]
        scratch += [VM((8, HEAD), F32), VM((8, 8, HEAD), F32), DMA((2, 8))]
    else:
        outs += [small, ((T, D), BF), dw, dw]
        out_specs += [WHOLE, ANY, ANY, ANY]
    return _call(functools.partial(_attn_back, layer=layer, count=count), "attn_back", args, specs, outs, out_specs, scratch, 5 * 10**10, talks)


TRIOS = range(21)


def _adamw(*refs, layers):
    refs = iter(refs)
    take = lambda count: list(itertools.islice(refs, count))
    (factor_ref,) = take(1)
    grads = take(3 * layers)
    given, out, held = (take(len(TRIOS)) for _ in range(3))
    g_held = take(len(grads))
    load_sem, grad_sem, store_sem = refs
    factor = factor_ref[:1, :1]
    where = [(which, sum(widths[:i]), width) for which, widths in enumerate(((D, HEAD, HEAD, D), (FF, FF), (D,))) for i, width in enumerate(widths)]
    fetch = [_local(a, b, grad_sem.at[i]) for i, (a, b) in enumerate(zip(grads, g_held))]

    def moves(layer, i):
        trio = TRIOS[i::7]
        return ([_local(given[k].at[layer], held[k].at[layer], load_sem.at[layer, k]) for k in trio],
                [_local(held[k].at[layer], out[k].at[layer], store_sem.at[layer, k]) for k in trio])

    every = [(layer, i) for layer in range(layers) for i in range(7)]
    for layer, i in every:
        if where[i][1] == 0:
            fetch[3 * layer + where[i][0]].start()
        _start(moves(layer, i)[0])
    for layer, i in every:
        which, start, width = where[i]
        if start == 0:
            fetch[3 * layer + which].wait()
        loads, stores = moves(layer, i)
        _wait(loads)
        w_ref, m_ref, v_ref = (held[k].at[layer] for k in TRIOS[i::7])
        g_ref = g_held[3 * layer + which]

        def step(r):
            at = _at(r, 16)
            g = g_ref[at, start : start + width].astype(F32) * factor
            m = 0.9 * m_ref[at, :] + 0.1 * g
            v = 0.95 * v_ref[at, :] + 0.05 * g * g
            w = w_ref[at, :].astype(F32)
            w_ref[at, :] = (w - 0.02 * (m * lax.rsqrt(v + 1e-8) + 0.1 * w)).astype(BF)
            m_ref[at, :] = m
            v_ref[at, :] = v

        _loop(g_ref.shape[0] // 16, step)
        _start(stores)
    for layer, i in every:
        _wait(moves(layer, i)[1])


def adamw(factor, grads, weights, m, v):
    layers = len(grads)
    flat, given = sum(grads, []), [*weights, *m, *v]
    whole = lambda a: VM(a.shape, a.dtype)
    return _call(functools.partial(_adamw, layers=layers), "adamw", [factor, *flat, *given], [WHOLE] + [ANY] * (len(flat) + len(given)),
                 [(a.shape, a.dtype) for a in given], [ANY] * len(given),
                 [whole(a) for a in given + flat] + [DMA((layers, len(given))), DMA((len(flat),)), DMA((layers, len(given)))], 10**9, None)


def rotary_tables(tokens):
    half = HEAD // 2
    rate = THETA ** (-np.arange(half, dtype=np.float64) / half)

    def table(places):
        angle = np.concatenate([places[:, None] * rate] * 2, 1)
        return jnp.asarray(np.stack([np.cos(angle), np.sin(angle)]), F32)

    return table(np.arange(COARSE)), table(np.arange(0, tokens, COARSE))


def solution(mesh):
    def step(x, dy, *arrays):
        weights, m, v = (arrays[i : i + 7] for i in (0, 7, 14))
        x, dy = x[0], dy[0]
        names = ("a", "hm", "q", "k", "v", "o", "la", "s", "r", "hid", "bt", "h1", "cos", "sin", "wa", "wgu", "wd")
        saved = dict(zip(names, forward(x, weights)))
        count = 8 * sum(w.size for w in weights)
        by_hm, *mlp1 = mlp_back(saved, dy, LAST, None, None)
        ggu1, gd1, sq_a, by_h, *attn1 = attn_back(saved, by_hm, saved["h1"], LAST, mlp1, [], count, 1)
        by_hm, *mlp0, ga1, sq_b = mlp_back(saved, by_h, FIRST, attn1, 2)
        ggu0, gd0, ga0, factor = attn_back(saved, by_hm, x, FIRST, mlp0, [sq_a, sq_b], count, 3)
        return tuple(adamw(factor, [[ga0, ggu0, gd0], [ga1, ggu1, gd1]], weights, m, v))

    states, cut = P(("rep", "dp"), None, None), P(None, "dp", None)
    return jax.shard_map(
        step,
        mesh=mesh,
        in_specs=(states, states) + (cut,) * 21,
        out_specs=(P("rep", "dp", None),) * 21,
        check_vma=False,
    )
```

```python
import functools
import itertools

import jax
import jax.numpy as jnp
import numpy as np
from jax import lax
from jax.experimental import pallas as pl
from jax.experimental.pallas import tpu as pltpu
from jax.sharding import PartitionSpec as P

HEAD, HEADS, D, FF = 128, 6, 768, 2048
THETA = 10000
SCALE = HEAD**-0.5
E = SCALE * 1.4426950408889634
NEG = -1e30
HIDDEN = NEG + NEG
EPS = 1e-6
QKV = D + 2 * HEAD
WA = QKV + D
GU = 2 * FF
ROWS, FROWS = D // 8, FF // 8
COARSE = 64
SPLITS = 3
PAIRS = HEADS // 2
B = 512
H = B // 2
STEP = 16
W = 256
FIRST, LAST = range(2)
HALF = FF // 2
X, Y, CORE = 4, 2, 1
AROUND = (CORE, Y, X, X ^ Y)

BF, F32 = jnp.bfloat16, jnp.float32
VM = pltpu.VMEM
DMA = pltpu.SemaphoreType.DMA
MESH = pl.DeviceIdType.MESH
ANY = pl.BlockSpec(memory_space=pltpu.HBM)


def _place():
    return lax.axis_index("dp"), lax.axis_index("rep")


def _greet(bits):
    me, rep = _place()
    barrier = pltpu.get_barrier_semaphore()
    for bit in bits:
        pl.semaphore_signal(barrier, inc=1, device_id=(rep, me ^ bit), device_id_type=MESH)
    pl.semaphore_wait(barrier, len(bits))


class _Copy:
    def __init__(self, make):
        self.make = make

    def start(self):
        self.make().start()

    def wait(self):
        self.make().wait()

    def wait_send(self):
        self.make().wait_send()

    def wait_recv(self):
        self.make().wait_recv()


def _local(src, dst, sem):
    return _Copy(lambda: pltpu.make_async_copy(src, dst, sem))


def _remote(src, dst, sems, k, bit):
    me, rep = _place()
    return _Copy(lambda: pltpu.make_async_remote_copy(src_ref=src, dst_ref=dst, send_sem=sems.at[0, k], recv_sem=sems.at[1, k],
                                                      device_id=(rep, me ^ bit), device_id_type=MESH))


def _start(copies):
    for c in copies:
        c.start()


def _wait(copies):
    for c in copies:
        c.wait()


class _Gather:
    def __init__(self, parts, full, sems, local, own=None):
        me, _ = _place()
        rows = parts[0].shape[0]
        half = rows // 2

        def at(dev, first=0, count=rows):
            return full.at[pl.ds(pl.multiple_of(dev * rows + first, 16), count), :]

        ids = itertools.count()

        def copy(bit, dev, first=0, count=rows, src=None):
            return _remote(at(dev, first, count) if src is None else src, at(dev, first, count), sems, next(ids), bit)

        mine = at(me) if own is None else own
        self.loads, col = [], 0
        for k, part in enumerate(parts):
            width = part.shape[1]
            self.loads.append(_local(part, mine.at[:, pl.ds(col, width)], local.at[k]))
            col += width
        self.store = [] if own is None else [_local(own, at(me), local.at[4])]
        self.x, self.y, self.core = (copy(bit, me, src=mine) for bit in (X, Y, CORE))
        self.far = [copy(X, me ^ Y, count=half), copy(Y, me ^ X, half, half)]
        self.near = [copy(CORE, me ^ X), copy(CORE, me ^ Y)]
        self.end = [copy(CORE, me ^ X ^ Y, count=half), copy(CORE, me ^ X ^ Y, half, half)]

    def load(self):
        _start(self.loads)

    def start(self):
        _wait(self.loads)
        _start([self.x, self.y, self.core] + self.store)

    def forward(self):
        self.x.wait_recv()
        self.y.wait_recv()
        _start(self.far + self.near)

    def last(self):
        for c in self.far:
            c.wait_recv()
        _start(self.end)

    def early(self):
        for c in [self.core] + self.near:
            c.wait_recv()
        _wait(self.store)

    def late(self):
        for c in self.end:
            c.wait_recv()
        for c in [self.x, self.y, self.core] + self.far + self.near + self.end:
            c.wait_send()

    def finish(self):
        self.early()
        self.late()


def _block(xy, other):
    me, _ = _place()
    return ((me // 2) ^ xy) * 2 + ((me % 2) ^ other)


def _blocks(full, rows, other):
    return [full.at[pl.ds(pl.multiple_of(_block(xy, other) * rows, 16), rows), :] for xy in range(4)]


class _Scatter:
    def __init__(self, keep, send, kept, came, ici, sems, local=None):
        self.kept, self.came, self.ici = kept, came, ici
        self.loads = [_local(keep[b], kept.at[b], local.at[b]) for b in range(4)] if local is not None else []
        self.keep = [kept.at[b] for b in range(4)] if self.loads else keep
        ids = itertools.count()
        self.core = [_remote(send[b], came.at[b], sems, next(ids), CORE) for b in range(4)]
        half = came.shape[1] // 2
        self.ways = ((pl.ds(0, half), X, 2, Y, 1), (pl.ds(half, half), Y, 1, X, 2))
        self.first = [_remote(kept.at[b, at, :], ici.at[k, at, :], sems, next(ids), bit) for at, bit, near, _, _ in self.ways for k, b in enumerate((near, 3))]
        self.second = [_remote(kept.at[b, at, :], ici.at[2, at, :], sems, next(ids), bit) for at, _, _, bit, b in self.ways]

    def start(self):
        for b in (3, 2, 1, 0):
            _start([self.core[b]] + self.loads[b : b + 1])

    def _add(self, out, start, rows, *terms):
        def add(i):
            at = pl.ds(pl.multiple_of(start + i * STEP, STEP), STEP)
            out[at, :] = sum(t[at, :].astype(F32) for t in terms).astype(BF)

        _loop(rows // STEP, add)

    def forward(self):
        for b in (3, 2, 1):
            self.core[b].wait_recv()
            _wait(self.loads[b : b + 1])
            self._add(self.kept.at[b], 0, self.came.shape[1], self.keep[b], self.came.at[b])
        _start(self.first)

    def pass_on(self):
        half = self.came.shape[1] // 2
        for i, way in enumerate(self.ways):
            self.first[2 * i + 1].wait_recv()
            self._add(self.kept.at[way[-1]], i * half, half, self.kept.at[way[-1]], self.ici.at[1])
            self.second[i].start()

    def finish(self, g_ref):
        self.core[0].wait_recv()
        _wait(self.loads[:1])
        for c in self.first[::2] + self.second:
            c.wait_recv()
        self._add(g_ref, 0, g_ref.shape[0], self.keep[0], self.came.at[0], self.ici.at[0], self.ici.at[2])

        def square(i, squares):
            g = g_ref[_at(i, STEP), :].astype(F32)
            return squares + g[:8] * g[:8] + g[8:] * g[8:]

        squares = lax.fori_loop(0, g_ref.shape[0] // STEP, square, jnp.zeros((8, g_ref.shape[1]), F32))
        for c in self.core + self.first + self.second:
            c.wait_send()
        return sum(squares[:, c : c + HEAD] for c in range(0, g_ref.shape[1], HEAD))


def _scatter_scratch(rows, n):
    return [VM((4, rows, n), BF), VM((4, rows, n), BF), VM((3, rows, n), BF), DMA((2, 10)), DMA((4,))]


def _split_out(full, rows, keep, send, sems):
    copies = [_local(src, ref.at[b], sems.at[k, b]) for k, ref in enumerate((keep, send)) for b, src in enumerate(_blocks(full, rows, k))]
    _start(copies)
    return copies


def _dot(a, b, ca, cb):
    return lax.dot_general(a, b, (((ca,), (cb,)), ((), ())), preferred_element_type=F32)


_mm = functools.partial(_dot, ca=1, cb=0)
_mt = functools.partial(_dot, ca=1, cb=1)
_tm = functools.partial(_dot, ca=0, cb=0)


def _at(i, n):
    return pl.ds(pl.multiple_of(i * n, n), n)


def _when(cond, *todo):
    @pl.when(cond)
    def _():
        for do in todo:
            do()


def _loop(n, body):
    def step(i, _):
        body(i)

    lax.fori_loop(0, n, step, None)


def _scale(wide):
    return lax.rsqrt(jnp.mean(wide * wide, -1, keepdims=True) + EPS)


def _norm_to(out, to, h, at):
    wide = h[at, :].astype(F32)
    out[to, :] = (wide * _scale(wide)).astype(BF)


def _norm_back(h, dy, by):
    wide, dy = h.astype(F32), dy.astype(F32)
    scale = _scale(wide)
    back = scale * (dy - wide * (scale * scale * jnp.mean(dy * wide, -1, keepdims=True)))
    return (by.astype(F32) + back.astype(BF).astype(F32)).astype(BF)


def _turn(t, cos, sin, times=1):
    t = t.astype(F32)
    return ((t * cos + pltpu.roll(t, HEAD // 2, 1) * sin) * times).astype(BF)


def _turn_back(t, cos, sin):
    return (t * cos - pltpu.roll(t, HEAD // 2, 1) * sin).astype(BF)


def _call(body, name, args, specs, outs, out_specs, scratch, flops, talks):
    return pl.pallas_call(
        body,
        in_specs=specs,
        out_specs=out_specs,
        scratch_shapes=scratch,
        out_shape=[jax.ShapeDtypeStruct(*o) for o in outs],
        compiler_params=pltpu.CompilerParams(vmem_limit_bytes=67043328, collective_id=talks, has_side_effects=talks is not None),
        cost_estimate=pl.CostEstimate(flops=flops, transcendentals=0, bytes_accessed=flops // 1000),
        name=name,
    )(*args)


def _pairs(hi, first, steps):
    first(0, 0, 0)

    def body(u):
        j, m = lax.div(u, PAIRS), lax.rem(u, PAIRS)
        later = jnp.minimum(u + 1, hi - 1)
        first(j, 2 * m + 1, 1)
        steps(j, 2 * m, 0)
        first(lax.div(later, PAIRS), 2 * lax.rem(later, PAIRS), 0)
        steps(j, 2 * m + 1, 1)

    _loop(hi, body)


def _halves(first, steps):
    first(0, 1, 0)

    def body(m):
        first(m, 0, 1)
        steps(m, 1, 0)
        first(jnp.minimum(m + 1, PAIRS - 1), 1, 0)
        steps(m, 0, 1)

    _loop(PAIRS, body)


def _hidden(shape, later, queries):
    return lax.broadcasted_iota(jnp.int32, shape, 1 - queries) - later > lax.broadcasted_iota(jnp.int32, shape, queries)


def _flash_fwd(iq, qh, k_s, vt_s, top_s, mix_s, s_s, m_s):
    def mix(s, top, cols, start, count):
        got = []
        for r in range(0, count, W):
            p = jnp.exp2(s[r : r + W, cols] - top).astype(BF)
            got.append(_mm(vt_s[:, pl.ds(pl.multiple_of(start + r, W), W)], p))
        return sum(got)

    def score_half(m, half, slot):
        rows, keys = pl.ds(pl.multiple_of(iq * B + half * H, H), H), pl.ds(pl.multiple_of(iq * B, B), H + half * H)
        s = _mt(k_s[keys, :], jnp.concatenate([qh[2 * m, rows, :], qh[2 * m + 1, rows, :]], 0))
        hide = _hidden((H, H), 0, 1)
        for i in range(2):
            cols, last = slice(i * H, (i + 1) * H), slice(half * H, (half + 1) * H)
            t = jnp.where(hide, HIDDEN, s[last, cols])
            top = t.max(axis=0, keepdims=True)
            s_s[slot][last, cols] = t
            if half:
                s_s[slot][:H, cols] = s[:H, cols]
                top = jnp.maximum(top, s[:H, cols].max(axis=0, keepdims=True))
            m_s[slot][:, cols] = top

    def rest_half(m, half, slot):
        for i in range(2):
            cols, to = slice(i * H, (i + 1) * H), slice(half * H, (half + 1) * H)
            top = m_s[slot][:, cols]
            top_s[2 * m + i, :, to] = top
            mix_s[2 * m + i, :, to] = mix(s_s[slot], top, cols, iq * B, H + half * H)

    _halves(score_half, rest_half)

    @pl.when(iq > 0)
    def _():
        rows = _at(iq, B)

        def score(j, n, slot):
            s = _mt(k_s[_at(j, B), :], qh[n, rows, :])
            s_s[slot][:] = s
            m_s[slot][:] = s.max(axis=0, keepdims=True)

        def rest(j, n, slot):
            old = top_s[n]
            top = jnp.maximum(old, m_s[slot][:])
            top_s[n] = top
            keep = jnp.exp2(old - top)
            for c in range(0, B, W):
                cols = slice(c, c + W)
                mix_s[n, :, cols] = mix_s[n, :, cols] * keep[:, cols] + mix(s_s[slot], top[:, cols], cols, j * B, B)

        _pairs(PAIRS * iq, score, rest)


def _forward(x, near, far, *refs, layers):
    (wq, wk, wv, wo, wg, wu, wd, a_o, hm_o, q_o, k_o, v_o, o_o, la_o, s_o, r_o, hid_o, bt_o, h1_o, cos_o, sin_o, wa_o, wgu_o, wd_o,
     h, hm, w_s, wgu_s, wd_s, cos, sin, qh, k_s, v_s, vt_s, o, la, a_s, top_s, mix_s, s0, s1, m0, m1, up_s, dn_s, hid, bt_s,
     g_own, d_own, sem, out_sem, load_sem, hm_sem, a_sem, a_loc, k_sem, k_loc, b_sem, b_loc, g_sem, g_loc, d_sem, d_loc) = refs
    tokens = h.shape[0]
    blocks = tokens // B
    A = lambda l: _Gather([wq.at[l, :, pl.ds(0, B)]], w_s.at[l, :, pl.ds(0, B)], a_sem.at[l], a_loc.at[l])
    K = lambda l: _Gather([wq.at[l, :, pl.ds(B, W)], wk.at[l], wv.at[l]], w_s.at[l, :, pl.ds(B, B)], k_sem.at[l], k_loc.at[l])
    O = lambda l: _Gather([wo.at[l]], w_s.at[l, :, pl.ds(QKV, D)], b_sem.at[l], b_loc.at[l])
    G = lambda l: _Gather([wg.at[l], wu.at[l]], wgu_o.at[l], g_sem.at[l], g_loc.at[l], g_own)
    N = lambda l: _Gather([wd.at[l]], wd_o.at[l], d_sem.at[l], d_loc.at[l], d_own)

    load = _local(x, h, sem.at[0])
    load.start()
    for g in (A, K, O, G, N):
        g(FIRST).load()
    _greet((CORE, Y, X))
    A(FIRST).start()
    K(FIRST).start()
    near_c, near_s = near[0], near[1]
    for i in range(far.shape[1]):
        far_c, far_s = far[0, i : i + 1, :], far[1, i : i + 1, :]
        rows = slice(i * COARSE, (i + 1) * COARSE)
        cos[rows, :] = far_c * near_c - far_s * near_s
        t = far_s * near_c + far_c * near_s
        sin[rows, :] = jnp.where(lax.broadcasted_iota(jnp.int32, t.shape, 1) < HEAD // 2, -t, t)
    tables = [_local(cos, cos_o, sem.at[1]), _local(sin, sin_o, sem.at[2])]
    _start(tables)
    _wait(tables)
    vt_s[HEAD:, :] = jnp.ones((8, tokens), BF)
    A(FIRST).forward()
    K(FIRST).forward()
    O(FIRST).start()
    G(FIRST).start()
    load.wait()
    A(FIRST).last()
    K(FIRST).last()
    A(FIRST).finish()

    def project(l, r, start):
        at = _at(r, B)
        if not start:
            _norm_to(o, at, h, at)
        c, s = cos[at, :], sin[at, :]
        columns = lambda m: _mm(o[at, :], w_s[l, :, m * W : (m + 1) * W]).astype(BF)
        ahead = columns(start)
        for m in (start, start + 1):
            t = ahead
            if m == start:
                ahead = columns(m + 1)
            left, right = t[:, :HEAD], t[:, HEAD:]
            if m < PAIRS:
                qh[2 * m, at, :] = _turn(left, c, s, E)
                qh[2 * m + 1, at, :] = _turn(right, c, s, E)
            else:
                k_s[at, :] = _turn(left, c, s)
                v_s[at, :] = right
                vt_s[:HEAD, at] = right.T

    normed = lambda l: _local(o, a_o.at[l], sem.at[2])

    def attend(l, iq):
        at = _at(iq, B)
        _when((l == FIRST) & (iq == 3), lambda: G(FIRST).forward(), lambda: N(FIRST).start(), lambda: O(FIRST).last())
        _when((l == LAST) & (iq == 2), lambda: G(LAST).forward())
        _when((l == LAST) & (iq == 3), lambda: N(LAST).forward())
        _flash_fwd(iq, qh, k_s, vt_s, top_s, mix_s, (s0, s1), (m0, m1))
        _when(iq == 0, lambda: normed(l).wait())
        lines = []
        for n in range(HEADS):
            total = mix_s[n, HEAD : HEAD + 1, :]
            o[at, n * HEAD : (n + 1) * HEAD] = (mix_s[n, :HEAD, :] * (1 / total)).astype(BF).T
            rest = -(top_s[n] + jnp.log2(total))
            for _ in range(SPLITS):
                part = rest.astype(BF).astype(F32)
                lines.append(part)
                rest = rest - part
        lines.append(jnp.zeros((HEAD - SPLITS * HEADS, B), F32))
        la[at, :] = jnp.concatenate(lines, 0).astype(BF).T

    middle = lambda l, r: _local(hm.at[_at(r, B), :], hm_o.at[l, _at(r, B), :], hm_sem.at[r])

    def merge(l, r):
        at = _at(r, B)
        _when((l == FIRST) & (r == 1), lambda: G(FIRST).last())
        out = _mm(o[at, :], w_s[l, :, QKV:]).astype(BF)
        hm[at, :] = (h[at, :].astype(F32) + out.astype(F32)).astype(BF)
        middle(l, r).start()

    def saved(i):
        slot, at, cols, quarter = lax.rem(i, 2), _at(lax.div(i, 2), B), _at(lax.rem(i, 2), HALF), _at(i, H)
        pairs = ((up_s.at[slot], s_o.at[at, cols]), (dn_s.at[slot], r_o.at[at, cols]), (bt_s.at[slot], bt_o.at[:, quarter]), (hid.at[at, cols], hid_o.at[at, cols]))
        return [_local(a, b, out_sem.at[slot, i]) for i, (a, b) in enumerate(pairs)]

    wide = _local(wd_o.at[FIRST], wd_s, sem.at[1])

    def widen(i):
        half, at = lax.rem(i, 2), _at(lax.div(i, 2), B)
        trio = lambda do: [lambda g=g: do(g(LAST)) for g in (A, K, O)]
        _when(i == 1, lambda: N(FIRST).forward(), *trio(_Gather.start), lambda: G(LAST).load())
        _when(i == 4, lambda: N(FIRST).last())
        _when(i == 6, lambda: N(FIRST).finish(), lambda: wide.start(), lambda: N(LAST).load())
        _when(i == 7, *trio(_Gather.forward), lambda: G(LAST).start())
        _when(i > 1, lambda: _wait(saved(i - 2)))

        @pl.when(half == 0)
        def _():
            _norm_to(a_s, slice(None), hm, at)

        bt_s[half] = a_s[_at(half, H), :].T
        ahead = None
        for c in range(0, HALF + W, W):
            now = ahead
            if c < HALF:
                at_gate, at_up = (pl.ds(pl.multiple_of(half * HALF + k + c, W), W) for k in (0, FF))
                ahead = _mm(a_s[:], wgu_s[:, at_gate]), _mm(a_s[:], wgu_s[:, at_up])
            if now is not None:
                cols = slice(c - W, c)
                gate, up = now
                sig = jax.nn.sigmoid(gate)
                silu = gate * sig
                up_s[half, :, cols] = silu
                dn_s[half, :, cols] = up * (sig + silu * (1 - sig))
                hid[at, pl.ds(pl.multiple_of(half * HALF + c - W, W), W)] = (silu * up).astype(BF)
        _start(saved(i))

    def narrow(r):
        at = _at(r, B)
        _when(r == 2, *[lambda g=g: g(LAST).last() for g in (A, K, O)], lambda: N(LAST).start())
        out = _mm(hid[at, :], wd_s[:]).astype(BF)
        h[at, :] = (hm[at, :].astype(F32) + out.astype(F32)).astype(BF)

    def layer(l):
        _loop(blocks, lambda r: project(l, r, 0))
        _when(l == FIRST, lambda: K(FIRST).finish())
        _start([normed(l)])
        _loop(blocks, lambda r: project(l, r, 2))
        pairs = ((qh, q_o), (k_s, k_o), (v_s, v_o), (w_s.at[l], wa_o), (o, o_o), (la, la_o))
        outs = [_local(a, b.at[l], sem.at[3 + i]) for i, (a, b) in enumerate(pairs)]
        _start(outs[:3])
        _when(l == FIRST, lambda: O(FIRST).forward())
        _loop(blocks, lambda iq: attend(l, iq))
        me, _ = _place()
        fetch = [_local(wgu_o.at[FIRST, at, :], wgu_s.at[at, :], load_sem.at[r]) for r, at in enumerate([_at(me ^ r, ROWS) for r in range(8)])]

        @pl.when(l == FIRST)
        def _():
            G(FIRST).early()
            _start(fetch[:6])
            O(FIRST).finish()
            for g in (A, K, O):
                g(LAST).load()

        _when(l == LAST, lambda: G(LAST).last(), lambda: _start(outs[3:6]))
        _loop(blocks, lambda r: merge(l, r))
        _when(l == LAST, lambda: N(LAST).last())

        @pl.when(l == FIRST)
        def _():
            G(FIRST).late()
            _start(fetch[6:])
            _wait(fetch)
            _start(outs[3:6])
            _loop(2 * blocks, widen)
            wide.wait()
            _loop(blocks, narrow)
            for g in (A, K, O):
                g(LAST).finish()
            for n in (2, 1):
                _wait(saved(2 * blocks - n))

        _wait(outs + [middle(l, r) for r in range(blocks)])
        _when(l == FIRST, lambda: _start([_local(h, h1_o, sem.at[0])]))

    _loop(layers, layer)
    G(LAST).finish()
    N(LAST).finish()
    _wait([_local(h, h1_o, sem.at[0])])


def forward(x, weights):
    T, layers = x.shape[0], weights[0].shape[0]
    tables = rotary_tables(T)
    L = lambda *s, t=BF: ((layers, *s), t)
    outs = [L(T, D), L(T, D), L(HEADS, T, HEAD), L(T, HEAD), L(T, HEAD), L(T, D), L(T, HEAD), ((T, FF), F32), ((T, FF), F32), ((T, FF), BF), ((D, T), BF),
            ((T, D), BF), ((T, HEAD), F32), ((T, HEAD), F32), L(D, WA), L(D, GU), L(FF, D)]
    line = VM((1, B), F32)
    scratch = [VM((T, D), BF), VM((T, D), BF), VM((layers, D, WA), BF), VM((D, GU), BF), VM((FF, D), BF), VM((T, HEAD), F32), VM((T, HEAD), F32),
               VM((HEADS, T, HEAD), BF), VM((T, HEAD), BF), VM((T, HEAD), BF), VM((HEAD + 8, T), BF), VM((T, D), BF), VM((T, HEAD), BF), VM((B, D), BF),
               VM((HEADS, 1, B), F32), VM((HEADS, HEAD + 8, B), F32), VM((B, B), F32), VM((B, B), F32), line, line, VM((2, B, HALF), F32), VM((2, B, HALF), F32), VM((T, FF), BF), VM((2, D, H), BF),
               VM((ROWS, GU), BF), VM((FROWS, D), BF), DMA((10,)), DMA((2, 4)), DMA((8,)), DMA((T // B,))] + [DMA((layers, 2, 9)), DMA((layers, 5))] * 5
    small = pl.BlockSpec(memory_space=VM)
    return _call(functools.partial(_forward, layers=layers), "forward", [x, *tables, *weights], [ANY, small, small] + [ANY] * 7, outs,
                 [ANY] * len(outs), scratch, 10**11, 0)


def _mlp_back(*refs, layer, last):
    hm_i, dy_i, wgu_i, wd_i, *refs = refs
    if last:
        dhm_o, kgu, sgu, kd, sd, b_s, *refs = refs
    else:
        s_i, r_i, hid_i, bt_i, keep, send, dhm_o, kgu, sgu, kd, sd, g_o, sq_o, up_s, dn_s, *refs = refs
    hm, dy, hid_s, wgu, wd, g0, g1, bt, dyt, db, sem, part_sem, split_sem, *scatter = refs
    tokens = hm.shape[0]
    blocks, parts = tokens // B, FF // W
    pending = lambda: _Scatter([keep.at[b] for b in range(4)], [send.at[b] for b in range(4)], *scatter)

    def columns(c):
        return _at(c, W), pl.ds(pl.multiple_of(FF + c * W, W), W)

    def weights(c):
        cols, up = columns(c)
        return [(wgu_i.at[layer, :, cols], wgu.at[:, cols]), (wgu_i.at[layer, :, up], wgu.at[:, up])]

    def early(c):
        slot, cols = lax.rem(c, 2), _at(c, W)
        pairs = [(wd_i.at[layer, cols, :], wd.at[cols, :])]
        pairs += weights(c) if last else [(r_i.at[:, cols], dn_s.at[slot]), (s_i.at[:, cols], up_s.at[slot])]
        return [_local(a, b, part_sem.at[slot, i]) for i, (a, b) in enumerate(pairs)]

    def rest(c):
        slot, cols = lax.rem(c, 2), _at(c, W)
        pairs = [] if last else [(hid_i.at[:, cols], hid_s.at[slot]), *weights(c)]
        return [_local(a, b, part_sem.at[slot, 3 + i]) for i, (a, b) in enumerate(pairs)]

    spans = [_at(r, B) for r in range(blocks)]
    dys = [_local(dy_i.at[at, :], dy.at[at, :], sem.at[r]) for r, at in enumerate(spans)]
    hms = [_local(hm_i.at[layer, at, :], hm.at[at, :], sem.at[blocks + r]) for r, at in enumerate(spans)]
    flip = [] if last else [_local(bt_i, bt, sem.at[2 * blocks])]
    if last:
        _start(hms[:1] + dys[:1] + early(0) + [c for pair in zip(hms[1:], dys[1:]) for c in pair] + early(1))
    else:
        _start(dys[:1] + early(0) + dys[1:] + flip + rest(0) + early(1) + hms)
        _greet(AROUND)
        pending().start()
    db[:] = jnp.zeros(db.shape, F32)

    def widen(c, slot, r, g):
        rows = slice(r * B, (r + 1) * B)
        if last:
            gate, up = (_mm(b_s[rows, :], wgu[:, cols]) for cols in columns(c))
        t = _mt(dy[rows, :], wd[_at(c, W), :]).astype(BF).astype(F32)
        if last:
            sig = jax.nn.sigmoid(gate)
            silu = gate * sig
            hid_s[slot, rows, :] = (silu * up).astype(BF)
            slope = up * (sig + silu * (1 - sig))
        else:
            silu, slope = up_s[slot, rows, :], dn_s[slot, rows, :]
        g[rows, :W] = (t * slope).astype(BF)
        g[rows, W:] = (t * silu).astype(BF)

    for r in range(blocks + 1):
        if r < blocks:
            rows = slice(r * B, (r + 1) * B)
            _wait([*hms[r : r + last], dys[r]])
            if r == 0:
                _wait(early(0))
            if last:
                _norm_to(b_s, rows, hm, rows)
                bt[:, rows] = b_s[rows, :].T
            dyt[:, rows] = dy[rows, :].T
        if r > 0:
            widen(0, 0, r - 1, g0)
    _wait(flip)

    def step(c, slot, g, later):
        cols, up = columns(c)
        after = jnp.minimum(c + 1, parts - 1)
        _when(c + 2 < parts, lambda: _start(early(c + 2)))
        _when(c + 1 < parts, lambda: _start(rest(c + 1)), lambda: _wait(early(c + 1)))
        _wait(rest(c))
        for r in range(blocks):
            widen(after, 1 - slot, r, later)
        both = jnp.concatenate([wgu[:, cols], wgu[:, up]], 1)
        for r in range(blocks):
            rows = slice(r * B, (r + 1) * B)
            db[rows, :] += _mt(g[rows, :], both)
        dw = _mm(bt[:], g[:]).astype(BF)
        wgu[:, cols] = dw[:, :W]
        wgu[:, up] = dw[:, W:]
        wd[cols, :] = _mm(dyt[:], hid_s[slot]).astype(BF).T
        if not last:
            _when(c == 1, lambda: pending().forward())
            _when(c == 4, lambda: pending().pass_on())

    def two(u):
        step(2 * u, 0, g0, g1)
        step(2 * u + 1, 1, g1, g0)

    _loop(parts // 2, two)
    copies = _split_out(wgu, ROWS, kgu, sgu, split_sem.at[0]) + _split_out(wd, FROWS, kd, sd, split_sem.at[1])
    if not last:
        _wait(hms)
    out = lambda r: _local(hm.at[_at(r, B), :], dhm_o.at[_at(r, B), :], sem.at[r])

    def back(r):
        at = _at(r, B)
        hm[at, :] = _norm_back(hm[at, :], db[at, :].astype(BF), dy[at, :])
        out(r).start()

    _loop(blocks, back)
    if not last:
        sq_o[:] = pending().finish(g_o)
    _wait(copies + [out(r) for r in range(blocks)])


WHOLE = pl.BlockSpec(memory_space=VM)


def mlp_back(saved, dy, layer, pending, talks):
    T = dy.shape[0]
    last = pending is None
    gu, d = ((4, ROWS, GU), BF), ((4, FROWS, D), BF)
    args = [saved["hm"], dy, saved["wgu"], saved["wd"]]
    outs, out_specs = [((T, D), BF), gu, gu, d, d], [ANY] * 5
    scratch = [VM((T, D), BF), VM((T, D), BF), VM((2, T, W), BF), VM((D, GU), BF), VM((FF, D), BF), VM((T, 2 * W), BF), VM((T, 2 * W), BF),
               VM((D, T), BF), VM((D, T), BF), VM((T, D), F32), DMA((9,)), DMA((2, 6)), DMA((2, 2, 4))]
    if last:
        scratch = [VM((T, D), BF)] + scratch
    else:
        args += [saved[n] for n in ("s", "r", "hid", "bt")] + pending
        outs += [((ROWS, WA), BF), ((8, HEAD), F32)]
        out_specs += [WHOLE, WHOLE]
        scratch = [VM((2, T, W), F32), VM((2, T, W), F32)] + scratch + _scatter_scratch(ROWS, WA)
    return _call(functools.partial(_mlp_back, layer=layer, last=last), "mlp_back", args, [ANY] * len(args), outs, out_specs, scratch, 4 * 10**10, talks)


def _flash_back(iq, qh, qt, doh, dot, la, dl, zs, k_s, v_s, dq, dkt, dvt, p_s, x_s):
    def give(slot, count, s, d, edge=B):
        for e in range(0, count, HEAD):
            cols = slice(e, e + HEAD)
            for r in range(0, B, H):
                rows = slice(r, r + H)
                p = jnp.exp2(s[rows, cols])
                if e >= edge:
                    p = jnp.where(_hidden(p.shape, edge - e, 0), 0.0, p)
                p_s[slot][rows, cols] = p.astype(BF)
                x_s[slot][rows, cols] = (p * d[rows, cols]).astype(BF)

    def weigh_half(m, half, slot):
        rows, keys = pl.ds(pl.multiple_of(iq * B + half * H, H), H), pl.ds(pl.multiple_of(iq * B, B), H + half * H)
        pair = (2 * m, 2 * m + 1)
        q = jnp.concatenate([jnp.concatenate([qh[n, rows, :], la[rows, :] * zs[n, :H, :]], 1) for n in pair], 0)
        do = jnp.concatenate([jnp.concatenate([doh[n, rows, :], dl[rows, :] * zs[n, :H, :]], 1) for n in pair], 0)
        z = zs[HEADS, : H + half * H, :]
        s = _mt(q, jnp.concatenate([k_s[keys, :], z], 1))
        d = _mt(do, jnp.concatenate([v_s[keys, :], z], 1))
        give(slot, H + half * H, s, d, half * H)

    def rest_half(m, half, slot):
        rows, keys = pl.ds(pl.multiple_of(iq * B + half * H, H), H), pl.ds(pl.multiple_of(iq * B, B), H + half * H)
        pair = (2 * m, 2 * m + 1)
        p, x = p_s[slot][:, : H + half * H], x_s[slot][:, : H + half * H]
        dvt[:, keys] += _mm(jnp.concatenate([dot[n, :, rows] for n in pair], 1), p)
        dkt[:, keys] += _mm(jnp.concatenate([qt[n, :, rows] for n in pair], 1), x)
        g = _mm(x, k_s[keys, :])
        for i, n in enumerate(pair):
            dq[n, half * H : (half + 1) * H, :] = g[i * H : (i + 1) * H, :]

    _halves(weigh_half, rest_half)

    @pl.when(iq > 0)
    def _():
        rows = _at(iq, B)

        def weigh(j, n, slot):
            keys = _at(j, B)
            s = _mt(jnp.concatenate([qh[n, rows, :], la[rows, :]], 1), jnp.concatenate([k_s[keys, :], zs[n]], 1))
            d = _mt(jnp.concatenate([doh[n, rows, :], dl[rows, :]], 1), jnp.concatenate([v_s[keys, :], zs[n]], 1))
            give(slot, B, s, d)

        def rest(j, n, slot):
            keys = _at(j, B)
            dvt[:, keys] += _mm(dot[n, :, rows], p_s[slot][:])
            dkt[:, keys] += _mm(qt[n, :, rows], x_s[slot][:])
            dq[n] += _mm(x_s[slot][:], k_s[keys, :])

        _pairs(PAIRS * iq, weigh, rest)


def _attn_back(*refs, layer, count):
    first = layer == FIRST
    dhm_i, h_i, a_i, q_i, k_i, v_i, o_i, la_i, cos_i, sin_i, wa_i, kgu, sgu, kd, sd, *refs = refs
    if first:
        sq_a, sq_b, ggu_o, gd_o, ga_o, factor_o, *refs = refs
    else:
        ggu_o, gd_o, sq_o, dh_o, keep_o, send_o, *refs = refs
    (dhm, h, qh, k_s, v_s, o, la, cos, sin, wa, doh, dqkv, a_s, qt, dot, dl, zs, dq, dkt, dvt, p0, p1, x0, x1, sem, split_sem, *refs) = refs
    scatter_gu, scatter_d, refs = refs[:5], refs[5:10], refs[10:]
    tokens = h.shape[0]
    blocks = tokens // B
    pending = lambda: [_Scatter([a.at[b] for b in range(4)], [c.at[b] for b in range(4)], *s) for a, c, s in ((kgu, sgu, scatter_gu), (kd, sd, scatter_d))]

    def piece(i, a, b):
        return _local(a, b, sem.at[i])

    wo = piece(0, wa_i.at[layer, :, pl.ds(QKV, D)], wa.at[:, pl.ds(QKV, D)])
    groups = []
    for r in range(blocks):
        at = _at(r, B)
        pairs = ((dhm_i.at[at, :], dhm.at[at, :]), (q_i.at[layer, :, at, :], qh.at[:, at, :]), (o_i.at[layer, at, :], o.at[at, :]))
        groups.append([piece(1 + 3 * r + i, a, b) for i, (a, b) in enumerate(pairs)])
    pairs = [(la_i.at[layer], la), (k_i.at[layer], k_s), (v_i.at[layer], v_s), (cos_i, cos), (sin_i, sin), (a_i.at[layer], a_s)]
    if not first:
        pairs += [(h_i, h), (wa_i.at[layer, :, pl.ds(0, QKV)], wa.at[:, pl.ds(0, QKV)])]
    late = [piece(1 + 3 * blocks + i, a, b) for i, (a, b) in enumerate(pairs)]
    _start([wo] + sum(groups, []) + late)
    _greet(range(1, 8) if first else AROUND)
    for s in pending():
        s.start()
    dkt[:] = jnp.zeros(dkt.shape, F32)
    dvt[:] = jnp.zeros(dvt.shape, F32)
    lane = lax.broadcasted_iota(jnp.int32, (1, HEAD), 1)
    for n in range(HEADS + 1):
        ours = lax.div(lane, SPLITS) == n if n < HEADS else lane < SPLITS * HEADS
        zs[n] = jnp.broadcast_to(ours.astype(F32).astype(BF), (B, HEAD))
    wo.wait()

    def lead(r):
        at = _at(r, B)
        columns = lambda m: _mt(dhm[at, :], wa[m * W : (m + 1) * W, QKV:]).astype(BF)
        ahead = columns(0)
        means = jnp.zeros((B, HEAD), F32)
        for n in range(HEADS):
            if n % 2 == 0:
                do = ahead
                if n + 2 < HEADS:
                    ahead = columns(n // 2 + 1)
            by = do[:, n % 2 * HEAD : (n % 2 + 1) * HEAD]
            doh[n, at, :] = by
            dot[n, :, at] = by.T
            qt[n, :, at] = qh[n, at, :].T
            mean = jnp.sum(by.astype(F32) * o[at, n * HEAD : (n + 1) * HEAD].astype(F32), -1, keepdims=True)
            means = jnp.where(lax.div(lane, SPLITS) == n, -mean, means)
        high = means.astype(BF).astype(F32)
        middle = (means - high).astype(BF).astype(F32)
        parts = jnp.where(lax.rem(lane, SPLITS) == 1, middle, means - high - middle)
        dl[at, :] = jnp.where(lax.rem(lane, SPLITS) == 0, high, parts).astype(BF)

    def begin(r):
        for k in range(blocks):
            _when(r == k, lambda: _wait(groups[k]))
        lead(r)

    _loop(blocks, begin)
    for s in pending():
        s.forward()
    wa[:, QKV:] = _tm(o[:], dhm[:]).astype(BF)
    if first:
        own = [_Scatter(*[_blocks(wa.at[:, cols], ROWS, k) for k in range(2)], *s) for cols, s in
               ((pl.ds(QKV, D), refs[:4]), (pl.ds(0, QKV), [scatter_gu[0].at[:, :, pl.ds(0, QKV)], *refs[4:7]]))]
        own[0].start()
    _wait(late)

    def attend(g):
        iq = blocks - 1 - g
        at = _at(iq, B)
        _when(g == 2, *[lambda s=s: s.pass_on() for s in pending()])
        if first:
            _when(g == 1, lambda: own[0].forward())
            _when(g == 2, lambda: own[0].pass_on())
        _flash_back(iq, qh, qt, doh, dot, la, dl, zs, k_s, v_s, dq, dkt, dvt, (p0, p1), (x0, x1))
        c, s = cos[at, :], sin[at, :]

        def turn(m):
            for n in (2 * m, 2 * m + 1):
                dqkv[at, _at(n, HEAD)] = _turn_back(dq[n] * SCALE, c, s)

        _loop(PAIRS, turn)
        dqkv[at, D : D + HEAD] = _turn_back((dkt[:, at] * (SCALE / E)).T, c, s)
        dqkv[at, D + HEAD :] = dvt[:, at].T.astype(BF)

    _loop(blocks, attend)
    dw = lambda: wa.__setitem__((slice(None), slice(0, QKV)), _tm(a_s[:], dqkv[:]).astype(BF))
    if first:
        dw()
        mine, all_s, all_sem = refs[7:]
        own[1].start()
        gu, d = pending()
        squares = gu.finish(ggu_o) + d.finish(gd_o) + sq_a[:] + sq_b[:]
        own[1].forward()
        squares += own[0].finish(ga_o.at[:, pl.ds(QKV, D)])
        own[1].pass_on()
        mine[:] = own[1].finish(ga_o.at[:, pl.ds(0, QKV)]) + squares
        me, _ = _place()
        copies = [_remote(mine, all_s.at[me], all_sem, r, r) for r in range(1, 8)]
        _start(copies)
        all_s[me] = mine[:]
        _wait(copies)
        total = jnp.sum(jnp.sum(jnp.sum(all_s[:], axis=0), axis=1, keepdims=True), axis=0, keepdims=True)
        factor_o[:] = jnp.broadcast_to(jnp.minimum(1.0, 0.5 * lax.rsqrt(total / count + 1e-30)), factor_o.shape)
    else:
        out = lambda r: _local(h.at[_at(r, B), :], dh_o.at[_at(r, B), :], split_sem.at[2, r])

        def back(r):
            at = _at(r, B)
            o[at, :] = _mt(dqkv[at, :], wa[:, :QKV]).astype(BF)
            h[at, :] = _norm_back(h[at, :], o[at, :], dhm[at, :])
            out(r).start()

        _loop(blocks, back)
        dw()
        copies = _split_out(wa, ROWS, keep_o, send_o, split_sem)
        gu, d = pending()
        sq_o[:] = gu.finish(ggu_o) + d.finish(gd_o)
        _wait(copies + [out(r) for r in range(blocks)])


def attn_back(saved, dhm, h, layer, pending, squares, count, talks):
    T = h.shape[0]
    args = [dhm, h] + [saved[n] for n in ("a", "q", "k", "v", "o", "la", "cos", "sin", "wa")] + [*pending, *squares]
    specs = [ANY] * (11 + len(pending)) + [WHOLE] * len(squares)
    dw, small = ((4, ROWS, WA), BF), ((8, HEAD), F32)
    outs, out_specs = [((ROWS, GU), BF), ((FROWS, D), BF)], [WHOLE, WHOLE]
    tile = VM((B, B), BF)
    scratch = [VM((T, D), BF), VM((T, D), BF), VM((HEADS, T, HEAD), BF), VM((T, HEAD), BF), VM((T, HEAD), BF), VM((T, D), BF), VM((T, HEAD), BF),
               VM((T, HEAD), F32), VM((T, HEAD), F32), VM((D, WA), BF), VM((HEADS, T, HEAD), BF), VM((T, QKV), BF), VM((T, D), BF),
               VM((HEADS, HEAD, T), BF), VM((HEADS, HEAD, T), BF), VM((T, HEAD), BF), VM((HEADS + 1, B, HEAD), BF), VM((HEADS, B, HEAD), F32),
               VM((HEAD, T), F32), VM((HEAD, T), F32), tile, tile, tile, tile, DMA((21,)), DMA((3, 4)),
               *_scatter_scratch(ROWS, GU), *_scatter_scratch(FROWS, D)]
    if layer == FIRST:
        outs += [((ROWS, WA), BF), small]
        out_specs += [WHOLE, WHOLE]
        scratch.append(VM((4, ROWS, D), BF))
        for width in (D, QKV):
            scratch += [VM((4, ROWS, width), BF), VM((3, ROWS, width), BF), DMA((2, 10))]
        scratch += [VM((8, HEAD), F32), VM((8, 8, HEAD), F32), DMA((2, 8))]
    else:
        outs += [small, ((T, D), BF), dw, dw]
        out_specs += [WHOLE, ANY, ANY, ANY]
    return _call(functools.partial(_attn_back, layer=layer, count=count), "attn_back", args, specs, outs, out_specs, scratch, 5 * 10**10, talks)


TRIOS = range(21)


def _adamw(*refs, layers):
    refs = iter(refs)
    take = lambda count: list(itertools.islice(refs, count))
    (factor_ref,) = take(1)
    grads = take(3 * layers)
    given, out, held = (take(len(TRIOS)) for _ in range(3))
    g_held = take(len(grads))
    load_sem, grad_sem, store_sem = refs
    factor = factor_ref[:1, :1]
    where = [(which, sum(widths[:i]), width) for which, widths in enumerate(((D, HEAD, HEAD, D), (FF, FF), (D,))) for i, width in enumerate(widths)]
    fetch = [_local(a, b, grad_sem.at[i]) for i, (a, b) in enumerate(zip(grads, g_held))]

    def moves(layer, i):
        trio = TRIOS[i::7]
        return ([_local(given[k].at[layer], held[k].at[layer], load_sem.at[layer, k]) for k in trio],
                [_local(held[k].at[layer], out[k].at[layer], store_sem.at[layer, k]) for k in trio])

    every = [(layer, i) for layer in range(layers) for i in range(7)]
    for layer, i in every:
        if where[i][1] == 0:
            fetch[3 * layer + where[i][0]].start()
        _start(moves(layer, i)[0])
    for layer, i in every:
        which, start, width = where[i]
        if start == 0:
            fetch[3 * layer + which].wait()
        loads, stores = moves(layer, i)
        _wait(loads)
        w_ref, m_ref, v_ref = (held[k].at[layer] for k in TRIOS[i::7])
        g_ref = g_held[3 * layer + which]

        def step(r):
            at = _at(r, 16)
            g = g_ref[at, start : start + width].astype(F32) * factor
            m = 0.9 * m_ref[at, :] + 0.1 * g
            v = 0.95 * v_ref[at, :] + 0.05 * g * g
            w = w_ref[at, :].astype(F32)
            w_ref[at, :] = (w - 0.02 * (m * lax.rsqrt(v + 1e-8) + 0.1 * w)).astype(BF)
            m_ref[at, :] = m
            v_ref[at, :] = v

        _loop(g_ref.shape[0] // 16, step)
        _start(stores)
    for layer, i in every:
        _wait(moves(layer, i)[1])


def adamw(factor, grads, weights, m, v):
    layers = len(grads)
    flat, given = sum(grads, []), [*weights, *m, *v]
    whole = lambda a: VM(a.shape, a.dtype)
    return _call(functools.partial(_adamw, layers=layers), "adamw", [factor, *flat, *given], [WHOLE] + [ANY] * (len(flat) + len(given)),
                 [(a.shape, a.dtype) for a in given], [ANY] * len(given),
                 [whole(a) for a in given + flat] + [DMA((layers, len(given))), DMA((len(flat),)), DMA((layers, len(given)))], 10**9, None)


def rotary_tables(tokens):
    half = HEAD // 2
    rate = THETA ** (-np.arange(half, dtype=np.float64) / half)

    def table(places):
        angle = np.concatenate([places[:, None] * rate] * 2, 1)
        return jnp.asarray(np.stack([np.cos(angle), np.sin(angle)]), F32)

    return table(np.arange(COARSE)), table(np.arange(0, tokens, COARSE))


def solution(mesh):
    def step(x, dy, *arrays):
        weights, m, v = (arrays[i : i + 7] for i in (0, 7, 14))
        x, dy = x[0], dy[0]
        names = ("a", "hm", "q", "k", "v", "o", "la", "s", "r", "hid", "bt", "h1", "cos", "sin", "wa", "wgu", "wd")
        saved = dict(zip(names, forward(x, weights)))
        count = 8 * sum(w.size for w in weights)
        by_hm, *mlp1 = mlp_back(saved, dy, LAST, None, None)
        ggu1, gd1, sq_a, by_h, *attn1 = attn_back(saved, by_hm, saved["h1"], LAST, mlp1, [], count, 1)
        by_hm, *mlp0, ga1, sq_b = mlp_back(saved, by_h, FIRST, attn1, 2)
        ggu0, gd0, ga0, factor = attn_back(saved, by_hm, x, FIRST, mlp0, [sq_a, sq_b], count, 3)
        return tuple(adamw(factor, [[ga0, ggu0, gd0], [ga1, ggu1, gd1]], weights, m, v))

    states, cut = P(("rep", "dp"), None, None), P(None, "dp", None)
    return jax.shard_map(
        step,
        mesh=mesh,
        in_specs=(states, states) + (cut,) * 21,
        out_specs=(P("rep", "dp", None),) * 21,
        check_vma=False,
    )
```
